8 devices in a mesh: dp: 1 (over z), tpy: 2 (over y), tpx: 4 (over x, core).
Axes of the slice: x: 2, y: 2, z: 1, core: 2. Of those that a mesh axis runs over, the one named last changes fastest.
Arguments:
- embeds: bfloat16 [3, 128, 4096], P(None, 'dp', 'tpy')
- start_pos: int32 [128], P('dp')
- k_cache: bfloat16 [2, 128, 64, 32, 128], P(None, ('dp', 'tpy'), None, 'tpx')
- v_cache: bfloat16 [2, 128, 64, 32, 128], P(None, ('dp', 'tpy'), None, 'tpx')
- w_query: bfloat16 [2, 4096, 4096], P(None, 'tpy', 'tpx')
- w_key: bfloat16 [2, 4096, 4096], P(None, 'tpy', 'tpx')
- w_value: bfloat16 [2, 4096, 4096], P(None, 'tpy', 'tpx')
- w_out: bfloat16 [2, 4096, 4096], P(None, 'tpx', 'tpy')
- w_gate: bfloat16 [2, 4096, 11008], P(None, 'tpy', 'tpx')
- w_up: bfloat16 [2, 4096, 11008], P(None, 'tpy', 'tpx')
- w_down: bfloat16 [2, 11008, 4096], P(None, 'tpx', 'tpy')
- q_gain: bfloat16 [2, 4096], P(None, 'tpx')
- k_gain: bfloat16 [2, 4096], P(None, 'tpx')
- attn_gain: bfloat16 [2, 4096], P(None, 'tpy')
- mlp_gain: bfloat16 [2, 4096], P(None, 'tpy')
Outputs:
- output 1: bfloat16 [3, 128, 4096], P(None, 'dp', 'tpy')
- output 2: bfloat16 [2, 128, 64, 32, 128], P(None, ('dp', 'tpy'), None, 'tpx')
- output 3: bfloat16 [2, 128, 64, 32, 128], P(None, ('dp', 'tpy'), None, 'tpx')
All inputs are finite; a program needn't handle non-finite values.
Results may differ from the reference program's by a relative error of at most 0.02.
Values are sent between devices in bfloat16 or wider.
A program may use at most 1 GiB of HBM per device.

```python
import math
import jax
import jax.numpy as jnp
from jax import lax

D = 4096
HEADS = 32
KV_HEADS = 32
FF = 11008
HEAD = 128
BATCH = 128
SEQ = 64
STEPS = 3
LAYERS = 2
PROFILE = 16
EPS = 1e-6
THETA = 500000.0
Q_WIDTH = HEADS * HEAD
KV_WIDTH = KV_HEADS * HEAD
GROUP = HEADS // KV_HEADS
BLOCK_COLS = D // PROFILE
SCORE_SCALE = 1.0 / math.sqrt(HEAD)


def setup_inputs(seed: int = 0, part: int = 0) -> dict:
    base_key = jax.random.key(seed)
    shared = jax.random.split(base_key, 16)
    part_keys = jax.random.split(jax.random.fold_in(base_key, part), 6)
    embeds = jax.random.normal(part_keys[0], (STEPS, BATCH, D), jnp.float32)
    last_start = SEQ - 3
    draw_a = jax.random.randint(part_keys[1], (BATCH,), 0, last_start + 1)
    draw_b = jax.random.randint(part_keys[2], (BATCH,), 0, last_start + 1)
    top_row = jax.random.randint(part_keys[3], (), 0, BATCH)
    start_pos = jnp.where(jnp.arange(BATCH) == top_row, last_start, (draw_a * draw_b) // last_start).astype(jnp.int32)
    k_cache = jax.random.normal(part_keys[4], (LAYERS, BATCH, SEQ, KV_HEADS, HEAD), jnp.float32)
    v_cache = jax.random.normal(part_keys[5], (LAYERS, BATCH, SEQ, KV_HEADS, HEAD), jnp.float32)
    in_scale = 1.0 / math.sqrt(D)
    q_heads = jnp.exp(0.4 * jax.random.normal(shared[0], (LAYERS, 1, HEADS, 1), jnp.float32))
    k_heads = jnp.exp(0.4 * jax.random.normal(shared[1], (LAYERS, 1, KV_HEADS, 1), jnp.float32))
    v_heads = jnp.exp(0.4 * jax.random.normal(shared[2], (LAYERS, 1, KV_HEADS, 1), jnp.float32))
    w_query = (jax.random.normal(shared[3], (LAYERS, D, HEADS, HEAD), jnp.float32) * q_heads * in_scale).reshape(LAYERS, D, Q_WIDTH)
    w_key = (jax.random.normal(shared[4], (LAYERS, D, KV_HEADS, HEAD), jnp.float32) * k_heads * in_scale).reshape(LAYERS, D, KV_WIDTH)
    w_value = (jax.random.normal(shared[5], (LAYERS, D, KV_HEADS, HEAD), jnp.float32) * v_heads * in_scale).reshape(LAYERS, D, KV_WIDTH)
    out_profile = jnp.repeat(jnp.exp(0.5 * jax.random.normal(shared[6], (LAYERS, 1, PROFILE), jnp.float32)), BLOCK_COLS, axis=2)
    down_profile = jnp.repeat(jnp.exp(0.5 * jax.random.normal(shared[7], (LAYERS, 1, PROFILE), jnp.float32)), BLOCK_COLS, axis=2)
    w_out = jax.random.normal(shared[8], (LAYERS, Q_WIDTH, D), jnp.float32) * out_profile / math.sqrt(Q_WIDTH)
    w_gate = jax.random.normal(shared[9], (LAYERS, D, FF), jnp.float32) * in_scale
    w_up = jax.random.normal(shared[10], (LAYERS, D, FF), jnp.float32) * in_scale
    w_down = jax.random.normal(shared[11], (LAYERS, FF, D), jnp.float32) * down_profile / math.sqrt(FF)
    q_gain = jax.random.uniform(shared[12], (LAYERS, Q_WIDTH), jnp.float32, minval=0.5, maxval=1.5)
    k_gain = jax.random.uniform(shared[13], (LAYERS, KV_WIDTH), jnp.float32, minval=0.5, maxval=1.5)
    attn_gain = jax.random.uniform(shared[14], (LAYERS, D), jnp.float32, minval=0.5, maxval=1.5)
    mlp_gain = jax.random.uniform(shared[15], (LAYERS, D), jnp.float32, minval=0.5, maxval=1.5)
    return {
        'embeds': embeds.astype(jnp.bfloat16),
        'start_pos': start_pos,
        'k_cache': k_cache.astype(jnp.bfloat16),
        'v_cache': v_cache.astype(jnp.bfloat16),
        'w_query': w_query.astype(jnp.bfloat16),
        'w_key': w_key.astype(jnp.bfloat16),
        'w_value': w_value.astype(jnp.bfloat16),
        'w_out': w_out.astype(jnp.bfloat16),
        'w_gate': w_gate.astype(jnp.bfloat16),
        'w_up': w_up.astype(jnp.bfloat16),
        'w_down': w_down.astype(jnp.bfloat16),
        'q_gain': q_gain.astype(jnp.bfloat16),
        'k_gain': k_gain.astype(jnp.bfloat16),
        'attn_gain': attn_gain.astype(jnp.bfloat16),
        'mlp_gain': mlp_gain.astype(jnp.bfloat16),
    }


def rms_scale(values):
    return lax.rsqrt(jnp.mean(values * values, axis=-1, keepdims=True) + EPS)


def rope_rotate(values, positions):
    half_dim = HEAD // 2
    inv_freq = jnp.power(THETA, jnp.arange(half_dim, dtype=jnp.float32) * (-2.0 / HEAD))
    angles = positions.astype(jnp.float32)[..., None] * inv_freq
    cos_part = jnp.cos(angles)[..., None, :]
    sin_part = jnp.sin(angles)[..., None, :]
    first_half = values[..., :half_dim]
    second_half = values[..., half_dim:]
    return jnp.concatenate([first_half * cos_part - second_half * sin_part, second_half * cos_part + first_half * sin_part], axis=-1)


def decode_step(caches, step_in, params, start_pos):
    k_layer, v_layer = caches
    hidden, step_idx = step_in
    w_query, w_key, w_value, w_out, w_gate, w_up, w_down, q_gain, k_gain, attn_gain, mlp_gain = params
    positions = start_pos + step_idx
    q_raw = jnp.dot(hidden, w_query, preferred_element_type=jnp.float32).astype(jnp.bfloat16).astype(jnp.float32)
    k_raw = jnp.dot(hidden, w_key, preferred_element_type=jnp.float32).astype(jnp.bfloat16).astype(jnp.float32)
    v_new = jnp.dot(hidden, w_value, preferred_element_type=jnp.float32).astype(jnp.bfloat16).reshape(BATCH, KV_HEADS, HEAD)
    q_norm = q_raw * rms_scale(q_raw) * q_gain.astype(jnp.float32)
    k_norm = k_raw * rms_scale(k_raw) * k_gain.astype(jnp.float32)
    q_rot = rope_rotate(q_norm.reshape(BATCH, HEADS, HEAD), positions).astype(jnp.bfloat16)
    k_rot = rope_rotate(k_norm.reshape(BATCH, KV_HEADS, HEAD), positions).astype(jnp.bfloat16)
    slot_hit = (jnp.arange(SEQ)[None, :] == positions[:, None])[:, :, None, None]
    k_layer = jnp.where(slot_hit, k_rot[:, None], k_layer)
    v_layer = jnp.where(slot_hit, v_new[:, None], v_layer)
    q_grp = q_rot.reshape(BATCH, KV_HEADS, GROUP, HEAD).astype(jnp.float32)
    scores = jnp.einsum('bkgd,bskd->bkgs', q_grp, k_layer.astype(jnp.float32)) * SCORE_SCALE
    visible = (jnp.arange(SEQ)[None, :] <= positions[:, None])[:, None, None, :]
    attn_probs = jax.nn.softmax(jnp.where(visible, scores, -1e30), axis=-1).astype(jnp.bfloat16)
    attn_mix = jnp.einsum('bkgs,bskd->bkgd', attn_probs.astype(jnp.float32), v_layer.astype(jnp.float32)).astype(jnp.bfloat16).reshape(BATCH, Q_WIDTH)
    attn_out = jnp.dot(attn_mix, w_out, preferred_element_type=jnp.float32).astype(jnp.bfloat16).astype(jnp.float32)
    middle = (hidden.astype(jnp.float32) + attn_out * rms_scale(attn_out) * attn_gain.astype(jnp.float32)).astype(jnp.bfloat16)
    gate_val = jnp.dot(middle, w_gate, preferred_element_type=jnp.float32).astype(jnp.bfloat16).astype(jnp.float32)
    up_val = jnp.dot(middle, w_up, preferred_element_type=jnp.float32).astype(jnp.bfloat16).astype(jnp.float32)
    gated_act = (jax.nn.silu(gate_val) * up_val).astype(jnp.bfloat16)
    down_out = jnp.dot(gated_act, w_down, preferred_element_type=jnp.float32).astype(jnp.bfloat16).astype(jnp.float32)
    result = (middle.astype(jnp.float32) + down_out * rms_scale(down_out) * mlp_gain.astype(jnp.float32)).astype(jnp.bfloat16)
    return (k_layer, v_layer), result


def reference(embeds, start_pos, k_cache, v_cache, w_query, w_key, w_value, w_out, w_gate, w_up, w_down, q_gain, k_gain, attn_gain, mlp_gain):
    def layer_body(hidden_seq, layer_in):
        params = layer_in[2:]

        def step_body(caches, step_in):
            return decode_step(caches, step_in, params, start_pos)

        caches, outputs = lax.scan(step_body, (layer_in[0], layer_in[1]), (hidden_seq, jnp.arange(STEPS)))
        return outputs, caches

    final_hidden, new_caches = lax.scan(layer_body, embeds, (k_cache, v_cache, w_query, w_key, w_value, w_out, w_gate, w_up, w_down, q_gain, k_gain, attn_gain, mlp_gain))
    return final_hidden, new_caches[0], new_caches[1]
```

```python
import functools
import math
import jax
import jax.numpy as jnp
from jax import lax
from jax.experimental import pallas as pl
from jax.experimental.pallas import tpu as pltpu
from jax.sharding import PartitionSpec as P

HEAD_DIM = 128
EPS = 1e-6
THETA = 500000.0
SCORE_SCALE = 1.0 / math.sqrt(HEAD_DIM)
NEG_BIG = -1e30
MESH = pl.DeviceIdType.MESH
BF = jnp.bfloat16
F32 = jnp.float32

L = 2
T = 3
NB = 2
RB = 32
R = T * RB
HL = 8
DW = 2048
QW = HL * HEAD_DIM
FW = 2752
FP = 2816
SEQ = 64
SH = SEQ * HL
CB = 4
NCH = RB // CB
TW = 512
HALF = DW // 2
GU_TILES = [(0, 512), (512, 512), (1024, 512), (1536, 512), (2048, 512), (2560, 256)]
QKV_TILES = [(0, 0), (0, 512), (0, 1024), (0, 1536), (1, 0), (1, 512)]


def dot(a, b):
    return jnp.dot(a, b, preferred_element_type=F32)


def dot_t(a, b):
    return lax.dot_general(a, b, (((1,), (1,)), ((), ())), preferred_element_type=F32)


def main_kernel(start_ref, emb_ref, kc_ref, vc_ref, wq_ref, wk_ref, wv_ref, wo_ref, wg_ref, wu_ref, wd_ref,
                qg_ref, kg_ref, ag_ref, mg_ref, cos_ref, sin_ref,
                y_ref, kn_ref, vn_ref,
                X, W1, WO, WD, GP, GR, C, OB, QS, KS, VS, OS, KO, VO, KB, VB, XP, XC, XS, XR, AF, RSUM, RSC, ST, SR,
                in_sem, q_wsem, g_wsem, o_wsem, d_wsem, kv_sem, ko_sem, y_sem,
                g_ss, g_rs, c_ss, c_rs, o_ss, o_rs, p_ss, p_rs, x_ss, x_rs, a_ss, a_rs, st_ss, st_rs):
    ty = lax.axis_index("tpy")
    tx = lax.axis_index("tpx")
    core = lax.rem(tx, 2)
    oy = 1 - ty
    cx = tx + 1 - 2 * core
    xx = lax.rem(tx + 2, 4)
    dx = 3 - tx
    ypeer = {"tpy": oy}
    cpeer = {"tpx": cx}
    xpeer = {"tpx": xx}
    xdiag = {"tpx": dx}
    ydiag = {"tpy": oy, "tpx": cx}
    own_half = pl.ds(pl.multiple_of(core * HALF, HALF), HALF)
    oth_half = pl.ds(pl.multiple_of((1 - core) * HALF, HALF), HALF)

    def rc(src, dst, ss, rs, dev):
        return pltpu.make_async_remote_copy(src_ref=src, dst_ref=dst, send_sem=ss, recv_sem=rs, device_id=dev, device_id_type=MESH)

    def lc(src, dst, sem):
        return pltpu.make_async_copy(src, dst, sem)

    def emb_copies():
        out = []
        for m in range(NB):
            for y in range(2):
                for t in range(T):
                    out.append(lc(emb_ref.at[t, pl.ds(y * NB * RB + m * RB, RB)], X.at[m, y, pl.ds(t * RB, RB)], in_sem.at[(m * 2 + y) * T + t]))
        return out

    def qkv_load(l, n):
        j, c0 = QKV_TILES[n]
        src = (wq_ref, wk_ref, wv_ref)[n // 2]
        return lc(src.at[l, :, pl.ds((n % 2) * TW, TW)], W1.at[j, :, pl.ds(c0, TW)], q_wsem.at[n])

    def qkv_loads(l):
        return [qkv_load(l, n) for n in range(6)]

    def gu_loads(l):
        return [lc((wg_ref, wu_ref)[j].at[l, pl.ds(r * 512, 512)], W1.at[j, pl.ds(r * 512, 512)], g_wsem.at[j * 4 + r]) for r in range(4) for j in range(2)]

    def wo_loads(l):
        return [lc(wo_ref.at[l], WO, o_wsem.at[0])]

    def wd_loads(l):
        return [lc(wd_ref.at[l, pl.ds(r * 688, 688)], WD.at[pl.ds(r * 688, 688)], d_wsem.at[r]) for r in range(4)]

    def start(copies):
        for cp in copies:
            cp.start()

    def wait(copies):
        for cp in copies:
            cp.wait()

    def kv_copies(l, m, c, slot):
        rows = pl.ds(m * RB + c * CB, CB)
        return [lc(kc_ref.at[l, rows], KB.at[slot], kv_sem.at[0, slot]), lc(vc_ref.at[l, rows], VB.at[slot], kv_sem.at[1, slot])]

    start(emb_copies())
    start(qkv_loads(0))

    barrier = pltpu.get_barrier_semaphore()
    for dev in (ypeer, cpeer, xpeer, xdiag, ydiag):
        pl.semaphore_signal(barrier, inc=1, device_id=dev, device_id_type=MESH)
    pl.semaphore_wait(barrier, 5)

    start(kv_copies(0, 0, 0, 0))
    start(kv_copies(0, 0, 1, 1))
    start(wo_loads(0))
    start(wd_loads(0))

    def tile_copy(m, j, n, c0, w):
        return rc(GP.at[m, j, oy, :, pl.ds(c0, w)], GR.at[m, j, :, pl.ds(c0, w)], g_ss.at[m, j, n], g_rs.at[m, j, n], ypeer)

    def compute_tile(m, j, c0, w):
        xm = X[m].reshape(2 * R, DW)
        res = dot(xm, W1[j, :, pl.ds(c0, w)]).astype(BF)
        GP[m, j, :, :, pl.ds(c0, w)] = res.reshape(2, R, w)

    def phase_q(m, l, first):
        for j, cnt in ((0, 4), (1, 2)):
            if first:
                for i in range(cnt):
                    qkv_load(l, j * 4 + i).wait()
                    compute_tile(m, j, i * TW, TW)
                    tile_copy(m, j, i, i * TW, TW).start()
            else:
                def body(i, _):
                    c0 = pl.multiple_of(i * TW, TW)
                    compute_tile(m, j, c0, TW)
                    tile_copy(m, j, i, c0, TW).start()
                    return 0
                lax.fori_loop(0, cnt, body, 0)

    def phase_g(m, l, send):
        def body(i, _):
            c0 = pl.multiple_of(i * TW, TW)
            for j in range(2):
                compute_tile(m, j, c0, TW)
                if send:
                    tile_copy(m, j, i, c0, TW).start()
            return 0
        lax.fori_loop(0, 5, body, 0)
        for j in range(2):
            compute_tile(m, j, 2560, 192)
            if send:
                tile_copy(m, j, 5, 2560, 256).start()

    def send_g(m):
        for n, (c0, w) in enumerate(GU_TILES):
            for j in range(2):
                tile_copy(m, j, n, c0, w).start()

    def stat_copies(kind, m):
        peers = (cpeer, xpeer, xdiag) if kind == 0 else (cpeer, ypeer, ydiag)
        return [rc(ST.at[kind, m], SR.at[kind, m, k], st_ss.at[kind, m, k], st_rs.at[kind, m, k], peers[k]) for k in range(3)]

    def stat_send(kind, m):
        v0 = jnp.sum(RSUM[0], axis=1, keepdims=True)
        v1 = jnp.sum(RSUM[1], axis=1, keepdims=True)
        lane = lax.broadcasted_iota(jnp.int32, (R, 128), 1)
        both = jnp.where(lane == 0, v0, v1)
        full = jnp.concatenate([both, jnp.zeros((128 - R, 128), F32)], axis=0)
        ST[kind, m] = full.T[0:8]
        start(stat_copies(kind, m))

    def stat_recv(kind, m):
        wait(stat_copies(kind, m))
        total = (ST[kind, m] + SR[kind, m, 0]) + (SR[kind, m, 1] + SR[kind, m, 2])
        back = jnp.concatenate([total] * 16, axis=0).T
        scale = lax.rsqrt(back / 4096.0 + EPS)
        RSC[0] = jnp.broadcast_to(scale[0:R, 0:1], (R, 128))
        RSC[1] = jnp.broadcast_to(scale[0:R, 1:2], (R, 128))

    def phase_s(m):
        for n, (j, c0) in enumerate(QKV_TILES):
            tile_copy(m, j, c0 // TW, c0, TW).wait()

        def body(i, _):
            rows = pl.ds(pl.multiple_of(i * 16, 16), 16)
            for j in range(2):
                acc = jnp.zeros((16, 128), F32)
                for h in range(8):
                    cols = pl.ds((j * 8 + h) * 128, 128)
                    z = (GP[m, 0, ty, rows, cols].astype(F32) + GR[m, 0, rows, cols].astype(F32)).astype(BF)
                    GR[m, 0, rows, cols] = z
                    zf = z.astype(F32)
                    acc = acc + zf * zf
                RSUM[j, rows] = acc
            for h in range(8):
                cols = pl.ds(h * 128, 128)
                GR[m, 1, rows, cols] = (GP[m, 1, ty, rows, cols].astype(F32) + GR[m, 1, rows, cols].astype(F32)).astype(BF)
            return 0
        lax.fori_loop(0, R // 16, body, 0)
        stat_send(0, m)

    def phase_t1(m, l):
        stat_recv(0, m)

        def body(i, _):
            rows = pl.ds(pl.multiple_of(i * 16, 16), 16)
            t = i // 2
            dst = pl.ds(pl.multiple_of(lax.rem(i, 2) * 16, 16), 16)
            cosv = cos_ref[m, rows]
            sinv = sin_ref[m, rows]
            for j, (out, gain) in enumerate(((QS, qg_ref), (KS, kg_ref))):
                scale = RSC[j, rows]
                for h in range(8):
                    z = GR[m, 0, rows, pl.ds((j * 8 + h) * 128, 128)].astype(F32)
                    z = z * scale * gain[l, :, pl.ds(h * 128, 128)]
                    rot = z * cosv + pltpu.roll(z, 64, 1) * sinv
                    out[t, dst, h, :] = rot.astype(BF).astype(F32)
            for h in range(8):
                VS[t, dst, h, :] = GR[m, 1, rows, pl.ds(h * 128, 128)].astype(F32)
            return 0
        lax.fori_loop(0, R // 16, body, 0)

    def ko_copies(l, m):
        rows = pl.ds(m * RB, RB)
        return [lc(KO.at[m], kn_ref.at[l, rows], ko_sem.at[0, m]), lc(VO.at[m], vn_ref.at[l, rows], ko_sem.at[1, m])]

    def o_copy(m):
        return rc(OB.at[m, ty], OB.at[m, ty], o_ss.at[m], o_rs.at[m], ypeer)

    def phase_t2(m, l):
        if l > 0:
            wait(ko_copies(l - 1, m))
        row = lax.broadcasted_iota(jnp.int32, (T * HL, SH), 0)
        col = lax.broadcasted_iota(jnp.int32, (T * HL, SH), 1)
        colm = jnp.where(lax.rem(row, HL) == lax.rem(col, HL), col, SH)
        rown = lax.broadcasted_iota(jnp.int32, (T * HL, T * HL), 0)
        coln = lax.broadcasted_iota(jnp.int32, (T * HL, T * HL), 1)
        newm = (lax.rem(rown, HL) == lax.rem(coln, HL)) & (coln <= rown)

        def chunk(c, _):
            slot = lax.rem(c, 2)
            wait(kv_copies(l, m, c, slot))
            for k in range(CB):
                i = c * CB + k
                q = QS[:, i].reshape(T * HL, HEAD_DIM).astype(BF)
                kn = KS[:, i].reshape(T * HL, HEAD_DIM).astype(BF)
                vn = VS[:, i].reshape(T * HL, HEAD_DIM).astype(BF)
                limit = start_ref[m * RB + i] * HL
                s_old = jnp.where(colm < limit, dot_t(q, KB[slot, k]) * SCORE_SCALE, NEG_BIG)
                s_new = jnp.where(newm, dot_t(q, kn) * SCORE_SCALE, NEG_BIG)
                top = jnp.maximum(jnp.max(s_old, axis=1, keepdims=True), jnp.max(s_new, axis=1, keepdims=True))
                e_old = jnp.exp(s_old - top)
                e_new = jnp.exp(s_new - top)
                den = jnp.sum(e_old, axis=1, keepdims=True) + jnp.sum(e_new, axis=1, keepdims=True)
                o = dot((e_old / den).astype(BF), VB[slot, k]) + dot((e_new / den).astype(BF), vn)
                OS[:, i] = o.reshape(T, HL, HEAD_DIM)
                KO[m, i] = kn
                VO[m, i] = vn

            @pl.when(c < NCH - 2)
            def _():
                start(kv_copies(l, m, c + 2, slot))
            return 0
        lax.fori_loop(0, NCH, chunk, 0)
        start(ko_copies(l, m))
        nxt = (l, m + 1) if m + 1 < NB else (l + 1, 0)
        if nxt[0] < L:
            start(kv_copies(nxt[0], nxt[1], 0, 0))
            start(kv_copies(nxt[0], nxt[1], 1, 1))

        def body(i, _):
            rows = pl.ds(pl.multiple_of(i * 16, 16), 16)
            t = i // 2
            src = pl.ds(pl.multiple_of(lax.rem(i, 2) * 16, 16), 16)
            for h in range(8):
                OB[m, ty, rows, pl.ds(h * 128, 128)] = OS[t, src, h, :].astype(BF)
            return 0
        lax.fori_loop(0, R // 16, body, 0)
        o_copy(m).start()

    def p_copy(m):
        return rc(XP.at[m, :, oth_half], XC.at[m], p_ss.at[m], p_rs.at[m], cpeer)

    def x_copy(ph, m):
        return rc(XS.at[m], XR.at[ph, m], x_ss.at[m], x_rs.at[ph, m], xpeer)

    def a_copy(m):
        return rc(AF.at[m, :, own_half], AF.at[m, :, own_half], a_ss.at[m], a_rs.at[m], cpeer)

    def phase_o(m, l):
        o_copy(m).wait()
        for half in (1 - core, core):
            def body(i, _):
                cols = pl.ds(pl.multiple_of(half * HALF + i * TW, TW), TW)
                XP[m, :, cols] = dot(OB[m].reshape(2 * R, QW), WO[:, cols]).astype(BF)
                return 0
            lax.fori_loop(0, 2, body, 0)
            if half is not core:
                p_copy(m).start()

    def phase_d(m, l):
        for n, (c0, w) in enumerate(GU_TILES):
            c_copy(m, n, c0, w).wait()
        for half in (1 - core, core):
            def body(i, _):
                cols = pl.ds(pl.multiple_of(half * HALF + i * TW, TW), TW)
                cm = C[m].reshape(2 * R, FP)
                XP[m, :, cols] = dot(cm[:, :FW], WD[:, cols]).astype(BF)
                return 0
            lax.fori_loop(0, 2, body, 0)
            if half is not core:
                p_copy(m).start()

    def phase_2(ph, m):
        p_copy(m).wait()

        def body(i, _):
            rows = pl.ds(pl.multiple_of(i * 16, 16), 16)
            XS[m, rows] = (XP[m, rows, own_half].astype(F32) + XC[m, rows].astype(F32)).astype(BF)
            return 0
        lax.fori_loop(0, 2 * R // 16, body, 0)
        x_copy(ph, m).start()

    def phase_3(ph, m):
        x_copy(ph, m).wait()

        def body(i, _):
            rows = pl.ds(pl.multiple_of(i * 16, 16), 16)
            z = (XS[m, rows].astype(F32) + XR[ph, m, rows].astype(F32)).astype(BF)
            AF[m, rows, own_half] = z
            zf = z.astype(F32)
            sq = zf * zf
            acc = sq[:, 0:128]
            for h in range(1, 8):
                acc = acc + sq[:, h * 128:(h + 1) * 128]
            RSUM[i // 6, pl.ds(pl.multiple_of(lax.rem(i, 6) * 16, 16), 16)] = acc
            return 0
        lax.fori_loop(0, 2 * R // 16, body, 0)
        a_copy(m).start()
        stat_send(1 + ph, m)

    def phase_h(ph, m, l):
        gain = (ag_ref, mg_ref)[ph]
        stat_recv(1 + ph, m)
        a_copy(m).wait()

        def body(i, _):
            y = i // 6
            rows = pl.ds(pl.multiple_of(lax.rem(i, 6) * 16, 16), 16)
            arow = pl.ds(pl.multiple_of(i * 16, 16), 16)
            scale = RSC[y, rows]
            for h in range(16):
                cols = pl.ds(h * 128, 128)
                X[m, y, rows, cols] = (X[m, y, rows, cols].astype(F32) + AF[m, arow, cols].astype(F32) * scale * gain[l, :, cols]).astype(BF)
            return 0
        lax.fori_loop(0, 2 * R // 16, body, 0)

    def c_copy(m, n, c0, w):
        return rc(C.at[m, ty, :, pl.ds(c0, w)], C.at[m, ty, :, pl.ds(c0, w)], c_ss.at[m, n], c_rs.at[m, n], ypeer)

    def phase_c(m, lo, hi):
        for n in range(lo, hi):
            c0, w = GU_TILES[n]
            for j in range(2):
                tile_copy(m, j, n, c0, w).wait()

            def body(i, _):
                rows = pl.ds(pl.multiple_of(i * 16, 16), 16)
                cols = pl.ds(c0, w)
                g = (GP[m, 0, ty, rows, cols].astype(F32) + GR[m, 0, rows, cols].astype(F32)).astype(BF).astype(F32)
                u = (GP[m, 1, ty, rows, cols].astype(F32) + GR[m, 1, rows, cols].astype(F32)).astype(BF).astype(F32)
                C[m, ty, rows, cols] = (jax.nn.silu(g) * u).astype(BF)
                return 0
            lax.fori_loop(0, R // 16, body, 0)
            c_copy(m, n, c0, w).start()

    def y_copies(m):
        out = []
        for y in range(2):
            for t in range(T):
                out.append(lc(X.at[m, y, pl.ds(t * RB, RB)], y_ref.at[t, pl.ds(y * NB * RB + m * RB, RB)], y_sem.at[(m * 2 + y) * T + t]))
        return out

    A, B = 0, 1
    wait(emb_copies())
    phase_q(A, 0, True)
    phase_q(B, 0, False)
    for l in range(L):
        start(gu_loads(l))
        phase_s(A)
        phase_t1(A, l)
        phase_t2(A, l)
        phase_s(B)
        phase_t1(B, l)
        wait(wo_loads(l))
        phase_o(A, l)
        phase_2(0, A)
        phase_t2(B, l)
        phase_3(0, A)
        phase_o(B, l)
        phase_h(0, A, l)
        phase_2(0, B)
        if l + 1 < L:
            start(wo_loads(l + 1))
        wait(gu_loads(l))
        phase_g(A, l, True)
        phase_3(0, B)
        phase_h(0, B, l)
        phase_g(B, l, False)
        if l + 1 < L:
            start(qkv_loads(l + 1))
        phase_c(A, 0, 6)
        send_g(B)
        wait(wd_loads(l))
        phase_d(A, l)
        phase_2(1, A)
        phase_c(B, 0, 3)
        phase_3(1, A)
        phase_h(1, A, l)
        phase_c(B, 3, 6)
        if l + 1 < L:
            phase_q(A, l + 1, True)
        else:
            start(y_copies(A))
        phase_d(B, l)
        if l + 1 < L:
            start(wd_loads(l + 1))
        phase_2(1, B)
        phase_3(1, B)
        phase_h(1, B, l)
        if l + 1 < L:
            phase_q(B, l + 1, False)
        else:
            start(y_copies(B))
    wait(y_copies(A))
    wait(y_copies(B))
    for m in range(NB):
        wait(ko_copies(L - 1, m))


def cache_kernel(start_ref, k_ref, v_ref, kn_ref, vn_ref, ko_ref, vo_ref):
    c = pl.program_id(1)
    ko_ref[...] = k_ref[...]
    vo_ref[...] = v_ref[...]
    for i in range(k_ref.shape[1]):
        p = start_ref[c * k_ref.shape[1] + i]
        for t in range(T):
            ko_ref[0, i, p + t] = kn_ref[0, i, t]
            vo_ref[0, i, p + t] = vn_ref[0, i, t]


def solution(mesh):
    act_spec = P(None, 'dp', 'tpy')
    cache_spec = P(None, ('dp', 'tpy'), None, 'tpx', None)
    col_spec = P(None, 'tpy', 'tpx')
    row_spec = P(None, 'tpx', 'tpy')
    head_gain = P(None, 'tpx')
    width_gain = P(None, 'tpy')

    def device_fn(embeds, start_pos, k_cache, v_cache, w_query, w_key, w_value, w_out, w_gate, w_up, w_down, q_gain, k_gain, attn_gain, mlp_gain):
        rows = NB * RB
        start_local = lax.dynamic_slice_in_dim(start_pos, lax.axis_index('tpy') * rows, rows)
        pos = (start_local.reshape(NB, 1, RB) + jnp.arange(T, dtype=jnp.int32)[None, :, None]).reshape(NB, R)
        inv_freq = jnp.power(THETA, jnp.arange(HEAD_DIM // 2, dtype=F32) * (-2.0 / HEAD_DIM))
        ang = pos.astype(F32)[..., None] * inv_freq
        cos_part, sin_part = jnp.cos(ang), jnp.sin(ang)
        cos2 = jnp.concatenate([cos_part, cos_part], axis=-1)
        sin2 = jnp.concatenate([-sin_part, sin_part], axis=-1)
        gains = [g.astype(F32).reshape(L, 1, -1) for g in (q_gain, k_gain, attn_gain, mlp_gain)]
        hbm = pl.BlockSpec(memory_space=pl.ANY)
        vm = pl.BlockSpec(memory_space=pltpu.VMEM)
        dma = pltpu.SemaphoreType.DMA
        y, kn, vn = pl.pallas_call(
            main_kernel,
            out_shape=[
                jax.ShapeDtypeStruct(embeds.shape, BF),
                jax.ShapeDtypeStruct((L, rows, T * HL, HEAD_DIM), BF),
                jax.ShapeDtypeStruct((L, rows, T * HL, HEAD_DIM), BF),
            ],
            in_specs=[pl.BlockSpec(memory_space=pltpu.SMEM)] + [hbm] * 10 + [vm] * 6,
            out_specs=[hbm] * 3,
            scratch_shapes=[
                pltpu.VMEM((NB, 2, R, DW), BF),
                pltpu.VMEM((2, DW, FW), BF),
                pltpu.VMEM((QW, DW), BF),
                pltpu.VMEM((FW, DW), BF),
                pltpu.VMEM((NB, 2, 2, R, FP), BF),
                pltpu.VMEM((NB, 2, R, FP), BF),
                pltpu.VMEM((NB, 2, R, FP), BF),
                pltpu.VMEM((NB, 2, R, QW), BF),
                pltpu.VMEM((T, RB, HL, HEAD_DIM), F32),
                pltpu.VMEM((T, RB, HL, HEAD_DIM), F32),
                pltpu.VMEM((T, RB, HL, HEAD_DIM), F32),
                pltpu.VMEM((T, RB, HL, HEAD_DIM), F32),
                pltpu.VMEM((NB, RB, T * HL, HEAD_DIM), BF),
                pltpu.VMEM((NB, RB, T * HL, HEAD_DIM), BF),
                pltpu.VMEM((2, CB, SH, HEAD_DIM), BF),
                pltpu.VMEM((2, CB, SH, HEAD_DIM), BF),
                pltpu.VMEM((NB, 2 * R, DW), BF),
                pltpu.VMEM((NB, 2 * R, HALF), BF),
                pltpu.VMEM((NB, 2 * R, HALF), BF),
                pltpu.VMEM((2, NB, 2 * R, HALF), BF),
                pltpu.VMEM((NB, 2 * R, DW), BF),
                pltpu.VMEM((2, R, 128), F32),
                pltpu.VMEM((2, R, 128), F32),
                pltpu.VMEM((3, NB, 8, 128), F32),
                pltpu.VMEM((3, NB, 3, 8, 128), F32),
                dma((NB * 2 * T,)), dma((6,)), dma((8,)), dma((1,)), dma((4,)), dma((2, 2)), dma((2, NB)), dma((NB * 2 * T,)),
                dma((NB, 2, 6)), dma((NB, 2, 6)), dma((NB, 6)), dma((NB, 6)), dma((NB,)), dma((NB,)),
                dma((NB,)), dma((NB,)), dma((NB,)), dma((2, NB)), dma((NB,)), dma((NB,)), dma((3, NB, 3)), dma((3, NB, 3)),
            ],
            compiler_params=pltpu.CompilerParams(collective_id=0, has_side_effects=True, vmem_limit_bytes=67043328),
            name="layers",
        )(start_local, embeds, k_cache.reshape(L, rows, SH, HEAD_DIM), v_cache.reshape(L, rows, SH, HEAD_DIM),
          w_query, w_key, w_value, w_out, w_gate, w_up, w_down, *gains, cos2, sin2)
        bc = 8
        big = pl.BlockSpec((1, bc, SEQ, HL, HEAD_DIM), lambda l, c, s: (l, c, 0, 0, 0))
        small = pl.BlockSpec((1, bc, T, HL, HEAD_DIM), lambda l, c, s: (l, c, 0, 0, 0))
        k_out, v_out = pl.pallas_call(
            cache_kernel,
            out_shape=[jax.ShapeDtypeStruct(k_cache.shape, BF)] * 2,
            grid_spec=pltpu.PrefetchScalarGridSpec(
                num_scalar_prefetch=1, grid=(L, rows // bc), in_specs=[big, big, small, small], out_specs=[big, big]),
            name="caches",
        )(start_local, k_cache, v_cache, kn.reshape(L, rows, T, HL, HEAD_DIM), vn.reshape(L, rows, T, HL, HEAD_DIM))
        return y, k_out, v_out

    return jax.shard_map(device_fn, mesh=mesh, in_specs=(act_spec, P('dp'), cache_spec, cache_spec, col_spec, col_spec, col_spec, row_spec, col_spec, col_spec, row_spec, head_gain, head_gain, width_gain, width_gain), out_specs=(act_spec, cache_spec, cache_spec), check_vma=False)
```

```python
import functools
import math
import jax
import jax.numpy as jnp
from jax import lax
from jax.experimental import pallas as pl
from jax.experimental.pallas import tpu as pltpu
from jax.sharding import PartitionSpec as P

HEAD_DIM = 128
EPS = 1e-6
THETA = 500000.0
SCORE_SCALE = 1.0 / math.sqrt(HEAD_DIM)
NEG_BIG = -1e30
MESH = pl.DeviceIdType.MESH
BF = jnp.bfloat16
F32 = jnp.float32

L = 2
T = 3
NB = 2
RB = 32
R = T * RB
HL = 8
DW = 2048
QW = HL * HEAD_DIM
FW = 2752
FP = 2816
SEQ = 64
SH = SEQ * HL
CB = 4
NCH = RB // CB
TW = 512
HALF = DW // 2
GU_TILES = [(0, 512), (512, 512), (1024, 512), (1536, 512), (2048, 512), (2560, 256)]
QKV_TILES = [(0, 0), (0, 512), (0, 1024), (0, 1536), (1, 0), (1, 512)]


def dot(a, b):
    return jnp.dot(a, b, preferred_element_type=F32)


def dot_t(a, b):
    return lax.dot_general(a, b, (((1,), (1,)), ((), ())), preferred_element_type=F32)


def main_kernel(start_ref, emb_ref, kc_ref, vc_ref, wq_ref, wk_ref, wv_ref, wo_ref, wg_ref, wu_ref, wd_ref,
                qg_ref, kg_ref, ag_ref, mg_ref, cos_ref, sin_ref,
                y_ref, kn_ref, vn_ref,
                X, W1, WO, WD, GP, GR, C, OB, QS, KS, VS, OS, KO, VO, KB, VB, XP, XC, XS, XR, AF, RSUM, RSC, ST, SR,
                in_sem, q_wsem, g_wsem, o_wsem, d_wsem, kv_sem, ko_sem, y_sem,
                g_ss, g_rs, c_ss, c_rs, o_ss, o_rs, p_ss, p_rs, x_ss, x_rs, a_ss, a_rs, st_ss, st_rs):
    ty = lax.axis_index("tpy")
    tx = lax.axis_index("tpx")
    core = lax.rem(tx, 2)
    oy = 1 - ty
    cx = tx + 1 - 2 * core
    xx = lax.rem(tx + 2, 4)
    dx = 3 - tx
    ypeer = {"tpy": oy}
    cpeer = {"tpx": cx}
    xpeer = {"tpx": xx}
    xdiag = {"tpx": dx}
    ydiag = {"tpy": oy, "tpx": cx}
    own_half = pl.ds(pl.multiple_of(core * HALF, HALF), HALF)
    oth_half = pl.ds(pl.multiple_of((1 - core) * HALF, HALF), HALF)

    def rc(src, dst, ss, rs, dev):
        return pltpu.make_async_remote_copy(src_ref=src, dst_ref=dst, send_sem=ss, recv_sem=rs, device_id=dev, device_id_type=MESH)

    def lc(src, dst, sem):
        return pltpu.make_async_copy(src, dst, sem)

    def emb_copies():
        out = []
        for m in range(NB):
            for y in range(2):
                for t in range(T):
                    out.append(lc(emb_ref.at[t, pl.ds(y * NB * RB + m * RB, RB)], X.at[m, y, pl.ds(t * RB, RB)], in_sem.at[(m * 2 + y) * T + t]))
        return out

    def qkv_load(l, n):
        j, c0 = QKV_TILES[n]
        src = (wq_ref, wk_ref, wv_ref)[n // 2]
        return lc(src.at[l, :, pl.ds((n % 2) * TW, TW)], W1.at[j, pl.ds(0, DW), pl.ds(c0, TW)], q_wsem.at[n])

    def qkv_loads(l):
        return [qkv_load(l, n) for n in range(6)]

    def gu_loads(l):
        return [lc((wg_ref, wu_ref)[j].at[l, pl.ds(r * 688, 688)], W1.at[j, pl.ds(r * 688, 688)], g_wsem.at[j * 4 + r]) for r in range(4) for j in range(2)]

    def wo_loads(l):
        return [lc(wo_ref.at[l], WO, o_wsem.at[0])]

    def wd_loads(l):
        return [lc(wd_ref.at[l, pl.ds(r * 688, 688)], WD.at[pl.ds(r * 688, 688)], d_wsem.at[r]) for r in range(4)]

    def start(copies):
        for cp in copies:
            cp.start()

    def wait(copies):
        for cp in copies:
            cp.wait()

    def kv_copies(l, m, c, slot):
        rows = pl.ds(m * RB + c * CB, CB)
        return [lc(kc_ref.at[l, rows], KB.at[slot], kv_sem.at[0, slot]), lc(vc_ref.at[l, rows], VB.at[slot], kv_sem.at[1, slot])]

    start(emb_copies())
    start(qkv_loads(0))

    barrier = pltpu.get_barrier_semaphore()
    for dev in (ypeer, cpeer, xpeer, xdiag, ydiag):
        pl.semaphore_signal(barrier, inc=1, device_id=dev, device_id_type=MESH)
    pl.semaphore_wait(barrier, 5)

    start(kv_copies(0, 0, 0, 0))
    start(kv_copies(0, 0, 1, 1))
    start(wo_loads(0))
    start(wd_loads(0))

    def tile_copy(m, j, n, c0, w):
        return rc(GP.at[m, j, oy, :, pl.ds(c0, w)], GR.at[m, j, :, pl.ds(c0, w)], g_ss.at[m, j, n], g_rs.at[m, j, n], ypeer)

    def compute_tile(m, j, c0, w, transposed=False):
        xm = X[m].reshape(2 * R, DW)
        if transposed:
            res = dot_t(xm, W1[j, pl.ds(c0, w), :]).astype(BF)
        else:
            res = dot(xm, W1[j, pl.ds(0, DW), pl.ds(c0, w)]).astype(BF)
        GP[m, j, :, :, pl.ds(c0, w)] = res.reshape(2, R, w)

    def phase_q(m, l, first):
        for j, cnt in ((0, 4), (1, 2)):
            if first:
                for i in range(cnt):
                    qkv_load(l, j * 4 + i).wait()
                    compute_tile(m, j, i * TW, TW)
                    tile_copy(m, j, i, i * TW, TW).start()
            else:
                def body(i, _):
                    c0 = pl.multiple_of(i * TW, TW)
                    compute_tile(m, j, c0, TW)
                    tile_copy(m, j, i, c0, TW).start()
                    return 0
                lax.fori_loop(0, cnt, body, 0)

    def phase_g(m, l, send):
        def body(i, _):
            c0 = pl.multiple_of(i * TW, TW)
            for j in range(2):
                compute_tile(m, j, c0, TW, True)
                if send:
                    tile_copy(m, j, i, c0, TW).start()
            return 0
        lax.fori_loop(0, 5, body, 0)
        for j in range(2):
            compute_tile(m, j, 2560, 192, True)
            if send:
                tile_copy(m, j, 5, 2560, 256).start()

    def send_g(m):
        for n, (c0, w) in enumerate(GU_TILES):
            for j in range(2):
                tile_copy(m, j, n, c0, w).start()

    def stat_copies(kind, m):
        peers = (cpeer, xpeer, xdiag) if kind == 0 else (cpeer, ypeer, ydiag)
        return [rc(ST.at[kind, m], SR.at[kind, m, k], st_ss.at[kind, m, k], st_rs.at[kind, m, k], peers[k]) for k in range(3)]

    def stat_send(kind, m):
        v0 = jnp.sum(RSUM[0], axis=1, keepdims=True)
        v1 = jnp.sum(RSUM[1], axis=1, keepdims=True)
        lane = lax.broadcasted_iota(jnp.int32, (R, 128), 1)
        both = jnp.where(lane == 0, v0, v1)
        full = jnp.concatenate([both, jnp.zeros((128 - R, 128), F32)], axis=0)
        ST[kind, m] = full.T[0:8]
        start(stat_copies(kind, m))

    def stat_recv(kind, m):
        wait(stat_copies(kind, m))
        total = (ST[kind, m] + SR[kind, m, 0]) + (SR[kind, m, 1] + SR[kind, m, 2])
        back = jnp.concatenate([total] * 16, axis=0).T
        scale = lax.rsqrt(back / 4096.0 + EPS)
        RSC[0] = jnp.broadcast_to(scale[0:R, 0:1], (R, 128))
        RSC[1] = jnp.broadcast_to(scale[0:R, 1:2], (R, 128))

    def phase_s(m):
        for n, (j, c0) in enumerate(QKV_TILES):
            tile_copy(m, j, c0 // TW, c0, TW).wait()

        def body(i, _):
            rows = pl.ds(pl.multiple_of(i * 16, 16), 16)
            for j in range(2):
                acc = jnp.zeros((16, 128), F32)
                for h in range(8):
                    cols = pl.ds((j * 8 + h) * 128, 128)
                    z = (GP[m, 0, ty, rows, cols].astype(F32) + GR[m, 0, rows, cols].astype(F32)).astype(BF)
                    GR[m, 0, rows, cols] = z
                    zf = z.astype(F32)
                    acc = acc + zf * zf
                RSUM[j, rows] = acc
            for h in range(8):
                cols = pl.ds(h * 128, 128)
                GR[m, 1, rows, cols] = (GP[m, 1, ty, rows, cols].astype(F32) + GR[m, 1, rows, cols].astype(F32)).astype(BF)
            return 0
        lax.fori_loop(0, R // 16, body, 0)
        stat_send(0, m)

    def phase_t1(m, l):
        stat_recv(0, m)

        def body(i, _):
            rows = pl.ds(pl.multiple_of(i * 16, 16), 16)
            t = i // 2
            dst = pl.ds(pl.multiple_of(lax.rem(i, 2) * 16, 16), 16)
            cosv = cos_ref[m, rows]
            sinv = sin_ref[m, rows]
            for j, (out, gain) in enumerate(((QS, qg_ref), (KS, kg_ref))):
                scale = RSC[j, rows]
                for h in range(8):
                    z = GR[m, 0, rows, pl.ds((j * 8 + h) * 128, 128)].astype(F32)
                    z = z * scale * gain[pl.ds(l, 1), pl.ds(h * 128, 128)].astype(F32)
                    rot = z * cosv + pltpu.roll(z, 64, 1) * sinv
                    out[t, dst, h, :] = rot.astype(BF).astype(F32)
            for h in range(8):
                VS[t, dst, h, :] = GR[m, 1, rows, pl.ds(h * 128, 128)].astype(F32)
            return 0
        lax.fori_loop(0, R // 16, body, 0)

    def ko_copies(l, m):
        rows = pl.ds(m * RB, RB)
        return [lc(KO.at[m], kn_ref.at[l, rows], ko_sem.at[0, m]), lc(VO.at[m], vn_ref.at[l, rows], ko_sem.at[1, m])]

    def o_copy(m):
        return rc(OB.at[m, ty], OB.at[m, ty], o_ss.at[m], o_rs.at[m], ypeer)

    def phase_t2(m, l):
        if l > 0:
            wait(ko_copies(l - 1, m))
        row = lax.broadcasted_iota(jnp.int32, (T * HL, SH), 0)
        col = lax.broadcasted_iota(jnp.int32, (T * HL, SH), 1)
        colm = jnp.where(lax.rem(row, HL) == lax.rem(col, HL), col, SH)
        rown = lax.broadcasted_iota(jnp.int32, (T * HL, T * HL), 0)
        coln = lax.broadcasted_iota(jnp.int32, (T * HL, T * HL), 1)
        newm = (lax.rem(rown, HL) == lax.rem(coln, HL)) & (coln <= rown)

        def chunk(c, _):
            slot = lax.rem(c, 2)
            wait(kv_copies(l, m, c, slot))
            for k in range(CB):
                i = c * CB + k
                q = QS[:, i].reshape(T * HL, HEAD_DIM).astype(BF)
                kn = KS[:, i].reshape(T * HL, HEAD_DIM).astype(BF)
                vn = VS[:, i].reshape(T * HL, HEAD_DIM).astype(BF)
                limit = start_ref[m * RB + i] * HL
                s_old = jnp.where(colm < limit, dot_t(q, KB[slot, k]) * SCORE_SCALE, NEG_BIG)
                s_new = jnp.where(newm, dot_t(q, kn) * SCORE_SCALE, NEG_BIG)
                top = jnp.maximum(jnp.max(s_old, axis=1, keepdims=True), jnp.max(s_new, axis=1, keepdims=True))
                e_old = jnp.exp(s_old - top)
                e_new = jnp.exp(s_new - top)
                den = jnp.sum(e_old, axis=1, keepdims=True) + jnp.sum(e_new, axis=1, keepdims=True)
                o = dot((e_old / den).astype(BF), VB[slot, k]) + dot((e_new / den).astype(BF), vn)
                OS[:, i] = o.reshape(T, HL, HEAD_DIM)
                KO[m, i] = kn
                VO[m, i] = vn

            @pl.when(c < NCH - 2)
            def _():
                start(kv_copies(l, m, c + 2, slot))
            return 0
        lax.fori_loop(0, NCH, chunk, 0)
        start(ko_copies(l, m))
        nxt = (l, m + 1) if m + 1 < NB else (l + 1, 0)
        if nxt[0] < L:
            start(kv_copies(nxt[0], nxt[1], 0, 0))
            start(kv_copies(nxt[0], nxt[1], 1, 1))

        def body(i, _):
            rows = pl.ds(pl.multiple_of(i * 16, 16), 16)
            t = i // 2
            src = pl.ds(pl.multiple_of(lax.rem(i, 2) * 16, 16), 16)
            for h in range(8):
                OB[m, ty, rows, pl.ds(h * 128, 128)] = OS[t, src, h, :].astype(BF)
            return 0
        lax.fori_loop(0, R // 16, body, 0)
        o_copy(m).start()

    def p_copy(m):
        return rc(XP.at[m, :, oth_half], XC.at[m], p_ss.at[m], p_rs.at[m], cpeer)

    def x_copy(ph, m):
        return rc(XS.at[m], XR.at[ph, m], x_ss.at[m], x_rs.at[ph, m], xpeer)

    def a_copy(m):
        return rc(AF.at[m, :, own_half], AF.at[m, :, own_half], a_ss.at[m], a_rs.at[m], cpeer)

    def phase_o(m, l):
        o_copy(m).wait()
        for half in (1 - core, core):
            def body(i, _):
                cols = pl.ds(pl.multiple_of(half * HALF + i * TW, TW), TW)
                XP[m, :, cols] = dot(OB[m].reshape(2 * R, QW), WO[:, cols]).astype(BF)
                return 0
            lax.fori_loop(0, 2, body, 0)
            if half is not core:
                p_copy(m).start()

    def phase_d(m, l):
        for n, (c0, w) in enumerate(GU_TILES):
            c_copy(m, n, c0, w).wait()
        for half in (1 - core, core):
            def body(i, _):
                cols = pl.ds(pl.multiple_of(half * HALF + i * TW, TW), TW)
                cm = C[m].reshape(2 * R, FP)
                XP[m, :, cols] = dot(cm[:, :FW], WD[:, cols]).astype(BF)
                return 0
            lax.fori_loop(0, 2, body, 0)
            if half is not core:
                p_copy(m).start()

    def phase_2(ph, m):
        p_copy(m).wait()

        def body(i, _):
            rows = pl.ds(pl.multiple_of(i * 16, 16), 16)
            XS[m, rows] = (XP[m, rows, own_half].astype(F32) + XC[m, rows].astype(F32)).astype(BF)
            return 0
        lax.fori_loop(0, 2 * R // 16, body, 0)
        x_copy(ph, m).start()

    def phase_3(ph, m):
        x_copy(ph, m).wait()

        def body(i, _):
            rows = pl.ds(pl.multiple_of(i * 16, 16), 16)
            z = (XS[m, rows].astype(F32) + XR[ph, m, rows].astype(F32)).astype(BF)
            AF[m, rows, own_half] = z
            zf = z.astype(F32)
            sq = zf * zf
            acc = sq[:, 0:128]
            for h in range(1, 8):
                acc = acc + sq[:, h * 128:(h + 1) * 128]
            RSUM[i // 6, pl.ds(pl.multiple_of(lax.rem(i, 6) * 16, 16), 16)] = acc
            return 0
        lax.fori_loop(0, 2 * R // 16, body, 0)
        a_copy(m).start()
        stat_send(1 + ph, m)

    def phase_h(ph, m, l):
        gain = (ag_ref, mg_ref)[ph]
        stat_recv(1 + ph, m)
        a_copy(m).wait()

        def body(i, _):
            y = i // 6
            rows = pl.ds(pl.multiple_of(lax.rem(i, 6) * 16, 16), 16)
            arow = pl.ds(pl.multiple_of(i * 16, 16), 16)
            scale = RSC[y, rows]
            for h in range(16):
                cols = pl.ds(h * 128, 128)
                X[m, y, rows, cols] = (X[m, y, rows, cols].astype(F32) + AF[m, arow, cols].astype(F32) * scale * gain[pl.ds(l, 1), cols].astype(F32)).astype(BF)
            return 0
        lax.fori_loop(0, 2 * R // 16, body, 0)

    def c_copy(m, n, c0, w):
        return rc(C.at[m, ty, :, pl.ds(c0, w)], C.at[m, ty, :, pl.ds(c0, w)], c_ss.at[m, n], c_rs.at[m, n], ypeer)

    def phase_c(m, lo, hi):
        for n in range(lo, hi):
            c0, w = GU_TILES[n]
            for j in range(2):
                tile_copy(m, j, n, c0, w).wait()

            def body(i, _):
                rows = pl.ds(pl.multiple_of(i * 16, 16), 16)
                cols = pl.ds(c0, w)
                g = (GP[m, 0, ty, rows, cols].astype(F32) + GR[m, 0, rows, cols].astype(F32)).astype(BF).astype(F32)
                u = (GP[m, 1, ty, rows, cols].astype(F32) + GR[m, 1, rows, cols].astype(F32)).astype(BF).astype(F32)
                C[m, ty, rows, cols] = (jax.nn.silu(g) * u).astype(BF)
                return 0
            lax.fori_loop(0, R // 16, body, 0)
            c_copy(m, n, c0, w).start()

    def y_copies(m):
        out = []
        for y in range(2):
            for t in range(T):
                out.append(lc(X.at[m, y, pl.ds(t * RB, RB)], y_ref.at[t, pl.ds(y * NB * RB + m * RB, RB)], y_sem.at[(m * 2 + y) * T + t]))
        return out

    A, B = 0, 1
    wait(emb_copies())
    phase_q(A, 0, True)
    phase_q(B, 0, False)
    for l in range(L):
        start(gu_loads(l))
        phase_s(A)
        phase_t1(A, l)
        phase_t2(A, l)
        phase_s(B)
        phase_t1(B, l)
        wait(wo_loads(l))
        phase_o(A, l)
        phase_2(0, A)
        phase_t2(B, l)
        phase_3(0, A)
        phase_o(B, l)
        phase_h(0, A, l)
        phase_2(0, B)
        if l + 1 < L:
            start(wo_loads(l + 1))
        wait(gu_loads(l))
        phase_g(A, l, True)
        phase_3(0, B)
        phase_h(0, B, l)
        phase_g(B, l, False)
        if l + 1 < L:
            start(qkv_loads(l + 1))
        phase_c(A, 0, 6)
        send_g(B)
        wait(wd_loads(l))
        phase_d(A, l)
        phase_2(1, A)
        phase_c(B, 0, 3)
        phase_3(1, A)
        phase_h(1, A, l)
        phase_c(B, 3, 6)
        if l + 1 < L:
            phase_q(A, l + 1, True)
        else:
            start(y_copies(A))
        phase_d(B, l)
        if l + 1 < L:
            start(wd_loads(l + 1))
        phase_2(1, B)
        phase_3(1, B)
        phase_h(1, B, l)
        if l + 1 < L:
            phase_q(B, l + 1, False)
        else:
            start(y_copies(B))
    wait(y_copies(A))
    wait(y_copies(B))
    for m in range(NB):
        wait(ko_copies(L - 1, m))


def cache_kernel(start_ref, k_ref, v_ref, kn_ref, vn_ref, ko_ref, vo_ref):
    c = pl.program_id(1)
    ko_ref[...] = k_ref[...]
    vo_ref[...] = v_ref[...]
    for i in range(k_ref.shape[1]):
        p = start_ref[c * k_ref.shape[1] + i]
        for t in range(T):
            ko_ref[0, i, p + t] = kn_ref[0, i, t]
            vo_ref[0, i, p + t] = vn_ref[0, i, t]


def solution(mesh):
    act_spec = P(None, 'dp', 'tpy')
    cache_spec = P(None, ('dp', 'tpy'), None, 'tpx', None)
    col_spec = P(None, 'tpy', 'tpx')
    row_spec = P(None, 'tpx', 'tpy')
    head_gain = P(None, 'tpx')
    width_gain = P(None, 'tpy')

    def device_fn(embeds, start_pos, k_cache, v_cache, w_query, w_key, w_value, w_out, w_gate, w_up, w_down, q_gain, k_gain, attn_gain, mlp_gain):
        rows = NB * RB
        start_local = lax.dynamic_slice_in_dim(start_pos, lax.axis_index('tpy') * rows, rows)
        pos = (start_local.reshape(NB, 1, RB) + jnp.arange(T, dtype=jnp.int32)[None, :, None]).reshape(NB, R)
        inv_freq = jnp.power(THETA, jnp.arange(HEAD_DIM // 2, dtype=F32) * (-2.0 / HEAD_DIM))
        ang = pos.astype(F32)[..., None] * inv_freq
        cos_part, sin_part = jnp.cos(ang), jnp.sin(ang)
        cos2 = jnp.concatenate([cos_part, cos_part], axis=-1)
        sin2 = jnp.concatenate([-sin_part, sin_part], axis=-1)
        hbm = pl.BlockSpec(memory_space=pl.ANY)
        vm = pl.BlockSpec(memory_space=pltpu.VMEM)
        dma = pltpu.SemaphoreType.DMA
        y, kn, vn = pl.pallas_call(
            main_kernel,
            out_shape=[
                jax.ShapeDtypeStruct(embeds.shape, BF),
                jax.ShapeDtypeStruct((L, rows, T * HL, HEAD_DIM), BF),
                jax.ShapeDtypeStruct((L, rows, T * HL, HEAD_DIM), BF),
            ],
            in_specs=[pl.BlockSpec(memory_space=pltpu.SMEM)] + [hbm] * 10 + [vm] * 6,
            out_specs=[hbm] * 3,
            scratch_shapes=[
                pltpu.VMEM((NB, 2, R, DW), BF),
                pltpu.VMEM((2, FW, DW), BF),
                pltpu.VMEM((QW, DW), BF),
                pltpu.VMEM((FW, DW), BF),
                pltpu.VMEM((NB, 2, 2, R, FP), BF),
                pltpu.VMEM((NB, 2, R, FP), BF),
                pltpu.VMEM((NB, 2, R, FP), BF),
                pltpu.VMEM((NB, 2, R, QW), BF),
                pltpu.VMEM((T, RB, HL, HEAD_DIM), F32),
                pltpu.VMEM((T, RB, HL, HEAD_DIM), F32),
                pltpu.VMEM((T, RB, HL, HEAD_DIM), F32),
                pltpu.VMEM((T, RB, HL, HEAD_DIM), F32),
                pltpu.VMEM((NB, RB, T * HL, HEAD_DIM), BF),
                pltpu.VMEM((NB, RB, T * HL, HEAD_DIM), BF),
                pltpu.VMEM((2, CB, SH, HEAD_DIM), BF),
                pltpu.VMEM((2, CB, SH, HEAD_DIM), BF),
                pltpu.VMEM((NB, 2 * R, DW), BF),
                pltpu.VMEM((NB, 2 * R, HALF), BF),
                pltpu.VMEM((NB, 2 * R, HALF), BF),
                pltpu.VMEM((2, NB, 2 * R, HALF), BF),
                pltpu.VMEM((NB, 2 * R, DW), BF),
                pltpu.VMEM((2, R, 128), F32),
                pltpu.VMEM((2, R, 128), F32),
                pltpu.VMEM((3, NB, 8, 128), F32),
                pltpu.VMEM((3, NB, 3, 8, 128), F32),
                dma((NB * 2 * T,)), dma((6,)), dma((8,)), dma((1,)), dma((4,)), dma((2, 2)), dma((2, NB)), dma((NB * 2 * T,)),
                dma((NB, 2, 6)), dma((NB, 2, 6)), dma((NB, 6)), dma((NB, 6)), dma((NB,)), dma((NB,)),
                dma((NB,)), dma((NB,)), dma((NB,)), dma((2, NB)), dma((NB,)), dma((NB,)), dma((3, NB, 3)), dma((3, NB, 3)),
            ],
            compiler_params=pltpu.CompilerParams(collective_id=0, has_side_effects=True, vmem_limit_bytes=67043328),
            name="layers",
        )(start_local, embeds, k_cache.reshape(L, rows, SH, HEAD_DIM), v_cache.reshape(L, rows, SH, HEAD_DIM),
          w_query, w_key, w_value, w_out, w_gate.transpose(0, 2, 1), w_up.transpose(0, 2, 1), w_down, q_gain, k_gain, attn_gain, mlp_gain, cos2, sin2)
        bc = 8
        big = pl.BlockSpec((1, bc, SEQ, HL, HEAD_DIM), lambda l, c, s: (l, c, 0, 0, 0))
        small = pl.BlockSpec((1, bc, T, HL, HEAD_DIM), lambda l, c, s: (l, c, 0, 0, 0))
        k_out, v_out = pl.pallas_call(
            cache_kernel,
            out_shape=[jax.ShapeDtypeStruct(k_cache.shape, BF)] * 2,
            grid_spec=pltpu.PrefetchScalarGridSpec(
                num_scalar_prefetch=1, grid=(L, rows // bc), in_specs=[big, big, small, small], out_specs=[big, big]),
            name="caches",
        )(start_local, k_cache, v_cache, kn.reshape(L, rows, T, HL, HEAD_DIM), vn.reshape(L, rows, T, HL, HEAD_DIM))
        return y, k_out, v_out

    return jax.shard_map(device_fn, mesh=mesh, in_specs=(act_spec, P('dp'), cache_spec, cache_spec, col_spec, col_spec, col_spec, row_spec, col_spec, col_spec, row_spec, head_gain, head_gain, width_gain, width_gain), out_specs=(act_spec, cache_spec, cache_spec), check_vma=False)
```

```python
import functools
import math
import jax
import jax.numpy as jnp
from jax import lax
from jax.experimental import pallas as pl
from jax.experimental.pallas import tpu as pltpu
from jax.sharding import PartitionSpec as P

HEAD_DIM = 128
EPS = 1e-6
THETA = 500000.0
SCORE_SCALE = 1.0 / math.sqrt(HEAD_DIM)
NEG_BIG = -1e30
MESH = pl.DeviceIdType.MESH
BF = jnp.bfloat16
F32 = jnp.float32

L = 2
T = 3
NB = 2
RB = 32
R = T * RB
HL = 8
DW = 2048
QW = HL * HEAD_DIM
FW = 2752
FP = 2816
SEQ = 64
SH = SEQ * HL
CB = 4
NCH = RB // CB
TW = 512
HALF = DW // 2
GU_TILES = [(0, 512), (512, 512), (1024, 512), (1536, 512), (2048, 512), (2560, 256)]
QKV_TILES = [(0, 0), (0, 512), (0, 1024), (0, 1536), (1, 0), (1, 512)]


def dot(a, b):
    return jnp.dot(a, b, preferred_element_type=F32)


def dot_t(a, b):
    return lax.dot_general(a, b, (((1,), (1,)), ((), ())), preferred_element_type=F32)


def main_kernel(start_ref, emb_ref, kc_ref, vc_ref, wq_ref, wk_ref, wv_ref, wo_ref, wg_ref, wu_ref, wd_ref,
                qg_ref, kg_ref, ag_ref, mg_ref, cos_ref, sin_ref,
                y_ref, kn_ref, vn_ref,
                X, W1, WO, WD, GP, GR, C, OB, QS, KS, VS, OS, KO, VO, KB, VB, XP, XC, XS, XR, AF, RSUM, RSC, ST, SR,
                in_sem, q_wsem, g_wsem, o_wsem, d_wsem, kv_sem, ko_sem, y_sem,
                g_ss, g_rs, c_ss, c_rs, o_ss, o_rs, p_ss, p_rs, x_ss, x_rs, a_ss, a_rs, st_ss, st_rs):
    ty = lax.axis_index("tpy")
    tx = lax.axis_index("tpx")
    core = lax.rem(tx, 2)
    oy = 1 - ty
    cx = tx + 1 - 2 * core
    xx = lax.rem(tx + 2, 4)
    dx = 3 - tx
    ypeer = {"tpy": oy}
    cpeer = {"tpx": cx}
    xpeer = {"tpx": xx}
    xdiag = {"tpx": dx}
    ydiag = {"tpy": oy, "tpx": cx}
    own_half = pl.ds(pl.multiple_of(core * HALF, HALF), HALF)
    oth_half = pl.ds(pl.multiple_of((1 - core) * HALF, HALF), HALF)

    def rc(src, dst, ss, rs, dev):
        return pltpu.make_async_remote_copy(src_ref=src, dst_ref=dst, send_sem=ss, recv_sem=rs, device_id=dev, device_id_type=MESH)

    def lc(src, dst, sem):
        return pltpu.make_async_copy(src, dst, sem)

    def emb_copies():
        out = []
        for m in range(NB):
            for y in range(2):
                for t in range(T):
                    out.append(lc(emb_ref.at[t, pl.ds(y * NB * RB + m * RB, RB)], X.at[m, y, pl.ds(t * RB, RB)], in_sem.at[(m * 2 + y) * T + t]))
        return out

    def qkv_load(l, n):
        j, c0 = QKV_TILES[n]
        src = (wq_ref, wk_ref, wv_ref)[n // 2]
        return lc(src.at[l, :, pl.ds((n % 2) * TW, TW)], W1.at[j, pl.ds(0, DW), pl.ds(c0, TW)], q_wsem.at[n])

    def qkv_loads(l):
        return [qkv_load(l, n) for n in range(6)]

    def gu_loads(l):
        return [lc((wg_ref, wu_ref)[j].at[l, pl.ds(r * 688, 688)], W1.at[j, pl.ds(r * 688, 688)], g_wsem.at[j * 4 + r]) for r in range(4) for j in range(2)]

    def wo_loads(l):
        return [lc(wo_ref.at[l], WO, o_wsem.at[0])]

    def wd_loads(l):
        return [lc(wd_ref.at[l, pl.ds(r * 688, 688)], WD.at[pl.ds(r * 688, 688)], d_wsem.at[r]) for r in range(4)]

    def start(copies):
        for cp in copies:
            cp.start()

    def wait(copies):
        for cp in copies:
            cp.wait()

    def kv_copies(l, m, c, slot):
        rows = pl.ds(m * RB + c * CB, CB)
        return [lc(kc_ref.at[l, rows], KB.at[slot], kv_sem.at[0, slot]), lc(vc_ref.at[l, rows], VB.at[slot], kv_sem.at[1, slot])]

    start(emb_copies())
    start(qkv_loads(0))

    barrier = pltpu.get_barrier_semaphore()
    for dev in (ypeer, cpeer, xpeer, xdiag, ydiag):
        pl.semaphore_signal(barrier, inc=1, device_id=dev, device_id_type=MESH)
    pl.semaphore_wait(barrier, 5)

    start(kv_copies(0, 0, 0, 0))
    start(kv_copies(0, 0, 1, 1))
    start(wo_loads(0))
    start(wd_loads(0))

    def tile_copy(m, j, n, c0, w):
        return rc(GP.at[m, j, oy, :, pl.ds(c0, w)], GR.at[m, j, :, pl.ds(c0, w)], g_ss.at[m, j, n], g_rs.at[m, j, n], ypeer)

    def compute_tile(m, j, c0, w, transposed=False):
        xm = X[m].reshape(2 * R, DW)
        if transposed:
            res = dot_t(xm, W1[j, pl.ds(c0, w), :]).astype(BF)
        else:
            res = dot(xm, W1[j, pl.ds(0, DW), pl.ds(c0, w)]).astype(BF)
        GP[m, j, :, :, pl.ds(c0, w)] = res.reshape(2, R, w)

    def phase_q(m, l, first):
        for j, cnt in ((0, 4), (1, 2)):
            if first:
                for i in range(cnt):
                    qkv_load(l, j * 4 + i).wait()
                    compute_tile(m, j, i * TW, TW)
                    tile_copy(m, j, i, i * TW, TW).start()
            else:
                def body(i, _):
                    c0 = pl.multiple_of(i * TW, TW)
                    compute_tile(m, j, c0, TW)
                    tile_copy(m, j, i, c0, TW).start()
                    return 0
                lax.fori_loop(0, cnt, body, 0)

    def phase_g(m, l, send):
        def body(i, _):
            c0 = pl.multiple_of(i * TW, TW)
            for j in range(2):
                compute_tile(m, j, c0, TW, True)
                if send:
                    tile_copy(m, j, i, c0, TW).start()
            return 0
        lax.fori_loop(0, 5, body, 0)
        for j in range(2):
            compute_tile(m, j, 2560, 192, True)
            if send:
                tile_copy(m, j, 5, 2560, 256).start()

    def send_g(m):
        for n, (c0, w) in enumerate(GU_TILES):
            for j in range(2):
                tile_copy(m, j, n, c0, w).start()

    def stat_copies(kind, m):
        peers = (cpeer, xpeer, xdiag) if kind == 0 else (cpeer, ypeer, ydiag)
        return [rc(ST.at[kind, m], SR.at[kind, m, k], st_ss.at[kind, m, k], st_rs.at[kind, m, k], peers[k]) for k in range(3)]

    def stat_send(kind, m):
        v0 = jnp.sum(RSUM[0], axis=1, keepdims=True)
        v1 = jnp.sum(RSUM[1], axis=1, keepdims=True)
        lane = lax.broadcasted_iota(jnp.int32, (R, 128), 1)
        both = jnp.where(lane == 0, v0, v1)
        full = jnp.concatenate([both, jnp.zeros((128 - R, 128), F32)], axis=0)
        ST[kind, m] = full.T[0:8]
        start(stat_copies(kind, m))

    def stat_recv(kind, m):
        wait(stat_copies(kind, m))
        total = (ST[kind, m] + SR[kind, m, 0]) + (SR[kind, m, 1] + SR[kind, m, 2])
        back = jnp.concatenate([total] * 16, axis=0).T
        scale = lax.rsqrt(back / 4096.0 + EPS)
        RSC[0] = jnp.broadcast_to(scale[0:R, 0:1], (R, 128))
        RSC[1] = jnp.broadcast_to(scale[0:R, 1:2], (R, 128))

    def phase_s(m):
        for n, (j, c0) in enumerate(QKV_TILES):
            tile_copy(m, j, c0 // TW, c0, TW).wait()

        def body(i, _):
            rows = pl.ds(pl.multiple_of(i * 16, 16), 16)
            for j in range(2):
                acc = jnp.zeros((16, 128), F32)
                for h in range(8):
                    cols = pl.ds((j * 8 + h) * 128, 128)
                    z = (GP[m, 0, ty, rows, cols].astype(F32) + GR[m, 0, rows, cols].astype(F32)).astype(BF)
                    GR[m, 0, rows, cols] = z
                    zf = z.astype(F32)
                    acc = acc + zf * zf
                RSUM[j, rows] = acc
            for h in range(8):
                cols = pl.ds(h * 128, 128)
                GR[m, 1, rows, cols] = (GP[m, 1, ty, rows, cols].astype(F32) + GR[m, 1, rows, cols].astype(F32)).astype(BF)
            return 0
        lax.fori_loop(0, R // 16, body, 0)
        stat_send(0, m)

    def phase_t1(m, l):
        stat_recv(0, m)

        def body(i, _):
            rows = pl.ds(pl.multiple_of(i * 16, 16), 16)
            t = i // 2
            dst = pl.ds(pl.multiple_of(lax.rem(i, 2) * 16, 16), 16)
            cosv = cos_ref[m, rows]
            sinv = sin_ref[m, rows]
            for j, (out, gain) in enumerate(((QS, qg_ref), (KS, kg_ref))):
                scale = RSC[j, rows]
                for h in range(8):
                    z = GR[m, 0, rows, pl.ds((j * 8 + h) * 128, 128)].astype(F32)
                    z = z * scale * gain[pl.ds(l, 1), pl.ds(h * 128, 128)].astype(F32)
                    rot = z * cosv + pltpu.roll(z, 64, 1) * sinv
                    out[t, dst, h, :] = rot.astype(BF).astype(F32)
            for h in range(8):
                VS[t, dst, h, :] = GR[m, 1, rows, pl.ds(h * 128, 128)].astype(F32)
            return 0
        lax.fori_loop(0, R // 16, body, 0)

    def ko_copies(l, m):
        rows = pl.ds(m * RB, RB)
        return [lc(KO.at[m], kn_ref.at[l, rows], ko_sem.at[0, m]), lc(VO.at[m], vn_ref.at[l, rows], ko_sem.at[1, m])]

    def o_copy(m):
        return rc(OB.at[m, ty], OB.at[m, ty], o_ss.at[m], o_rs.at[m], ypeer)

    def phase_t2(m, l):
        if l > 0:
            wait(ko_copies(l - 1, m))
        row = lax.broadcasted_iota(jnp.int32, (T * HL, SH), 0)
        col = lax.broadcasted_iota(jnp.int32, (T * HL, SH), 1)
        colm = jnp.where(lax.rem(row, HL) == lax.rem(col, HL), col, SH)
        rown = lax.broadcasted_iota(jnp.int32, (T * HL, T * HL), 0)
        coln = lax.broadcasted_iota(jnp.int32, (T * HL, T * HL), 1)
        newm = (lax.rem(rown, HL) == lax.rem(coln, HL)) & (coln <= rown)

        def chunk(c, _):
            slot = lax.rem(c, 2)
            wait(kv_copies(l, m, c, slot))
            for k in range(CB):
                i = c * CB + k
                q = QS[:, i].reshape(T * HL, HEAD_DIM).astype(BF)
                kn = KS[:, i].reshape(T * HL, HEAD_DIM).astype(BF)
                vn = VS[:, i].reshape(T * HL, HEAD_DIM).astype(BF)
                limit = start_ref[m * RB + i] * HL
                s_old = jnp.where(colm < limit, dot_t(q, KB[slot, k]) * SCORE_SCALE, NEG_BIG)
                s_new = jnp.where(newm, dot_t(q, kn) * SCORE_SCALE, NEG_BIG)
                top = jnp.maximum(jnp.max(s_old, axis=1, keepdims=True), jnp.max(s_new, axis=1, keepdims=True))
                e_old = jnp.exp(s_old - top)
                e_new = jnp.exp(s_new - top)
                den = jnp.sum(e_old, axis=1, keepdims=True) + jnp.sum(e_new, axis=1, keepdims=True)
                o = dot((e_old / den).astype(BF), VB[slot, k]) + dot((e_new / den).astype(BF), vn)
                OS[:, i] = o.reshape(T, HL, HEAD_DIM)
                KO[m, i] = kn
                VO[m, i] = vn

            @pl.when(c < NCH - 2)
            def _():
                start(kv_copies(l, m, c + 2, slot))
            return 0
        lax.fori_loop(0, NCH, chunk, 0)
        start(ko_copies(l, m))
        nxt = (l, m + 1) if m + 1 < NB else (l + 1, 0)
        if nxt[0] < L:
            start(kv_copies(nxt[0], nxt[1], 0, 0))
            start(kv_copies(nxt[0], nxt[1], 1, 1))

        def body(i, _):
            rows = pl.ds(pl.multiple_of(i * 16, 16), 16)
            t = i // 2
            src = pl.ds(pl.multiple_of(lax.rem(i, 2) * 16, 16), 16)
            for h in range(8):
                OB[m, ty, rows, pl.ds(h * 128, 128)] = OS[t, src, h, :].astype(BF)
            return 0
        lax.fori_loop(0, R // 16, body, 0)
        o_copy(m).start()

    def p_copy(m):
        return rc(XP.at[m, :, oth_half], XC.at[m], p_ss.at[m], p_rs.at[m], cpeer)

    def x_copy(ph, m):
        return rc(XS.at[m], XR.at[ph, m], x_ss.at[m], x_rs.at[ph, m], xpeer)

    def a_copy(m):
        return rc(AF.at[m, :, own_half], AF.at[m, :, own_half], a_ss.at[m], a_rs.at[m], cpeer)

    def phase_o(m, l):
        o_copy(m).wait()
        for half in (1 - core, core):
            def body(i, _):
                cols = pl.ds(pl.multiple_of(half * HALF + i * TW, TW), TW)
                XP[m, :, cols] = dot(OB[m].reshape(2 * R, QW), WO[:, cols]).astype(BF)
                return 0
            lax.fori_loop(0, 2, body, 0)
            if half is not core:
                p_copy(m).start()

    def phase_d(m, l):
        for n, (c0, w) in enumerate(GU_TILES):
            c_copy(m, n, c0, w).wait()
        for half in (1 - core, core):
            def body(i, _):
                cols = pl.ds(pl.multiple_of(half * HALF + i * TW, TW), TW)
                cm = C[m].reshape(2 * R, FP)
                XP[m, :, cols] = dot(cm[:, :FW], WD[:, cols]).astype(BF)
                return 0
            lax.fori_loop(0, 2, body, 0)
            if half is not core:
                p_copy(m).start()

    def phase_2(ph, m):
        p_copy(m).wait()

        def body(i, _):
            rows = pl.ds(pl.multiple_of(i * 16, 16), 16)
            XS[m, rows] = (XP[m, rows, own_half].astype(F32) + XC[m, rows].astype(F32)).astype(BF)
            return 0
        lax.fori_loop(0, 2 * R // 16, body, 0)
        x_copy(ph, m).start()

    def phase_3(ph, m):
        x_copy(ph, m).wait()

        def body(i, _):
            rows = pl.ds(pl.multiple_of(i * 16, 16), 16)
            z = (XS[m, rows].astype(F32) + XR[ph, m, rows].astype(F32)).astype(BF)
            AF[m, rows, own_half] = z
            zf = z.astype(F32)
            sq = zf * zf
            acc = sq[:, 0:128]
            for h in range(1, 8):
                acc = acc + sq[:, h * 128:(h + 1) * 128]
            RSUM[i // 6, pl.ds(pl.multiple_of(lax.rem(i, 6) * 16, 16), 16)] = acc
            return 0
        lax.fori_loop(0, 2 * R // 16, body, 0)
        a_copy(m).start()
        stat_send(1 + ph, m)

    def phase_h(ph, m, l):
        gain = (ag_ref, mg_ref)[ph]
        stat_recv(1 + ph, m)
        a_copy(m).wait()

        def body(i, _):
            y = i // 6
            rows = pl.ds(pl.multiple_of(lax.rem(i, 6) * 16, 16), 16)
            arow = pl.ds(pl.multiple_of(i * 16, 16), 16)
            scale = RSC[y, rows]
            for h in range(16):
                cols = pl.ds(h * 128, 128)
                X[m, y, rows, cols] = (X[m, y, rows, cols].astype(F32) + AF[m, arow, cols].astype(F32) * scale * gain[pl.ds(l, 1), cols].astype(F32)).astype(BF)
            return 0
        lax.fori_loop(0, 2 * R // 16, body, 0)

    def c_copy(m, n, c0, w):
        return rc(C.at[m, ty, :, pl.ds(c0, w)], C.at[m, ty, :, pl.ds(c0, w)], c_ss.at[m, n], c_rs.at[m, n], ypeer)

    def phase_c(m, lo, hi):
        for n in range(lo, hi):
            c0, w = GU_TILES[n]
            for j in range(2):
                tile_copy(m, j, n, c0, w).wait()

            def body(i, _):
                rows = pl.ds(pl.multiple_of(i * 16, 16), 16)
                cols = pl.ds(c0, w)
                g = (GP[m, 0, ty, rows, cols].astype(F32) + GR[m, 0, rows, cols].astype(F32)).astype(BF).astype(F32)
                u = (GP[m, 1, ty, rows, cols].astype(F32) + GR[m, 1, rows, cols].astype(F32)).astype(BF).astype(F32)
                C[m, ty, rows, cols] = (jax.nn.silu(g) * u).astype(BF)
                return 0
            lax.fori_loop(0, R // 16, body, 0)
            c_copy(m, n, c0, w).start()

    def y_copies(m):
        out = []
        for y in range(2):
            for t in range(T):
                out.append(lc(X.at[m, y, pl.ds(t * RB, RB)], y_ref.at[t, pl.ds(y * NB * RB + m * RB, RB)], y_sem.at[(m * 2 + y) * T + t]))
        return out

    A, B = 0, 1
    wait(emb_copies())
    phase_q(A, 0, True)
    phase_q(B, 0, False)
    for l in range(L):
        start(gu_loads(l))
        phase_s(A)
        phase_t1(A, l)
        phase_t2(A, l)
        phase_s(B)
        phase_t1(B, l)
        wait(wo_loads(l))
        phase_o(A, l)
        phase_2(0, A)
        phase_t2(B, l)
        phase_3(0, A)
        phase_o(B, l)
        phase_h(0, A, l)
        phase_2(0, B)
        if l + 1 < L:
            start(wo_loads(l + 1))
        wait(gu_loads(l))
        phase_g(A, l, True)
        phase_3(0, B)
        phase_h(0, B, l)
        phase_g(B, l, False)
        if l + 1 < L:
            start(qkv_loads(l + 1))
        phase_c(A, 0, 6)
        send_g(B)
        wait(wd_loads(l))
        phase_d(A, l)
        phase_2(1, A)
        phase_c(B, 0, 3)
        phase_3(1, A)
        phase_h(1, A, l)
        phase_c(B, 3, 6)
        if l + 1 < L:
            phase_q(A, l + 1, True)
        else:
            start(y_copies(A))
        phase_d(B, l)
        if l + 1 < L:
            start(wd_loads(l + 1))
        phase_2(1, B)
        phase_3(1, B)
        phase_h(1, B, l)
        if l + 1 < L:
            phase_q(B, l + 1, False)
        else:
            start(y_copies(B))
    wait(y_copies(A))
    wait(y_copies(B))
    for m in range(NB):
        wait(ko_copies(L - 1, m))


def cache_kernel(start_ref, kn_ref, vn_ref, ki_ref, vi_ref, ko_ref, vo_ref, sem):
    def copies(l, i):
        p = start_ref[i]
        return [
            pltpu.make_async_copy(kn_ref.at[l, i], ko_ref.at[l, i, pl.ds(p, T)], sem.at[0]),
            pltpu.make_async_copy(vn_ref.at[l, i], vo_ref.at[l, i, pl.ds(p, T)], sem.at[1]),
        ]

    def go(l, i):
        for cp in copies(l, i):
            cp.start()

    def done(l, i):
        for cp in copies(l, i):
            cp.wait()

    for l in range(L):
        lax.fori_loop(0, NB * RB, lambda i, _: (go(l, i), 0)[1], 0)
    for l in range(L):
        lax.fori_loop(0, NB * RB, lambda i, _: (done(l, i), 0)[1], 0)


def solution(mesh):
    act_spec = P(None, 'dp', 'tpy')
    cache_spec = P(None, ('dp', 'tpy'), None, 'tpx', None)
    col_spec = P(None, 'tpy', 'tpx')
    row_spec = P(None, 'tpx', 'tpy')
    head_gain = P(None, 'tpx')
    width_gain = P(None, 'tpy')

    def device_fn(embeds, start_pos, k_cache, v_cache, w_query, w_key, w_value, w_out, w_gate, w_up, w_down, q_gain, k_gain, attn_gain, mlp_gain):
        rows = NB * RB
        start_local = lax.dynamic_slice_in_dim(start_pos, lax.axis_index('tpy') * rows, rows)
        pos = (start_local.reshape(NB, 1, RB) + jnp.arange(T, dtype=jnp.int32)[None, :, None]).reshape(NB, R)
        inv_freq = jnp.power(THETA, jnp.arange(HEAD_DIM // 2, dtype=F32) * (-2.0 / HEAD_DIM))
        ang = pos.astype(F32)[..., None] * inv_freq
        cos_part, sin_part = jnp.cos(ang), jnp.sin(ang)
        cos2 = jnp.concatenate([cos_part, cos_part], axis=-1)
        sin2 = jnp.concatenate([-sin_part, sin_part], axis=-1)
        hbm = pl.BlockSpec(memory_space=pl.ANY)
        vm = pl.BlockSpec(memory_space=pltpu.VMEM)
        dma = pltpu.SemaphoreType.DMA
        same = [(0, 0), (1, 1)]
        k_copy = lax.ppermute(k_cache, 'tpy', same)
        v_copy = lax.ppermute(v_cache, 'tpy', same)
        y, kn, vn = pl.pallas_call(
            main_kernel,
            out_shape=[
                jax.ShapeDtypeStruct(embeds.shape, BF),
                jax.ShapeDtypeStruct((L, rows, T * HL, HEAD_DIM), BF),
                jax.ShapeDtypeStruct((L, rows, T * HL, HEAD_DIM), BF),
            ],
            in_specs=[pl.BlockSpec(memory_space=pltpu.SMEM)] + [hbm] * 10 + [vm] * 6,
            out_specs=[hbm] * 3,
            scratch_shapes=[
                pltpu.VMEM((NB, 2, R, DW), BF),
                pltpu.VMEM((2, FW, DW), BF),
                pltpu.VMEM((QW, DW), BF),
                pltpu.VMEM((FW, DW), BF),
                pltpu.VMEM((NB, 2, 2, R, FP), BF),
                pltpu.VMEM((NB, 2, R, FP), BF),
                pltpu.VMEM((NB, 2, R, FP), BF),
                pltpu.VMEM((NB, 2, R, QW), BF),
                pltpu.VMEM((T, RB, HL, HEAD_DIM), F32),
                pltpu.VMEM((T, RB, HL, HEAD_DIM), F32),
                pltpu.VMEM((T, RB, HL, HEAD_DIM), F32),
                pltpu.VMEM((T, RB, HL, HEAD_DIM), F32),
                pltpu.VMEM((NB, RB, T * HL, HEAD_DIM), BF),
                pltpu.VMEM((NB, RB, T * HL, HEAD_DIM), BF),
                pltpu.VMEM((2, CB, SH, HEAD_DIM), BF),
                pltpu.VMEM((2, CB, SH, HEAD_DIM), BF),
                pltpu.VMEM((NB, 2 * R, DW), BF),
                pltpu.VMEM((NB, 2 * R, HALF), BF),
                pltpu.VMEM((NB, 2 * R, HALF), BF),
                pltpu.VMEM((2, NB, 2 * R, HALF), BF),
                pltpu.VMEM((NB, 2 * R, DW), BF),
                pltpu.VMEM((2, R, 128), F32),
                pltpu.VMEM((2, R, 128), F32),
                pltpu.VMEM((3, NB, 8, 128), F32),
                pltpu.VMEM((3, NB, 3, 8, 128), F32),
                dma((NB * 2 * T,)), dma((6,)), dma((8,)), dma((1,)), dma((4,)), dma((2, 2)), dma((2, NB)), dma((NB * 2 * T,)),
                dma((NB, 2, 6)), dma((NB, 2, 6)), dma((NB, 6)), dma((NB, 6)), dma((NB,)), dma((NB,)),
                dma((NB,)), dma((NB,)), dma((NB,)), dma((2, NB)), dma((NB,)), dma((NB,)), dma((3, NB, 3)), dma((3, NB, 3)),
            ],
            compiler_params=pltpu.CompilerParams(collective_id=0, has_side_effects=True, vmem_limit_bytes=67043328),
            name="layers",
        )(start_local, embeds, k_cache.reshape(L, rows, SH, HEAD_DIM), v_cache.reshape(L, rows, SH, HEAD_DIM),
          w_query, w_key, w_value, w_out, w_gate.transpose(0, 2, 1), w_up.transpose(0, 2, 1), w_down, q_gain, k_gain, attn_gain, mlp_gain, cos2, sin2)
        k_out, v_out = pl.pallas_call(
            cache_kernel,
            out_shape=[jax.ShapeDtypeStruct(k_cache.shape, BF)] * 2,
            in_specs=[pl.BlockSpec(memory_space=pltpu.SMEM), vm, vm, hbm, hbm],
            out_specs=[hbm, hbm],
            scratch_shapes=[dma((2,))],
            input_output_aliases={3: 0, 4: 1},
            name="caches",
        )(start_local, kn.reshape(L, rows, T, HL, HEAD_DIM), vn.reshape(L, rows, T, HL, HEAD_DIM), k_copy, v_copy)
        return y, k_out, v_out

    return jax.shard_map(device_fn, mesh=mesh, in_specs=(act_spec, P('dp'), cache_spec, cache_spec, col_spec, col_spec, col_spec, row_spec, col_spec, col_spec, row_spec, head_gain, head_gain, width_gain, width_gain), out_specs=(act_spec, cache_spec, cache_spec), check_vma=False)
```

```python
import functools
import math
import jax
import jax.numpy as jnp
from jax import lax
from jax.experimental import pallas as pl
from jax.experimental.pallas import tpu as pltpu
from jax.sharding import PartitionSpec as P

HEAD_DIM = 128
EPS = 1e-6
THETA = 500000.0
SCORE_SCALE = 1.0 / math.sqrt(HEAD_DIM)
NEG_BIG = -1e30
MESH = pl.DeviceIdType.MESH
BF = jnp.bfloat16
F32 = jnp.float32

L = 2
T = 3
NB = 2
RB = 32
R = T * RB
HL = 8
DW = 2048
QW = HL * HEAD_DIM
FW = 2752
FP = 2816
SEQ = 64
SH = SEQ * HL
CB = 4
NCH = RB // CB
SLOTS = 4
TW = 512
HALF = DW // 2
GU_TILES = [(0, 512), (512, 512), (1024, 512), (1536, 512), (2048, 512), (2560, 256)]
QKV_TILES = [(0, 0), (0, 512), (0, 1024), (0, 1536), (1, 0), (1, 512)]


def dot(a, b):
    return jnp.dot(a, b, preferred_element_type=F32)


def dot_t(a, b):
    return lax.dot_general(a, b, (((1,), (1,)), ((), ())), preferred_element_type=F32)


def main_kernel(start_ref, emb_ref, kc_ref, vc_ref, wq_ref, wk_ref, wv_ref, wo_ref, wg_ref, wu_ref, wd_ref,
                qg_ref, kg_ref, ag_ref, mg_ref, cos_ref, sin_ref,
                y_ref, kn_ref, vn_ref,
                X, W1, WO, WD, GP, GR, C, OB, QS, KS, VS, OS, KO, VO, KB, VB, XP, XC, XS, XR, AF, RSUM, RSC, ST, SR,
                in_sem, q_wsem, g_wsem, o_wsem, d_wsem, kv_sem, ko_sem, y_sem,
                g_ss, g_rs, c_ss, c_rs, o_ss, o_rs, p_ss, p_rs, x_ss, x_rs, a_ss, a_rs, st_ss, st_rs):
    ty = lax.axis_index("tpy")
    tx = lax.axis_index("tpx")
    core = lax.rem(tx, 2)
    oy = 1 - ty
    cx = tx + 1 - 2 * core
    xx = lax.rem(tx + 2, 4)
    dx = 3 - tx
    ypeer = {"tpy": oy}
    cpeer = {"tpx": cx}
    xpeer = {"tpx": xx}
    xdiag = {"tpx": dx}
    ydiag = {"tpy": oy, "tpx": cx}
    own_half = pl.ds(pl.multiple_of(core * HALF, HALF), HALF)
    oth_half = pl.ds(pl.multiple_of((1 - core) * HALF, HALF), HALF)

    def rc(src, dst, ss, rs, dev):
        return pltpu.make_async_remote_copy(src_ref=src, dst_ref=dst, send_sem=ss, recv_sem=rs, device_id=dev, device_id_type=MESH)

    def lc(src, dst, sem):
        return pltpu.make_async_copy(src, dst, sem)

    def emb_copies():
        out = []
        for m in range(NB):
            for y in range(2):
                for t in range(T):
                    out.append(lc(emb_ref.at[t, pl.ds(y * NB * RB + m * RB, RB)], X.at[m, y, pl.ds(t * RB, RB)], in_sem.at[(m * 2 + y) * T + t]))
        return out

    def qkv_load(l, n):
        j, c0 = QKV_TILES[n]
        src = (wq_ref, wk_ref, wv_ref)[n // 2]
        return lc(src.at[l, :, pl.ds((n % 2) * TW, TW)], W1.at[j, pl.ds(0, DW), pl.ds(c0, TW)], q_wsem.at[n])

    def qkv_loads(l):
        return [qkv_load(l, n) for n in range(6)]

    def gu_loads(l):
        return [lc((wg_ref, wu_ref)[j].at[l, pl.ds(r * 688, 688)], W1.at[j, pl.ds(r * 688, 688)], g_wsem.at[j * 4 + r]) for r in range(4) for j in range(2)]

    def wo_loads(l):
        return [lc(wo_ref.at[l], WO, o_wsem.at[0])]

    def wd_loads(l):
        return [lc(wd_ref.at[l, pl.ds(r * 688, 688)], WD.at[pl.ds(r * 688, 688)], d_wsem.at[r]) for r in range(4)]

    def start(copies):
        for cp in copies:
            cp.start()

    def wait(copies):
        for cp in copies:
            cp.wait()

    def kv_copies(l, m, c, slot):
        rows = pl.ds(m * RB + c * CB, CB)
        return [lc(kc_ref.at[l, rows], KB.at[slot], kv_sem.at[0, slot]), lc(vc_ref.at[l, rows], VB.at[slot], kv_sem.at[1, slot])]

    start(emb_copies())
    start(qkv_loads(0))

    barrier = pltpu.get_barrier_semaphore()
    for dev in (ypeer, cpeer, xpeer, xdiag, ydiag):
        pl.semaphore_signal(barrier, inc=1, device_id=dev, device_id_type=MESH)
    pl.semaphore_wait(barrier, 5)

    for c in range(SLOTS):
        start(kv_copies(0, 0, c, c))
    start(wo_loads(0))
    start(wd_loads(0))

    def tile_copy(m, j, n, c0, w):
        return rc(GP.at[m, j, oy, :, pl.ds(c0, w)], GR.at[m, j, :, pl.ds(c0, w)], g_ss.at[m, j, n], g_rs.at[m, j, n], ypeer)

    def compute_tile(m, j, c0, w, transposed=False):
        xm = X[m].reshape(2 * R, DW)
        if transposed:
            res = dot_t(xm, W1[j, pl.ds(c0, w), :]).astype(BF)
        else:
            res = dot(xm, W1[j, pl.ds(0, DW), pl.ds(c0, w)]).astype(BF)
        GP[m, j, :, :, pl.ds(c0, w)] = res.reshape(2, R, w)

    def phase_q(m, l, first):
        for j, cnt in ((0, 4), (1, 2)):
            if first:
                for i in range(cnt):
                    qkv_load(l, j * 4 + i).wait()
                    compute_tile(m, j, i * TW, TW)
                    tile_copy(m, j, i, i * TW, TW).start()
            else:
                def body(i, _):
                    c0 = pl.multiple_of(i * TW, TW)
                    compute_tile(m, j, c0, TW)
                    tile_copy(m, j, i, c0, TW).start()
                    return 0
                lax.fori_loop(0, cnt, body, 0)

    def phase_g(m, sent):
        def body(i, _):
            c0 = pl.multiple_of(i * TW, TW)
            for j in range(2):
                compute_tile(m, j, c0, TW, True)

                @pl.when(i < sent)
                def _():
                    tile_copy(m, j, i, c0, TW).start()
            return 0
        lax.fori_loop(0, 5, body, 0)
        for j in range(2):
            compute_tile(m, j, 2560, 192, True)

    def send_g(m, lo, hi):
        for n in range(lo, hi):
            c0, w = GU_TILES[n]
            for j in range(2):
                tile_copy(m, j, n, c0, w).start()

    def stat_copies(kind, m):
        peers = (cpeer, xpeer, xdiag) if kind == 0 else (cpeer, ypeer, ydiag)
        return [rc(ST.at[kind, m], SR.at[kind, m, k], st_ss.at[kind, m, k], st_rs.at[kind, m, k], peers[k]) for k in range(3)]

    def stat_send(kind, m):
        v0 = jnp.sum(RSUM[0], axis=1, keepdims=True)
        v1 = jnp.sum(RSUM[1], axis=1, keepdims=True)
        lane = lax.broadcasted_iota(jnp.int32, (R, 128), 1)
        both = jnp.where(lane == 0, v0, v1)
        full = jnp.concatenate([both, jnp.zeros((128 - R, 128), F32)], axis=0)
        ST[kind, m] = full.T[0:8]
        start(stat_copies(kind, m))

    def stat_recv(kind, m):
        wait(stat_copies(kind, m))
        total = (ST[kind, m] + SR[kind, m, 0]) + (SR[kind, m, 1] + SR[kind, m, 2])
        back = jnp.concatenate([total] * 16, axis=0).T
        scale = lax.rsqrt(back / 4096.0 + EPS)
        RSC[0] = jnp.broadcast_to(scale[0:R, 0:1], (R, 128))
        RSC[1] = jnp.broadcast_to(scale[0:R, 1:2], (R, 128))

    def phase_s(m):
        for n, (j, c0) in enumerate(QKV_TILES):
            tile_copy(m, j, c0 // TW, c0, TW).wait()

        def body(i, _):
            rows = pl.ds(pl.multiple_of(i * 16, 16), 16)
            for j in range(2):
                acc = jnp.zeros((16, 128), F32)
                for h in range(8):
                    cols = pl.ds((j * 8 + h) * 128, 128)
                    z = (GP[m, 0, ty, rows, cols].astype(F32) + GR[m, 0, rows, cols].astype(F32)).astype(BF)
                    GR[m, 0, rows, cols] = z
                    zf = z.astype(F32)
                    acc = acc + zf * zf
                RSUM[j, rows] = acc
            for h in range(8):
                cols = pl.ds(h * 128, 128)
                GR[m, 1, rows, cols] = (GP[m, 1, ty, rows, cols].astype(F32) + GR[m, 1, rows, cols].astype(F32)).astype(BF)
            return 0
        lax.fori_loop(0, R // 16, body, 0)
        stat_send(0, m)

    def phase_t1(m, l):
        stat_recv(0, m)

        def body(i, _):
            rows = pl.ds(pl.multiple_of(i * 16, 16), 16)
            t = i // 2
            dst = pl.ds(pl.multiple_of(lax.rem(i, 2) * 16, 16), 16)
            cosv = cos_ref[m, rows]
            sinv = sin_ref[m, rows]
            for j, (out, gain) in enumerate(((QS, qg_ref), (KS, kg_ref))):
                scale = RSC[j, rows]
                for h in range(8):
                    z = GR[m, 0, rows, pl.ds((j * 8 + h) * 128, 128)].astype(F32)
                    z = z * scale * gain[pl.ds(l, 1), pl.ds(h * 128, 128)].astype(F32)
                    rot = z * cosv + pltpu.roll(z, 64, 1) * sinv
                    out[t, dst, h, :] = rot.astype(BF).astype(F32)
            for h in range(8):
                VS[t, dst, h, :] = GR[m, 1, rows, pl.ds(h * 128, 128)].astype(F32)
            return 0
        lax.fori_loop(0, R // 16, body, 0)

    def ko_copies(l, m):
        rows = pl.ds(m * RB, RB)
        return [lc(KO.at[m], kn_ref.at[l, rows], ko_sem.at[0, m]), lc(VO.at[m], vn_ref.at[l, rows], ko_sem.at[1, m])]

    def o_copy(m):
        return rc(OB.at[m, ty], OB.at[m, ty], o_ss.at[m], o_rs.at[m], ypeer)

    def phase_t2(m, l):
        if l > 0:
            wait(ko_copies(l - 1, m))
        row = lax.broadcasted_iota(jnp.int32, (T * HL, SH), 0)
        col = lax.broadcasted_iota(jnp.int32, (T * HL, SH), 1)
        colm = jnp.where(lax.rem(row, HL) == lax.rem(col, HL), col, SH)
        rown = lax.broadcasted_iota(jnp.int32, (T * HL, T * HL), 0)
        coln = lax.broadcasted_iota(jnp.int32, (T * HL, T * HL), 1)
        newm = (lax.rem(rown, HL) == lax.rem(coln, HL)) & (coln <= rown)

        def chunk(c, _):
            slot = lax.rem(c, SLOTS)
            wait(kv_copies(l, m, c, slot))
            for k in range(CB):
                i = c * CB + k
                q = QS[:, i].reshape(T * HL, HEAD_DIM).astype(BF)
                kn = KS[:, i].reshape(T * HL, HEAD_DIM).astype(BF)
                vn = VS[:, i].reshape(T * HL, HEAD_DIM).astype(BF)
                limit = start_ref[m * RB + i] * HL
                s_old = jnp.where(colm < limit, dot_t(q, KB[slot, k]) * SCORE_SCALE, NEG_BIG)
                s_new = jnp.where(newm, dot_t(q, kn) * SCORE_SCALE, NEG_BIG)
                top = jnp.maximum(jnp.max(s_old, axis=1, keepdims=True), jnp.max(s_new, axis=1, keepdims=True))
                e_old = jnp.exp(s_old - top)
                e_new = jnp.exp(s_new - top)
                den = jnp.sum(e_old, axis=1, keepdims=True) + jnp.sum(e_new, axis=1, keepdims=True)
                o = dot((e_old / den).astype(BF), VB[slot, k]) + dot((e_new / den).astype(BF), vn)
                OS[:, i] = o.reshape(T, HL, HEAD_DIM)
                KO[m, i] = kn
                VO[m, i] = vn

            @pl.when(c < NCH - SLOTS)
            def _():
                start(kv_copies(l, m, c + SLOTS, slot))
            return 0
        lax.fori_loop(0, NCH, chunk, 0)
        start(ko_copies(l, m))
        nxt = (l, m + 1) if m + 1 < NB else (l + 1, 0)
        if nxt[0] < L:
            for c in range(SLOTS):
                start(kv_copies(nxt[0], nxt[1], c, c))

        def body(i, _):
            rows = pl.ds(pl.multiple_of(i * 16, 16), 16)
            t = i // 2
            src = pl.ds(pl.multiple_of(lax.rem(i, 2) * 16, 16), 16)
            for h in range(8):
                OB[m, ty, rows, pl.ds(h * 128, 128)] = OS[t, src, h, :].astype(BF)
            return 0
        lax.fori_loop(0, R // 16, body, 0)
        o_copy(m).start()

    def p_copy(m):
        return rc(XP.at[m, :, oth_half], XC.at[m], p_ss.at[m], p_rs.at[m], cpeer)

    def x_copy(ph, m):
        return rc(XS.at[m], XR.at[ph, m], x_ss.at[m], x_rs.at[ph, m], xpeer)

    def a_copy(m):
        return rc(AF.at[m, :, own_half], AF.at[m, :, own_half], a_ss.at[m], a_rs.at[m], cpeer)

    def phase_o(m, l):
        o_copy(m).wait()
        for half in (1 - core, core):
            def body(i, _):
                cols = pl.ds(pl.multiple_of(half * HALF + i * TW, TW), TW)
                XP[m, :, cols] = dot(OB[m].reshape(2 * R, QW), WO[:, cols]).astype(BF)
                return 0
            lax.fori_loop(0, 2, body, 0)
            if half is not core:
                p_copy(m).start()

    def phase_d(m, l):
        for n, (c0, w) in enumerate(GU_TILES):
            c_copy(m, n, c0, w).wait()
        for half in (1 - core, core):
            def body(i, _):
                cols = pl.ds(pl.multiple_of(half * HALF + i * TW, TW), TW)
                cm = C[m].reshape(2 * R, FP)
                XP[m, :, cols] = dot(cm[:, :FW], WD[:, cols]).astype(BF)
                return 0
            lax.fori_loop(0, 2, body, 0)
            if half is not core:
                p_copy(m).start()

    def phase_2(ph, m):
        p_copy(m).wait()

        def body(i, _):
            rows = pl.ds(pl.multiple_of(i * 16, 16), 16)
            XS[m, rows] = (XP[m, rows, own_half].astype(F32) + XC[m, rows].astype(F32)).astype(BF)
            return 0
        lax.fori_loop(0, 2 * R // 16, body, 0)
        x_copy(ph, m).start()

    def phase_3(ph, m):
        x_copy(ph, m).wait()

        def body(i, _):
            rows = pl.ds(pl.multiple_of(i * 16, 16), 16)
            z = (XS[m, rows].astype(F32) + XR[ph, m, rows].astype(F32)).astype(BF)
            AF[m, rows, own_half] = z
            zf = z.astype(F32)
            sq = zf * zf
            acc = sq[:, 0:128]
            for h in range(1, 8):
                acc = acc + sq[:, h * 128:(h + 1) * 128]
            RSUM[i // 6, pl.ds(pl.multiple_of(lax.rem(i, 6) * 16, 16), 16)] = acc
            return 0
        lax.fori_loop(0, 2 * R // 16, body, 0)
        a_copy(m).start()
        stat_send(1 + ph, m)

    def phase_h(ph, m, l):
        gain = (ag_ref, mg_ref)[ph]
        stat_recv(1 + ph, m)
        a_copy(m).wait()

        def body(i, _):
            y = i // 6
            rows = pl.ds(pl.multiple_of(lax.rem(i, 6) * 16, 16), 16)
            arow = pl.ds(pl.multiple_of(i * 16, 16), 16)
            scale = RSC[y, rows]
            for h in range(16):
                cols = pl.ds(h * 128, 128)
                X[m, y, rows, cols] = (X[m, y, rows, cols].astype(F32) + AF[m, arow, cols].astype(F32) * scale * gain[pl.ds(l, 1), cols].astype(F32)).astype(BF)
            return 0
        lax.fori_loop(0, 2 * R // 16, body, 0)

    def c_copy(m, n, c0, w):
        return rc(C.at[m, ty, :, pl.ds(c0, w)], C.at[m, ty, :, pl.ds(c0, w)], c_ss.at[m, n], c_rs.at[m, n], ypeer)

    def phase_c(m, lo, hi):
        for n in range(lo, hi):
            c0, w = GU_TILES[n]
            for j in range(2):
                tile_copy(m, j, n, c0, w).wait()

            def body(i, _):
                rows = pl.ds(pl.multiple_of(i * 16, 16), 16)
                cols = pl.ds(c0, w)
                g = (GP[m, 0, ty, rows, cols].astype(F32) + GR[m, 0, rows, cols].astype(F32)).astype(BF).astype(F32)
                u = (GP[m, 1, ty, rows, cols].astype(F32) + GR[m, 1, rows, cols].astype(F32)).astype(BF).astype(F32)
                C[m, ty, rows, cols] = (jax.nn.silu(g) * u).astype(BF)
                return 0
            lax.fori_loop(0, R // 16, body, 0)
            c_copy(m, n, c0, w).start()

    def y_copies(m):
        out = []
        for y in range(2):
            for t in range(T):
                out.append(lc(X.at[m, y, pl.ds(t * RB, RB)], y_ref.at[t, pl.ds(y * NB * RB + m * RB, RB)], y_sem.at[(m * 2 + y) * T + t]))
        return out

    A, B = 0, 1
    wait(emb_copies())
    phase_q(A, 0, True)
    phase_q(B, 0, False)
    for l in range(L):
        phase_s(A)
        phase_t1(A, l)
        phase_t2(A, l)
        start(gu_loads(l))
        phase_s(B)
        phase_t1(B, l)
        wait(wo_loads(l))
        phase_o(A, l)
        phase_2(0, A)
        phase_t2(B, l)
        phase_3(0, A)
        phase_o(B, l)
        phase_h(0, A, l)
        phase_2(0, B)
        if l + 1 < L:
            start(wo_loads(l + 1))
        wait(gu_loads(l))
        phase_g(A, 3)
        phase_3(0, B)
        send_g(A, 3, 6)
        phase_h(0, B, l)
        phase_g(B, 0)
        if l + 1 < L:
            start(qkv_loads(l + 1))
        phase_c(A, 0, 6)
        send_g(B, 0, 3)
        wait(wd_loads(l))
        phase_d(A, l)
        phase_2(1, A)
        phase_c(B, 0, 2)
        phase_3(1, A)
        send_g(B, 3, 6)
        phase_h(1, A, l)
        phase_c(B, 2, 6)
        if l + 1 < L:
            phase_q(A, l + 1, True)
        else:
            start(y_copies(A))
        phase_d(B, l)
        if l + 1 < L:
            start(wd_loads(l + 1))
        phase_2(1, B)
        phase_3(1, B)
        phase_h(1, B, l)
        if l + 1 < L:
            phase_q(B, l + 1, False)
        else:
            start(y_copies(B))
    wait(y_copies(A))
    wait(y_copies(B))
    for m in range(NB):
        wait(ko_copies(L - 1, m))


def cache_kernel(start_ref, k_ref, v_ref, kn_ref, vn_ref, ko_ref, vo_ref):
    c = pl.program_id(1)
    ko_ref[...] = k_ref[...]
    vo_ref[...] = v_ref[...]
    for i in range(k_ref.shape[1]):
        p = start_ref[c * k_ref.shape[1] + i]
        for t in range(T):
            ko_ref[0, i, p + t] = kn_ref[0, i, t]
            vo_ref[0, i, p + t] = vn_ref[0, i, t]


def solution(mesh):
    act_spec = P(None, 'dp', 'tpy')
    cache_spec = P(None, ('dp', 'tpy'), None, 'tpx', None)
    col_spec = P(None, 'tpy', 'tpx')
    row_spec = P(None, 'tpx', 'tpy')
    head_gain = P(None, 'tpx')
    width_gain = P(None, 'tpy')

    def device_fn(embeds, start_pos, k_cache, v_cache, w_query, w_key, w_value, w_out, w_gate, w_up, w_down, q_gain, k_gain, attn_gain, mlp_gain):
        rows = NB * RB
        start_local = lax.dynamic_slice_in_dim(start_pos, lax.axis_index('tpy') * rows, rows)
        pos = (start_local.reshape(NB, 1, RB) + jnp.arange(T, dtype=jnp.int32)[None, :, None]).reshape(NB, R)
        inv_freq = jnp.power(THETA, jnp.arange(HEAD_DIM // 2, dtype=F32) * (-2.0 / HEAD_DIM))
        ang = pos.astype(F32)[..., None] * inv_freq
        cos_part, sin_part = jnp.cos(ang), jnp.sin(ang)
        cos2 = jnp.concatenate([cos_part, cos_part], axis=-1)
        sin2 = jnp.concatenate([-sin_part, sin_part], axis=-1)
        hbm = pl.BlockSpec(memory_space=pl.ANY)
        vm = pl.BlockSpec(memory_space=pltpu.VMEM)
        dma = pltpu.SemaphoreType.DMA
        y, kn, vn = pl.pallas_call(
            main_kernel,
            out_shape=[
                jax.ShapeDtypeStruct(embeds.shape, BF),
                jax.ShapeDtypeStruct((L, rows, T * HL, HEAD_DIM), BF),
                jax.ShapeDtypeStruct((L, rows, T * HL, HEAD_DIM), BF),
            ],
            in_specs=[pl.BlockSpec(memory_space=pltpu.SMEM)] + [hbm] * 10 + [vm] * 6,
            out_specs=[hbm] * 3,
            scratch_shapes=[
                pltpu.VMEM((NB, 2, R, DW), BF),
                pltpu.VMEM((2, FW, DW), BF),
                pltpu.VMEM((QW, DW), BF),
                pltpu.VMEM((FW, DW), BF),
                pltpu.VMEM((NB, 2, 2, R, FP), BF),
                pltpu.VMEM((NB, 2, R, FP), BF),
                pltpu.VMEM((NB, 2, R, FP), BF),
                pltpu.VMEM((NB, 2, R, QW), BF),
                pltpu.VMEM((T, RB, HL, HEAD_DIM), F32),
                pltpu.VMEM((T, RB, HL, HEAD_DIM), F32),
                pltpu.VMEM((T, RB, HL, HEAD_DIM), F32),
                pltpu.VMEM((T, RB, HL, HEAD_DIM), F32),
                pltpu.VMEM((NB, RB, T * HL, HEAD_DIM), BF),
                pltpu.VMEM((NB, RB, T * HL, HEAD_DIM), BF),
                pltpu.VMEM((SLOTS, CB, SH, HEAD_DIM), BF),
                pltpu.VMEM((SLOTS, CB, SH, HEAD_DIM), BF),
                pltpu.VMEM((NB, 2 * R, DW), BF),
                pltpu.VMEM((NB, 2 * R, HALF), BF),
                pltpu.VMEM((NB, 2 * R, HALF), BF),
                pltpu.VMEM((2, NB, 2 * R, HALF), BF),
                pltpu.VMEM((NB, 2 * R, DW), BF),
                pltpu.VMEM((2, R, 128), F32),
                pltpu.VMEM((2, R, 128), F32),
                pltpu.VMEM((3, NB, 8, 128), F32),
                pltpu.VMEM((3, NB, 3, 8, 128), F32),
                dma((NB * 2 * T,)), dma((6,)), dma((8,)), dma((1,)), dma((4,)), dma((2, SLOTS)), dma((2, NB)), dma((NB * 2 * T,)),
                dma((NB, 2, 6)), dma((NB, 2, 6)), dma((NB, 6)), dma((NB, 6)), dma((NB,)), dma((NB,)),
                dma((NB,)), dma((NB,)), dma((NB,)), dma((2, NB)), dma((NB,)), dma((NB,)), dma((3, NB, 3)), dma((3, NB, 3)),
            ],
            compiler_params=pltpu.CompilerParams(collective_id=0, has_side_effects=True, vmem_limit_bytes=67043328),
            name="layers",
        )(start_local, embeds, k_cache.reshape(L, rows, SH, HEAD_DIM), v_cache.reshape(L, rows, SH, HEAD_DIM),
          w_query, w_key, w_value, w_out, w_gate.transpose(0, 2, 1), w_up.transpose(0, 2, 1), w_down, q_gain, k_gain, attn_gain, mlp_gain, cos2, sin2)
        bc = 8
        big = pl.BlockSpec((1, bc, SEQ, HL, HEAD_DIM), lambda l, c, s: (l, c, 0, 0, 0))
        small = pl.BlockSpec((1, bc, T, HL, HEAD_DIM), lambda l, c, s: (l, c, 0, 0, 0))
        k_out, v_out = pl.pallas_call(
            cache_kernel,
            out_shape=[jax.ShapeDtypeStruct(k_cache.shape, BF)] * 2,
            grid_spec=pltpu.PrefetchScalarGridSpec(
                num_scalar_prefetch=1, grid=(L, rows // bc), in_specs=[big, big, small, small], out_specs=[big, big]),
            name="caches",
        )(start_local, k_cache, v_cache, kn.reshape(L, rows, T, HL, HEAD_DIM), vn.reshape(L, rows, T, HL, HEAD_DIM))
        return y, k_out, v_out

    return jax.shard_map(device_fn, mesh=mesh, in_specs=(act_spec, P('dp'), cache_spec, cache_spec, col_spec, col_spec, col_spec, row_spec, col_spec, col_spec, row_spec, head_gain, head_gain, width_gain, width_gain), out_specs=(act_spec, cache_spec, cache_spec), check_vma=False)
```

```python
import functools
import math
import jax
import jax.numpy as jnp
from jax import lax
from jax.experimental import pallas as pl
from jax.experimental.pallas import tpu as pltpu
from jax.sharding import PartitionSpec as P

HEAD_DIM = 128
EPS = 1e-6
THETA = 500000.0
SCORE_SCALE = 1.0 / math.sqrt(HEAD_DIM)
NEG_BIG = -1e30
MESH = pl.DeviceIdType.MESH
BF = jnp.bfloat16
F32 = jnp.float32

L = 2
T = 3
NB = 4
RB = 16
R = T * RB
HL = 8
DW = 2048
QW = HL * HEAD_DIM
FW = 2752
FP = 2816
SEQ = 64
SH = SEQ * HL
CB = 4
NCH = RB // CB
SLOTS = 4
TW = 512
HALF = DW // 2
RC = R // 16
GU_TILES = [(0, 512), (512, 512), (1024, 512), (1536, 512), (2048, 512), (2560, 256)]
QKV_TILES = [(0, 0), (0, 512), (0, 1024), (0, 1536), (1, 0), (1, 512)]


ORDER = [
    ("Q", 0, 0),
    ("Qs", 0, 0, 0, 6),
    ("Q", 1, 0),
    ("Qs", 1, 0, 0, 4),
    ("Q", 2, 0),
    ("Qs", 1, 0, 4, 6),
    ("Q", 3, 0),
    ("S", 0, 0),
    ("T", 0, 0),
    ("Qs", 2, 0, 0, 2),
    ("Lg", 0),
    ("Qs", 2, 0, 2, 4),
    ("O", 0, 0),
    ("S", 1, 0),
    ("2", 0, 0, 0),
    ("Qs", 2, 0, 4, 6),
    ("Qs", 3, 0, 0, 2),
    ("T", 1, 0),
    ("S", 2, 0),
    ("3", 0, 0, 0),
    ("Qs", 3, 0, 2, 6),
    ("T", 2, 0),
    ("H", 0, 0, 0),
    ("G", 0, 0),
    ("Gs", 0, 0, 0, 4),
    ("S", 3, 0),
    ("O", 1, 0),
    ("2", 0, 1, 0),
    ("C", 0, 0, 0, 1),
    ("3", 0, 1, 0),
    ("Gs", 0, 0, 4, 5),
    ("C", 0, 0, 1, 3),
    ("O", 2, 0),
    ("C", 0, 0, 3, 4),
    ("T", 3, 0),
    ("2", 0, 2, 0),
    ("H", 0, 1, 0),
    ("Gs", 0, 0, 5, 6),
    ("G", 1, 0),
    ("Gs", 1, 0, 0, 2),
    ("C", 0, 0, 4, 5),
    ("O", 3, 0),
    ("3", 0, 2, 0),
    ("2", 0, 3, 0),
    ("Gs", 1, 0, 2, 4),
    ("H", 0, 2, 0),
    ("C", 0, 0, 5, 6),
    ("C", 1, 0, 0, 3),
    ("3", 0, 3, 0),
    ("Gs", 1, 0, 4, 5),
    ("G", 2, 0),
    ("Gs", 2, 0, 0, 1),
    ("D", 0, 0),
    ("Gs", 2, 0, 1, 2),
    ("H", 0, 3, 0),
    ("Gs", 1, 0, 5, 6),
    ("C", 1, 0, 3, 4),
    ("2", 1, 0, 0),
    ("Gs", 2, 0, 2, 3),
    ("C", 2, 0, 0, 1),
    ("C", 1, 0, 4, 5),
    ("G", 3, 0),
    ("Gs", 3, 0, 0, 1),
    ("Lo", 1),
    ("3", 1, 0, 0),
    ("Gs", 3, 0, 1, 2),
    ("C", 3, 0, 0, 1),
    ("C", 1, 0, 5, 6),
    ("C", 2, 0, 1, 2),
    ("Gs", 2, 0, 3, 4),
    ("C", 2, 0, 2, 3),
    ("D", 1, 0),
    ("Gs", 3, 0, 2, 4),
    ("H", 1, 0, 0),
    ("2", 1, 1, 0),
    ("Gs", 2, 0, 4, 5),
    ("C", 3, 0, 1, 2),
    ("3", 1, 1, 0),
    ("Lq", 1),
    ("Gs", 2, 0, 5, 6),
    ("C", 3, 0, 2, 3),
    ("Gs", 3, 0, 4, 5),
    ("C", 3, 0, 3, 4),
    ("C", 2, 0, 3, 4),
    ("Q", 0, 1),
    ("Gs", 3, 0, 5, 6),
    ("C", 2, 0, 4, 5),
    ("H", 1, 1, 0),
    ("C", 2, 0, 5, 6),
    ("Qs", 0, 1, 0, 4),
    ("C", 3, 0, 4, 6),
    ("Qs", 0, 1, 4, 6),
    ("D", 2, 0),
    ("Q", 1, 1),
    ("Qs", 1, 1, 0, 2),
    ("2", 1, 2, 0),
    ("Qs", 1, 1, 2, 4),
    ("D", 3, 0),
    ("S", 0, 1),
    ("3", 1, 2, 0),
    ("2", 1, 3, 0),
    ("Qs", 1, 1, 4, 6),
    ("T", 0, 1),
    ("H", 1, 2, 0),
    ("Q", 2, 1),
    ("Qs", 2, 1, 0, 2),
    ("S", 1, 1),
    ("3", 1, 3, 0),
    ("O", 0, 1),
    ("Qs", 2, 1, 2, 6),
    ("T", 1, 1),
    ("2", 0, 0, 1),
    ("H", 1, 3, 0),
    ("Q", 3, 1),
    ("Lg", 1),
    ("S", 2, 1),
    ("Qs", 3, 1, 0, 2),
    ("3", 0, 0, 1),
    ("Qs", 3, 1, 2, 4),
    ("O", 1, 1),
    ("T", 2, 1),
    ("2", 0, 1, 1),
    ("H", 0, 0, 1),
    ("Qs", 3, 1, 4, 6),
    ("G", 0, 1),
    ("Gs", 0, 1, 0, 1),
    ("3", 0, 1, 1),
    ("Gs", 0, 1, 1, 3),
    ("S", 3, 1),
    ("O", 2, 1),
    ("C", 0, 1, 0, 1),
    ("2", 0, 2, 1),
    ("T", 3, 1),
    ("Gs", 0, 1, 3, 5),
    ("H", 0, 1, 1),
    ("G", 1, 1),
    ("O", 3, 1),
    ("Gs", 1, 1, 0, 1),
    ("3", 0, 2, 1),
    ("Gs", 1, 1, 1, 3),
    ("H", 0, 2, 1),
    ("2", 0, 3, 1),
    ("C", 0, 1, 1, 2),
    ("C", 1, 1, 0, 1),
    ("Gs", 1, 1, 3, 4),
    ("G", 2, 1),
    ("Gs", 1, 1, 4, 5),
    ("Gs", 2, 1, 0, 1),
    ("Gs", 0, 1, 5, 6),
    ("Gs", 2, 1, 1, 2),
    ("C", 1, 1, 1, 2),
    ("3", 0, 3, 1),
    ("C", 1, 1, 2, 3),
    ("C", 2, 1, 0, 1),
    ("C", 1, 1, 3, 4),
    ("H", 0, 3, 1),
    ("C", 2, 1, 1, 2),
    ("Gs", 2, 1, 2, 3),
    ("Gs", 1, 1, 5, 6),
    ("C", 0, 1, 2, 4),
    ("Gs", 2, 1, 3, 4),
    ("C", 2, 1, 2, 3),
    ("Gs", 2, 1, 4, 5),
    ("C", 1, 1, 4, 5),
    ("Gs", 2, 1, 5, 6),
    ("C", 2, 1, 3, 4),
    ("C", 0, 1, 4, 5),
    ("G", 3, 1),
    ("C", 0, 1, 5, 6),
    ("C", 2, 1, 4, 5),
    ("Gs", 3, 1, 0, 1),
    ("C", 1, 1, 5, 6),
    ("Gs", 3, 1, 1, 2),
    ("Ld", 1),
    ("C", 3, 1, 0, 1),
    ("Gs", 3, 1, 2, 3),
    ("D", 0, 1),
    ("C", 2, 1, 5, 6),
    ("Gs", 3, 1, 3, 4),
    ("D", 1, 1),
    ("C", 3, 1, 1, 2),
    ("Gs", 3, 1, 4, 6),
    ("2", 1, 0, 1),
    ("C", 3, 1, 2, 3),
    ("2", 1, 1, 1),
    ("C", 3, 1, 3, 5),
    ("D", 2, 1),
    ("C", 3, 1, 5, 6),
    ("2", 1, 2, 1),
    ("D", 3, 1),
    ("2", 1, 3, 1),
    ("3", 1, 0, 1),
    ("3", 1, 2, 1),
    ("H", 1, 0, 1),
    ("3", 1, 1, 1),
    ("3", 1, 3, 1),
    ("H", 1, 1, 1),
    ("H", 1, 2, 1),
    ("H", 1, 3, 1),
]


def lane_fold(z):
    return jnp.broadcast_to(jnp.sum(z, axis=1, keepdims=True), (z.shape[0], 128))


def dot(a, b):
    return jnp.dot(a, b, preferred_element_type=F32)


def dot_t(a, b):
    return lax.dot_general(a, b, (((1,), (1,)), ((), ())), preferred_element_type=F32)


def main_kernel(start_ref, emb_ref, kc_ref, vc_ref, wq_ref, wk_ref, wv_ref, wo_ref, wg_ref, wu_ref, wd_ref,
                qg_ref, kg_ref, ag_ref, mg_ref, cos_ref, sin_ref,
                y_ref, kn_ref, vn_ref,
                X, W1, WO, WD, GP, GR, C, OB, QS, KS, VS, OS, KO, VO, KB, VB, XP, XC, XS, XR, AF, RSUM, RSC, ST, SR,
                in_sem, q_wsem, g_wsem, o_wsem, d_wsem, kv_sem, ko_sem, y_sem,
                g_ss, g_rs, c_ss, c_rs, o_ss, o_rs, p_ss, p_rs, x_ss, x_rs, a_ss, a_rs, st_ss, st_rs):
    ty = lax.axis_index("tpy")
    tx = lax.axis_index("tpx")
    core = lax.rem(tx, 2)
    oy = 1 - ty
    cx = tx + 1 - 2 * core
    xx = lax.rem(tx + 2, 4)
    dx = 3 - tx
    ypeer = {"tpy": oy}
    cpeer = {"tpx": cx}
    xpeer = {"tpx": xx}
    xdiag = {"tpx": dx}
    ydiag = {"tpy": oy, "tpx": cx}
    own_half = pl.ds(pl.multiple_of(core * HALF, HALF), HALF)
    oth_half = pl.ds(pl.multiple_of((1 - core) * HALF, HALF), HALF)

    def rc(src, dst, ss, rs, dev):
        return pltpu.make_async_remote_copy(src_ref=src, dst_ref=dst, send_sem=ss, recv_sem=rs, device_id=dev, device_id_type=MESH)

    def lc(src, dst, sem):
        return pltpu.make_async_copy(src, dst, sem)

    def emb_copies():
        out = []
        for m in range(NB):
            for y in range(2):
                for t in range(T):
                    out.append(lc(emb_ref.at[t, pl.ds(y * NB * RB + m * RB, RB)], X.at[m, y, pl.ds(t * RB, RB)], in_sem.at[(m * 2 + y) * T + t]))
        return out

    def qkv_load(l, n):
        j, c0 = QKV_TILES[n]
        src = (wq_ref, wk_ref, wv_ref)[n // 2]
        return lc(src.at[l, :, pl.ds((n % 2) * TW, TW)], W1.at[j, pl.ds(0, DW), pl.ds(c0, TW)], q_wsem.at[n])

    def qkv_loads(l):
        return [qkv_load(l, n) for n in range(6)]

    def gu_loads(l):
        return [lc((wg_ref, wu_ref)[j].at[l, pl.ds(r * 688, 688)], W1.at[j, pl.ds(r * 688, 688)], g_wsem.at[j * 4 + r]) for r in range(4) for j in range(2)]

    def wo_loads(l):
        return [lc(wo_ref.at[l], WO, o_wsem.at[0])]

    def wd_loads(l):
        return [lc(wd_ref.at[l, pl.ds(r * 688, 688)], WD.at[pl.ds(r * 688, 688)], d_wsem.at[r]) for r in range(4)]

    def start(copies):
        for cp in copies:
            cp.start()

    def wait(copies):
        for cp in copies:
            cp.wait()

    def kv_copies(l, m, c, slot):
        rows = pl.ds(m * RB + c * CB, CB)
        return [lc(kc_ref.at[l, rows], KB.at[slot], kv_sem.at[0, slot]), lc(vc_ref.at[l, rows], VB.at[slot], kv_sem.at[1, slot])]

    start(emb_copies())
    start(qkv_loads(0))

    barrier = pltpu.get_barrier_semaphore()
    for dev in (ypeer, cpeer, xpeer, xdiag, ydiag):
        pl.semaphore_signal(barrier, inc=1, device_id=dev, device_id_type=MESH)
    pl.semaphore_wait(barrier, 5)

    for c in range(SLOTS):
        start(kv_copies(0, 0, c, c))
    start(wo_loads(0))
    start(wd_loads(0))

    def tile_copy(m, j, n, c0, w):
        return rc(GP.at[m, j, oy, :, pl.ds(c0, w)], GR.at[m, j, :, pl.ds(c0, w)], g_ss.at[m, j, n], g_rs.at[m, j, n], ypeer)

    def compute_tile(m, j, c0, w, transposed=False):
        xm = X[m].reshape(2 * R, DW)
        if transposed:
            res = dot_t(xm, W1[j, pl.ds(c0, w), :]).astype(BF)
        else:
            res = dot(xm, W1[j, pl.ds(0, DW), pl.ds(c0, w)]).astype(BF)
        GP[m, j, :, :, pl.ds(c0, w)] = res.reshape(2, R, w)

    def phase_q(m, l, fresh):
        for j, cnt in ((0, 4), (1, 2)):
            if fresh:
                for i in range(cnt):
                    qkv_load(l, j * 4 + i).wait()

            def body(i, _):
                compute_tile(m, j, pl.multiple_of(i * TW, TW), TW)
                return 0
            lax.fori_loop(0, cnt, body, 0)

    def send_q(m, lo, hi):
        for j, c0 in QKV_TILES[lo:hi]:
            tile_copy(m, j, c0 // TW, c0, TW).start()

    def phase_g(m):
        def body(i, _):
            for j in range(2):
                compute_tile(m, j, pl.multiple_of(i * TW, TW), TW, True)
            return 0
        lax.fori_loop(0, 5, body, 0)
        for j in range(2):
            compute_tile(m, j, 2560, 192, True)

    def send_g(m, lo, hi):
        def body(n, _):
            for j in range(2):
                tile_copy(m, j, n, pl.multiple_of(n * TW, TW), TW).start()
            return 0
        if lo < 5:
            lax.fori_loop(lo, min(hi, 5), body, 0)
        if hi == 6:
            for j in range(2):
                tile_copy(m, j, 5, 2560, 256).start()

    def stat_copies(kind, m):
        peers = (cpeer, xpeer, xdiag) if kind == 0 else (cpeer, ypeer, ydiag)
        return [rc(ST.at[kind, m], SR.at[kind, m, k], st_ss.at[kind, m, k], st_rs.at[kind, m, k], peers[k]) for k in range(3)]

    def stat_send(kind, m):
        v0 = RSUM[0]
        v1 = RSUM[1]
        lane = lax.broadcasted_iota(jnp.int32, (R, 128), 1)
        both = jnp.where(lane == 0, v0, v1)
        full = jnp.concatenate([both, jnp.zeros((128 - R, 128), F32)], axis=0)
        ST[kind, m] = full.T[0:8]
        start(stat_copies(kind, m))

    def stat_recv(kind, m):
        wait(stat_copies(kind, m))
        total = (ST[kind, m] + SR[kind, m, 0]) + (SR[kind, m, 1] + SR[kind, m, 2])
        back = jnp.concatenate([total] * 16, axis=0).T
        scale = lax.rsqrt(back / 4096.0 + EPS)
        RSC[0] = jnp.broadcast_to(scale[0:R, 0:1], (R, 128))
        RSC[1] = jnp.broadcast_to(scale[0:R, 1:2], (R, 128))

    def phase_s(m):
        for n, (j, c0) in enumerate(QKV_TILES):
            tile_copy(m, j, c0 // TW, c0, TW).wait()

        def body(i, _):
            rows = pl.ds(pl.multiple_of(i * 16, 16), 16)
            qk = pl.ds(0, 2 * QW)
            z = (GP[m, 0, ty, rows, qk].astype(F32) + GR[m, 0, rows, qk].astype(F32)).astype(BF)
            GR[m, 0, rows, qk] = z
            zf = z.astype(F32)
            sq = zf * zf
            RSUM[0, rows] = lane_fold(sq[:, :QW])
            RSUM[1, rows] = lane_fold(sq[:, QW:])
            cols = pl.ds(0, QW)
            GR[m, 1, rows, cols] = (GP[m, 1, ty, rows, cols].astype(F32) + GR[m, 1, rows, cols].astype(F32)).astype(BF)
            return 0
        lax.fori_loop(0, R // 16, body, 0)
        stat_send(0, m)

    def phase_t1(m, l):
        stat_recv(0, m)

        gain = jnp.concatenate([qg_ref[pl.ds(l, 1)], kg_ref[pl.ds(l, 1)]], axis=1).astype(F32)
        low = lax.rem(lax.broadcasted_iota(jnp.int32, (16, 2 * QW), 1), HEAD_DIM) < HEAD_DIM // 2

        def body(i, _):
            rows = pl.ds(pl.multiple_of(i * 16, 16), 16)
            scale = jnp.concatenate([RSC[0, rows]] * HL + [RSC[1, rows]] * HL, axis=1)
            z = GR[m, 0, rows, pl.ds(0, 2 * QW)].astype(F32) * scale * gain
            turned = jnp.where(low, pltpu.roll(z, 2 * QW - HEAD_DIM // 2, 1), pltpu.roll(z, HEAD_DIM // 2, 1))
            rot = z * jnp.concatenate([cos_ref[m, rows]] * (2 * HL), axis=1) + turned * jnp.concatenate([sin_ref[m, rows]] * (2 * HL), axis=1)
            rot = rot.astype(BF).astype(F32)
            v = GR[m, 1, rows, pl.ds(0, QW)].astype(F32)
            for h in range(HL):
                QS[i, :, h, :] = rot[:, h * HEAD_DIM:(h + 1) * HEAD_DIM]
                KS[i, :, h, :] = rot[:, QW + h * HEAD_DIM:QW + (h + 1) * HEAD_DIM]
                VS[i, :, h, :] = v[:, h * HEAD_DIM:(h + 1) * HEAD_DIM]
            return 0
        lax.fori_loop(0, R // 16, body, 0)

    def ko_copies(l, m):
        rows = pl.ds(m * RB, RB)
        return [lc(KO.at[m], kn_ref.at[l, rows], ko_sem.at[0, m]), lc(VO.at[m], vn_ref.at[l, rows], ko_sem.at[1, m])]

    def o_copy(m):
        return rc(OB.at[m, ty], OB.at[m, ty], o_ss.at[m], o_rs.at[m], ypeer)

    def phase_t2(m, l):
        if l > 0:
            wait(ko_copies(l - 1, m))
        row = lax.broadcasted_iota(jnp.int32, (T * HL, SH), 0)
        col = lax.broadcasted_iota(jnp.int32, (T * HL, SH), 1)
        colm = jnp.where(lax.rem(row, HL) == lax.rem(col, HL), col, SH)
        rown = lax.broadcasted_iota(jnp.int32, (T * HL, T * HL), 0)
        coln = lax.broadcasted_iota(jnp.int32, (T * HL, T * HL), 1)
        newm = (lax.rem(rown, HL) == lax.rem(coln, HL)) & (coln <= rown)

        nxt = (l, m + 1) if m + 1 < NB else (l + 1, 0)

        def chunk(c, _):
            slot = c
            wait(kv_copies(l, m, c, slot))
            for k in range(CB):
                i = c * CB + k
                q = QS[:, i].reshape(T * HL, HEAD_DIM).astype(BF)
                kn = KS[:, i].reshape(T * HL, HEAD_DIM).astype(BF)
                vn = VS[:, i].reshape(T * HL, HEAD_DIM).astype(BF)
                limit = start_ref[m * RB + i] * HL
                s_old = jnp.where(colm < limit, dot_t(q, KB[slot, k]) * SCORE_SCALE, NEG_BIG)
                s_new = jnp.where(newm, dot_t(q, kn) * SCORE_SCALE, NEG_BIG)
                top = jnp.maximum(jnp.max(s_old, axis=1, keepdims=True), jnp.max(s_new, axis=1, keepdims=True))
                e_old = jnp.exp(s_old - top)
                e_new = jnp.exp(s_new - top)
                den = jnp.sum(e_old, axis=1, keepdims=True) + jnp.sum(e_new, axis=1, keepdims=True)
                o = dot((e_old / den).astype(BF), VB[slot, k]) + dot((e_new / den).astype(BF), vn)
                OS[:, i] = o.reshape(T, HL, HEAD_DIM)
                KO[m, i] = kn
                VO[m, i] = vn
            if nxt[0] < L:
                start(kv_copies(nxt[0], nxt[1], c, slot))
            return 0
        lax.fori_loop(0, NCH, chunk, 0)
        start(ko_copies(l, m))

        def body(i, _):
            rows = pl.ds(pl.multiple_of(i * 16, 16), 16)
            for h in range(8):
                OB[m, ty, rows, pl.ds(h * 128, 128)] = OS[i, :, h, :].astype(BF)
            return 0
        lax.fori_loop(0, R // 16, body, 0)
        o_copy(m).start()

    def p_copy(m):
        return rc(XP.at[m, :, oth_half], XC.at[m], p_ss.at[m], p_rs.at[m], cpeer)

    def x_copy(ph, m):
        return rc(XS.at[m], XR.at[ph, m], x_ss.at[m], x_rs.at[ph, m], xpeer)

    def a_copy(m):
        return rc(AF.at[m, :, own_half], AF.at[m, :, own_half], a_ss.at[m], a_rs.at[m], cpeer)

    def phase_o(m, l):
        o_copy(m).wait()
        for half in (1 - core, core):
            def body(i, _):
                cols = pl.ds(pl.multiple_of(half * HALF + i * TW, TW), TW)
                XP[m, :, cols] = dot(OB[m].reshape(2 * R, QW), WO[:, cols]).astype(BF)
                return 0
            lax.fori_loop(0, 2, body, 0)
            if half is not core:
                p_copy(m).start()

    def phase_d(m, l):
        for n, (c0, w) in enumerate(GU_TILES):
            c_copy(m, n, c0, w).wait()
        for half in (1 - core, core):
            def body(i, _):
                cols = pl.ds(pl.multiple_of(half * HALF + i * TW, TW), TW)
                cm = C[m].reshape(2 * R, FP)
                XP[m, :, cols] = dot(cm[:, :FW], WD[:, cols]).astype(BF)
                return 0
            lax.fori_loop(0, 2, body, 0)
            if half is not core:
                p_copy(m).start()

    def phase_2(ph, m):
        p_copy(m).wait()

        def body(i, _):
            rows = pl.ds(pl.multiple_of(i * 16, 16), 16)
            XS[m, rows] = (XP[m, rows, own_half].astype(F32) + XC[m, rows].astype(F32)).astype(BF)
            return 0
        lax.fori_loop(0, 2 * R // 16, body, 0)
        x_copy(ph, m).start()

    def phase_3(ph, m):
        x_copy(ph, m).wait()

        def body(i, _):
            rows = pl.ds(pl.multiple_of(i * 16, 16), 16)
            z = (XS[m, rows].astype(F32) + XR[ph, m, rows].astype(F32)).astype(BF)
            AF[m, rows, own_half] = z
            zf = z.astype(F32)
            acc = lane_fold(zf * zf)
            RSUM[i // RC, pl.ds(pl.multiple_of(lax.rem(i, RC) * 16, 16), 16)] = acc
            return 0
        lax.fori_loop(0, 2 * R // 16, body, 0)
        a_copy(m).start()
        stat_send(1 + ph, m)

    def phase_h(ph, m, l):
        gain = (ag_ref, mg_ref)[ph]
        stat_recv(1 + ph, m)
        a_copy(m).wait()

        def body(i, _):
            y = i // RC
            rows = pl.ds(pl.multiple_of(lax.rem(i, RC) * 16, 16), 16)
            arow = pl.ds(pl.multiple_of(i * 16, 16), 16)
            scale = jnp.concatenate([RSC[y, rows]] * 16, axis=1)
            X[m, y, rows] = (X[m, y, rows].astype(F32) + AF[m, arow].astype(F32) * scale * gain[pl.ds(l, 1)].astype(F32)).astype(BF)
            return 0
        lax.fori_loop(0, 2 * R // 16, body, 0)

    def c_copy(m, n, c0, w):
        return rc(C.at[m, ty, :, pl.ds(c0, w)], C.at[m, ty, :, pl.ds(c0, w)], c_ss.at[m, n], c_rs.at[m, n], ypeer)

    def c_tile(m, n, c0, w):
        for j in range(2):
            tile_copy(m, j, n, c0, w).wait()

        def body(i, _):
            rows = pl.ds(pl.multiple_of(i * 16, 16), 16)
            cols = pl.ds(c0, w)
            g = (GP[m, 0, ty, rows, cols].astype(F32) + GR[m, 0, rows, cols].astype(F32)).astype(BF).astype(F32)
            u = (GP[m, 1, ty, rows, cols].astype(F32) + GR[m, 1, rows, cols].astype(F32)).astype(BF).astype(F32)
            C[m, ty, rows, cols] = (jax.nn.silu(g) * u).astype(BF)
            return 0
        lax.fori_loop(0, R // 16, body, 0)
        c_copy(m, n, c0, w).start()

    def phase_c(m, lo, hi):
        def body(n, _):
            c_tile(m, n, pl.multiple_of(n * TW, TW), TW)
            return 0
        if lo < 5:
            lax.fori_loop(lo, min(hi, 5), body, 0)
        if hi == 6:
            c_tile(m, 5, 2560, 256)

    def y_copies(m):
        out = []
        for y in range(2):
            for t in range(T):
                out.append(lc(X.at[m, y, pl.ds(t * RB, RB)], y_ref.at[t, pl.ds(y * NB * RB + m * RB, RB)], y_sem.at[(m * 2 + y) * T + t]))
        return out

    wait(emb_copies())
    seen = set()
    for op, *arg in ORDER:
        if op == "Lg":
            start(gu_loads(arg[0]))
        elif op == "Lq":
            start(qkv_loads(arg[0]))
        elif op == "Lo":
            start(wo_loads(arg[0]))
        elif op == "Ld":
            start(wd_loads(arg[0]))
        elif op == "Q":
            m, l = arg
            phase_q(m, l, ("q", l) not in seen)
            seen.add(("q", l))
        elif op == "Qs":
            m, l, lo, hi = arg
            send_q(m, lo, hi)
        elif op == "S":
            phase_s(arg[0])
        elif op == "T":
            m, l = arg
            phase_t1(m, l)
            phase_t2(m, l)
        elif op == "O":
            m, l = arg
            if ("o", l) not in seen:
                wait(wo_loads(l))
                seen.add(("o", l))
            phase_o(m, l)
        elif op == "2":
            phase_2(arg[0], arg[1])
        elif op == "3":
            phase_3(arg[0], arg[1])
        elif op == "H":
            ph, m, l = arg
            phase_h(ph, m, l)
            if ph == 1 and l == L - 1:
                start(y_copies(m))
        elif op == "G":
            m, l = arg
            if ("g", l) not in seen:
                wait(gu_loads(l))
                seen.add(("g", l))
            phase_g(m)
        elif op == "Gs":
            m, l, lo, hi = arg
            send_g(m, lo, hi)
        elif op == "C":
            m, l, lo, hi = arg
            phase_c(m, lo, hi)
        elif op == "D":
            m, l = arg
            if ("d", l) not in seen:
                wait(wd_loads(l))
                seen.add(("d", l))
            phase_d(m, l)
    for m in range(NB):
        wait(y_copies(m))
    for m in range(NB):
        wait(ko_copies(L - 1, m))


def cache_kernel(start_ref, k_ref, v_ref, kn_ref, vn_ref, ko_ref, vo_ref):
    c = pl.program_id(1)
    ko_ref[...] = k_ref[...]
    vo_ref[...] = v_ref[...]
    for i in range(k_ref.shape[1]):
        p = start_ref[c * k_ref.shape[1] + i]
        for t in range(T):
            ko_ref[0, i, p + t] = kn_ref[0, i, t]
            vo_ref[0, i, p + t] = vn_ref[0, i, t]


def solution(mesh):
    act_spec = P(None, 'dp', 'tpy')
    cache_spec = P(None, ('dp', 'tpy'), None, 'tpx', None)
    col_spec = P(None, 'tpy', 'tpx')
    row_spec = P(None, 'tpx', 'tpy')
    head_gain = P(None, 'tpx')
    width_gain = P(None, 'tpy')

    def device_fn(embeds, start_pos, k_cache, v_cache, w_query, w_key, w_value, w_out, w_gate, w_up, w_down, q_gain, k_gain, attn_gain, mlp_gain):
        rows = NB * RB
        start_local = lax.dynamic_slice_in_dim(start_pos, lax.axis_index('tpy') * rows, rows)
        pos = (start_local.reshape(NB, 1, RB) + jnp.arange(T, dtype=jnp.int32)[None, :, None]).reshape(NB, R)
        inv_freq = jnp.power(THETA, jnp.arange(HEAD_DIM // 2, dtype=F32) * (-2.0 / HEAD_DIM))
        ang = pos.astype(F32)[..., None] * inv_freq
        cos_part, sin_part = jnp.cos(ang), jnp.sin(ang)
        cos2 = jnp.concatenate([cos_part, cos_part], axis=-1)
        sin2 = jnp.concatenate([-sin_part, sin_part], axis=-1)
        hbm = pl.BlockSpec(memory_space=pl.ANY)
        vm = pl.BlockSpec(memory_space=pltpu.VMEM)
        dma = pltpu.SemaphoreType.DMA
        y, kn, vn = pl.pallas_call(
            main_kernel,
            out_shape=[
                jax.ShapeDtypeStruct(embeds.shape, BF),
                jax.ShapeDtypeStruct((L, rows, T * HL, HEAD_DIM), BF),
                jax.ShapeDtypeStruct((L, rows, T * HL, HEAD_DIM), BF),
            ],
            in_specs=[pl.BlockSpec(memory_space=pltpu.SMEM)] + [hbm] * 10 + [vm] * 6,
            out_specs=[hbm] * 3,
            scratch_shapes=[
                pltpu.VMEM((NB, 2, R, DW), BF),
                pltpu.VMEM((2, FW, DW), BF),
                pltpu.VMEM((QW, DW), BF),
                pltpu.VMEM((FW, DW), BF),
                pltpu.VMEM((NB, 2, 2, R, FP), BF),
                pltpu.VMEM((NB, 2, R, FP), BF),
                pltpu.VMEM((NB, 2, R, FP), BF),
                pltpu.VMEM((NB, 2, R, QW), BF),
                pltpu.VMEM((T, RB, HL, HEAD_DIM), F32),
                pltpu.VMEM((T, RB, HL, HEAD_DIM), F32),
                pltpu.VMEM((T, RB, HL, HEAD_DIM), F32),
                pltpu.VMEM((T, RB, HL, HEAD_DIM), F32),
                pltpu.VMEM((NB, RB, T * HL, HEAD_DIM), BF),
                pltpu.VMEM((NB, RB, T * HL, HEAD_DIM), BF),
                pltpu.VMEM((SLOTS, CB, SH, HEAD_DIM), BF),
                pltpu.VMEM((SLOTS, CB, SH, HEAD_DIM), BF),
                pltpu.VMEM((NB, 2 * R, DW), BF),
                pltpu.VMEM((NB, 2 * R, HALF), BF),
                pltpu.VMEM((NB, 2 * R, HALF), BF),
                pltpu.VMEM((2, NB, 2 * R, HALF), BF),
                pltpu.VMEM((NB, 2 * R, DW), BF),
                pltpu.VMEM((2, R, 128), F32),
                pltpu.VMEM((2, R, 128), F32),
                pltpu.VMEM((3, NB, 8, 128), F32),
                pltpu.VMEM((3, NB, 3, 8, 128), F32),
                dma((NB * 2 * T,)), dma((6,)), dma((8,)), dma((1,)), dma((4,)), dma((2, SLOTS)), dma((2, NB)), dma((NB * 2 * T,)),
                dma((NB, 2, 6)), dma((NB, 2, 6)), dma((NB, 6)), dma((NB, 6)), dma((NB,)), dma((NB,)),
                dma((NB,)), dma((NB,)), dma((NB,)), dma((2, NB)), dma((NB,)), dma((NB,)), dma((3, NB, 3)), dma((3, NB, 3)),
            ],
            compiler_params=pltpu.CompilerParams(collective_id=0, has_side_effects=True, vmem_limit_bytes=67043328),
            name="layers",
        )(start_local, embeds, k_cache.reshape(L, rows, SH, HEAD_DIM), v_cache.reshape(L, rows, SH, HEAD_DIM),
          w_query, w_key, w_value, w_out, w_gate.transpose(0, 2, 1), w_up.transpose(0, 2, 1), w_down, q_gain, k_gain, attn_gain, mlp_gain, cos2, sin2)
        bc = 8
        big = pl.BlockSpec((1, bc, SEQ, HL, HEAD_DIM), lambda l, c, s: (l, c, 0, 0, 0))
        small = pl.BlockSpec((1, bc, T, HL, HEAD_DIM), lambda l, c, s: (l, c, 0, 0, 0))
        k_out, v_out = pl.pallas_call(
            cache_kernel,
            out_shape=[jax.ShapeDtypeStruct(k_cache.shape, BF)] * 2,
            grid_spec=pltpu.PrefetchScalarGridSpec(
                num_scalar_prefetch=1, grid=(L, rows // bc), in_specs=[big, big, small, small], out_specs=[big, big]),
            name="caches",
        )(start_local, k_cache, v_cache, kn.reshape(L, rows, T, HL, HEAD_DIM), vn.reshape(L, rows, T, HL, HEAD_DIM))
        return y, k_out, v_out

    return jax.shard_map(device_fn, mesh=mesh, in_specs=(act_spec, P('dp'), cache_spec, cache_spec, col_spec, col_spec, col_spec, row_spec, col_spec, col_spec, row_spec, head_gain, head_gain, width_gain, width_gain), out_specs=(act_spec, cache_spec, cache_spec), check_vma=False)
```

```python
import functools
import math
import jax
import jax.numpy as jnp
from jax import lax
from jax.experimental import pallas as pl
from jax.experimental.pallas import tpu as pltpu
from jax.sharding import PartitionSpec as P

HEAD_DIM = 128
EPS = 1e-6
THETA = 500000.0
SCORE_SCALE = 1.0 / math.sqrt(HEAD_DIM)
NEG_BIG = -1e30
MESH = pl.DeviceIdType.MESH
BF = jnp.bfloat16
F32 = jnp.float32

L = 2
T = 3
NB = 4
RB = 16
R = T * RB
HL = 8
DW = 2048
QW = HL * HEAD_DIM
FW = 2752
FP = 2816
SEQ = 64
SH = SEQ * HL
CB = 4
NCH = RB // CB
SLOTS = 4
TW = 512
HALF = DW // 2
RC = R // 16
GU_SENDS = [(0, 1024), (1024, 1024), (2048, 768)]
QKV_TILES = [(0, 0), (0, 512), (0, 1024), (0, 1536), (1, 0), (1, 512)]


ORDER = [
    ("Q", 0, 0),
    ("Qs", 0, 0, 0, 1),
    ("Q", 1, 0),
    ("Qs", 0, 0, 1, 2),
    ("Qs", 1, 0, 0, 1),
    ("Q", 2, 0),
    ("S", 0, 0),
    ("Qs", 1, 0, 1, 2),
    ("T", 0, 0),
    ("Q", 3, 0),
    ("Qs", 2, 0, 0, 1),
    ("S", 1, 0),
    ("Qs", 2, 0, 1, 2),
    ("O", 0, 0),
    ("2", 0, 0, 0),
    ("Lg", 0),
    ("T", 1, 0),
    ("Qs", 3, 0, 0, 1),
    ("S", 2, 0),
    ("O", 1, 0),
    ("3", 0, 0, 0),
    ("T", 2, 0),
    ("Qs", 3, 0, 1, 2),
    ("H", 0, 0, 0),
    ("G", 0, 0),
    ("Gs", 0, 0, 0, 1),
    ("O", 2, 0),
    ("2", 0, 1, 0),
    ("Gs", 0, 0, 1, 3),
    ("S", 3, 0),
    ("3", 0, 1, 0),
    ("2", 0, 2, 0),
    ("T", 3, 0),
    ("3", 0, 2, 0),
    ("C", 0, 0, 0, 2),
    ("H", 0, 1, 0),
    ("G", 1, 0),
    ("Gs", 1, 0, 0, 1),
    ("O", 3, 0),
    ("H", 0, 2, 0),
    ("G", 2, 0),
    ("C", 0, 0, 2, 3),
    ("Gs", 2, 0, 0, 1),
    ("D", 0, 0),
    ("Gs", 1, 0, 1, 2),
    ("2", 1, 0, 0),
    ("2", 0, 3, 0),
    ("C", 1, 0, 0, 1),
    ("Gs", 1, 0, 2, 3),
    ("C", 2, 0, 0, 1),
    ("3", 0, 3, 0),
    ("3", 1, 0, 0),
    ("C", 1, 0, 1, 2),
    ("Lo", 1),
    ("C", 1, 0, 2, 3),
    ("Gs", 2, 0, 1, 2),
    ("H", 0, 3, 0),
    ("G", 3, 0),
    ("Gs", 3, 0, 0, 1),
    ("D", 1, 0),
    ("Lq", 1),
    ("2", 1, 1, 0),
    ("Gs", 3, 0, 1, 2),
    ("H", 1, 0, 0),
    ("3", 1, 1, 0),
    ("Gs", 2, 0, 2, 3),
    ("Gs", 3, 0, 2, 3),
    ("C", 2, 0, 1, 3),
    ("C", 3, 0, 0, 1),
    ("Q", 0, 1),
    ("C", 3, 0, 1, 2),
    ("D", 2, 0),
    ("H", 1, 1, 0),
    ("2", 1, 2, 0),
    ("C", 3, 0, 2, 3),
    ("Q", 1, 1),
    ("Qs", 0, 1, 0, 2),
    ("D", 3, 0),
    ("3", 1, 2, 0),
    ("2", 1, 3, 0),
    ("Qs", 1, 1, 0, 2),
    ("S", 0, 1),
    ("T", 0, 1),
    ("H", 1, 2, 0),
    ("Q", 2, 1),
    ("3", 1, 3, 0),
    ("S", 1, 1),
    ("Qs", 2, 1, 0, 1),
    ("O", 0, 1),
    ("2", 0, 0, 1),
    ("Qs", 2, 1, 1, 2),
    ("H", 1, 3, 0),
    ("T", 1, 1),
    ("Q", 3, 1),
    ("Lg", 1),
    ("S", 2, 1),
    ("3", 0, 0, 1),
    ("Qs", 3, 1, 0, 2),
    ("O", 1, 1),
    ("2", 0, 1, 1),
    ("T", 2, 1),
    ("H", 0, 0, 1),
    ("G", 0, 1),
    ("Gs", 0, 1, 0, 1),
    ("3", 0, 1, 1),
    ("Gs", 0, 1, 1, 3),
    ("O", 2, 1),
    ("S", 3, 1),
    ("C", 0, 1, 0, 1),
    ("2", 0, 2, 1),
    ("H", 0, 1, 1),
    ("T", 3, 1),
    ("C", 0, 1, 1, 2),
    ("3", 0, 2, 1),
    ("Ld", 1),
    ("G", 1, 1),
    ("Gs", 1, 1, 0, 1),
    ("C", 0, 1, 2, 3),
    ("O", 3, 1),
    ("2", 0, 3, 1),
    ("Gs", 1, 1, 1, 2),
    ("H", 0, 2, 1),
    ("C", 1, 1, 0, 1),
    ("G", 2, 1),
    ("Gs", 2, 1, 0, 1),
    ("3", 0, 3, 1),
    ("Gs", 2, 1, 1, 2),
    ("H", 0, 3, 1),
    ("Gs", 1, 1, 2, 3),
    ("C", 1, 1, 1, 2),
    ("C", 2, 1, 0, 1),
    ("Gs", 2, 1, 2, 3),
    ("G", 3, 1),
    ("D", 0, 1),
    ("C", 2, 1, 1, 2),
    ("Gs", 3, 1, 0, 1),
    ("C", 1, 1, 2, 3),
    ("C", 2, 1, 2, 3),
    ("Gs", 3, 1, 1, 3),
    ("D", 2, 1),
    ("D", 1, 1),
    ("C", 3, 1, 0, 1),
    ("2", 1, 0, 1),
    ("2", 1, 1, 1),
    ("C", 3, 1, 1, 3),
    ("2", 1, 2, 1),
    ("D", 3, 1),
    ("3", 1, 0, 1),
    ("3", 1, 1, 1),
    ("2", 1, 3, 1),
    ("H", 1, 1, 1),
    ("3", 1, 2, 1),
    ("3", 1, 3, 1),
    ("H", 1, 2, 1),
    ("H", 1, 0, 1),
    ("H", 1, 3, 1),
]


def lane_fold(z):
    return jnp.broadcast_to(jnp.sum(z, axis=1, keepdims=True), (z.shape[0], 128))


def dot(a, b):
    return jnp.dot(a, b, preferred_element_type=F32)


def dot_t(a, b):
    return lax.dot_general(a, b, (((1,), (1,)), ((), ())), preferred_element_type=F32)


def main_kernel(start_ref, emb_ref, kc_ref, vc_ref, wq_ref, wk_ref, wv_ref, wo_ref, wg_ref, wu_ref, wd_ref,
                qg_ref, kg_ref, ag_ref, mg_ref, cos_ref, sin_ref,
                y_ref, kn_ref, vn_ref,
                X, W1, WO, WD, GP, GR, C, OB, QS, KS, VS, OS, KO, VO, KB, VB, XP, XC, XS, XR, AF, RSUM, RSC, ST, SR,
                in_sem, q_wsem, g_wsem, o_wsem, d_wsem, kv_sem, ko_sem, y_sem,
                g_ss, g_rs, c_ss, c_rs, o_ss, o_rs, p_ss, p_rs, x_ss, x_rs, a_ss, a_rs, st_ss, st_rs):
    ty = lax.axis_index("tpy")
    tx = lax.axis_index("tpx")
    core = lax.rem(tx, 2)
    oy = 1 - ty
    cx = tx + 1 - 2 * core
    xx = lax.rem(tx + 2, 4)
    dx = 3 - tx
    ypeer = {"tpy": oy}
    cpeer = {"tpx": cx}
    xpeer = {"tpx": xx}
    xdiag = {"tpx": dx}
    ydiag = {"tpy": oy, "tpx": cx}
    own_half = pl.ds(pl.multiple_of(core * HALF, HALF), HALF)
    oth_half = pl.ds(pl.multiple_of((1 - core) * HALF, HALF), HALF)

    def rc(src, dst, ss, rs, dev):
        return pltpu.make_async_remote_copy(src_ref=src, dst_ref=dst, send_sem=ss, recv_sem=rs, device_id=dev, device_id_type=MESH)

    def lc(src, dst, sem):
        return pltpu.make_async_copy(src, dst, sem)

    def emb_copies():
        out = []
        for m in range(NB):
            for y in range(2):
                for t in range(T):
                    out.append(lc(emb_ref.at[t, pl.ds(y * NB * RB + m * RB, RB)], X.at[m, y, pl.ds(t * RB, RB)], in_sem.at[(m * 2 + y) * T + t]))
        return out

    def qkv_load(l, n):
        j, c0 = QKV_TILES[n]
        src = (wq_ref, wk_ref, wv_ref)[n // 2]
        return lc(src.at[l, :, pl.ds((n % 2) * TW, TW)], W1.at[j, pl.ds(0, DW), pl.ds(c0, TW)], q_wsem.at[n])

    def qkv_loads(l):
        return [qkv_load(l, n) for n in range(6)]

    def gu_loads(l):
        return [lc((wg_ref, wu_ref)[j].at[l, pl.ds(r * 688, 688)], W1.at[j, pl.ds(r * 688, 688)], g_wsem.at[j * 4 + r]) for r in range(4) for j in range(2)]

    def wo_loads(l):
        return [lc(wo_ref.at[l], WO, o_wsem.at[0])]

    def wd_loads(l):
        return [lc(wd_ref.at[l, pl.ds(r * 688, 688)], WD.at[pl.ds(r * 688, 688)], d_wsem.at[r]) for r in range(4)]

    def start(copies):
        for cp in copies:
            cp.start()

    def wait(copies):
        for cp in copies:
            cp.wait()

    def kv_copies(l, m, c, slot):
        rows = pl.ds(m * RB + c * CB, CB)
        return [lc(kc_ref.at[l, rows], KB.at[slot], kv_sem.at[0, slot]), lc(vc_ref.at[l, rows], VB.at[slot], kv_sem.at[1, slot])]

    start(emb_copies())
    start(qkv_loads(0))

    barrier = pltpu.get_barrier_semaphore()
    for dev in (ypeer, cpeer, xpeer, xdiag, ydiag):
        pl.semaphore_signal(barrier, inc=1, device_id=dev, device_id_type=MESH)
    pl.semaphore_wait(barrier, 5)

    for c in range(SLOTS):
        start(kv_copies(0, 0, c, c))
    start(wo_loads(0))
    start(wd_loads(0))

    def q_copy(m, n):
        cols = pl.ds(0, (2 * QW, QW)[n])
        return rc(GP.at[m, n, oy, :, cols], GR.at[m, n, :, cols], g_ss.at[m, n], g_rs.at[m, n], ypeer)

    def g_copy(m, n):
        cols = pl.ds(*GU_SENDS[n])
        return rc(GP.at[m, :, oy, :, cols], GR.at[m, :, :, cols], g_ss.at[m, n], g_rs.at[m, n], ypeer)

    def compute_tile(m, j, c0, w, transposed=False):
        xm = X[m].reshape(2 * R, DW)
        if transposed:
            res = dot_t(xm, W1[j, pl.ds(c0, w), :]).astype(BF)
        else:
            res = dot(xm, W1[j, pl.ds(0, DW), pl.ds(c0, w)]).astype(BF)
        GP[m, j, :, :, pl.ds(c0, w)] = res.reshape(2, R, w)

    def phase_q(m, l, fresh):
        for j, cnt in ((0, 4), (1, 2)):
            if fresh:
                for i in range(cnt):
                    qkv_load(l, j * 4 + i).wait()

            def body(i, _):
                compute_tile(m, j, pl.multiple_of(i * TW, TW), TW)
                return 0
            lax.fori_loop(0, cnt, body, 0)

    def send_q(m, lo, hi):
        for n in range(lo, hi):
            q_copy(m, n).start()

    def phase_g(m):
        def body(i, _):
            for j in range(2):
                compute_tile(m, j, pl.multiple_of(i * TW, TW), TW, True)
            return 0
        lax.fori_loop(0, 5, body, 0)
        for j in range(2):
            compute_tile(m, j, 2560, 192, True)

    def send_g(m, lo, hi):
        for n in range(lo, hi):
            g_copy(m, n).start()

    def stat_copies(kind, m):
        peers = (cpeer, xpeer, xdiag) if kind == 0 else (cpeer, ypeer, ydiag)
        return [rc(ST.at[kind, m], SR.at[kind, m, k], st_ss.at[kind, m, k], st_rs.at[kind, m, k], peers[k]) for k in range(3)]

    def stat_send(kind, m):
        v0 = RSUM[0]
        v1 = RSUM[1]
        lane = lax.broadcasted_iota(jnp.int32, (R, 128), 1)
        both = jnp.where(lane == 0, v0, v1)
        full = jnp.concatenate([both, jnp.zeros((128 - R, 128), F32)], axis=0)
        ST[kind, m] = full.T[0:8]
        start(stat_copies(kind, m))

    def stat_recv(kind, m):
        wait(stat_copies(kind, m))
        total = (ST[kind, m] + SR[kind, m, 0]) + (SR[kind, m, 1] + SR[kind, m, 2])
        back = jnp.concatenate([total] * 16, axis=0).T
        scale = lax.rsqrt(back / 4096.0 + EPS)
        RSC[0] = jnp.broadcast_to(scale[0:R, 0:1], (R, 128))
        RSC[1] = jnp.broadcast_to(scale[0:R, 1:2], (R, 128))

    def phase_s(m):
        for n in range(2):
            q_copy(m, n).wait()

        def body(i, _):
            rows = pl.ds(pl.multiple_of(i * 16, 16), 16)
            qk = pl.ds(0, 2 * QW)
            z = (GP[m, 0, ty, rows, qk].astype(F32) + GR[m, 0, rows, qk].astype(F32)).astype(BF)
            GR[m, 0, rows, qk] = z
            zf = z.astype(F32)
            sq = zf * zf
            RSUM[0, rows] = lane_fold(sq[:, :QW])
            RSUM[1, rows] = lane_fold(sq[:, QW:])
            cols = pl.ds(0, QW)
            GR[m, 1, rows, cols] = (GP[m, 1, ty, rows, cols].astype(F32) + GR[m, 1, rows, cols].astype(F32)).astype(BF)
            return 0
        lax.fori_loop(0, R // 16, body, 0)
        stat_send(0, m)

    def phase_t1(m, l):
        stat_recv(0, m)

        gain = jnp.concatenate([qg_ref[pl.ds(l, 1)], kg_ref[pl.ds(l, 1)]], axis=1).astype(F32)
        low = lax.rem(lax.broadcasted_iota(jnp.int32, (16, 2 * QW), 1), HEAD_DIM) < HEAD_DIM // 2

        def body(i, _):
            rows = pl.ds(pl.multiple_of(i * 16, 16), 16)
            scale = jnp.concatenate([RSC[0, rows]] * HL + [RSC[1, rows]] * HL, axis=1)
            z = GR[m, 0, rows, pl.ds(0, 2 * QW)].astype(F32) * scale * gain
            turned = jnp.where(low, pltpu.roll(z, 2 * QW - HEAD_DIM // 2, 1), pltpu.roll(z, HEAD_DIM // 2, 1))
            rot = z * jnp.concatenate([cos_ref[m, rows]] * (2 * HL), axis=1) + turned * jnp.concatenate([sin_ref[m, rows]] * (2 * HL), axis=1)
            rot = rot.astype(BF).astype(F32)
            v = GR[m, 1, rows, pl.ds(0, QW)].astype(F32)
            for h in range(HL):
                QS[i, :, h, :] = rot[:, h * HEAD_DIM:(h + 1) * HEAD_DIM]
                KS[i, :, h, :] = rot[:, QW + h * HEAD_DIM:QW + (h + 1) * HEAD_DIM]
                VS[i, :, h, :] = v[:, h * HEAD_DIM:(h + 1) * HEAD_DIM]
            return 0
        lax.fori_loop(0, R // 16, body, 0)

    def ko_copies(l, m):
        rows = pl.ds(m * RB, RB)
        return [lc(KO.at[m], kn_ref.at[l, rows], ko_sem.at[0, m]), lc(VO.at[m], vn_ref.at[l, rows], ko_sem.at[1, m])]

    def o_copy(m):
        return rc(OB.at[m, ty], OB.at[m, ty], o_ss.at[m], o_rs.at[m], ypeer)

    def phase_t2(m, l):
        if l > 0:
            wait(ko_copies(l - 1, m))
        row = lax.broadcasted_iota(jnp.int32, (T * HL, SH), 0)
        col = lax.broadcasted_iota(jnp.int32, (T * HL, SH), 1)
        colm = jnp.where(lax.rem(row, HL) == lax.rem(col, HL), col, SH)
        rown = lax.broadcasted_iota(jnp.int32, (T * HL, T * HL), 0)
        coln = lax.broadcasted_iota(jnp.int32, (T * HL, T * HL), 1)
        newm = (lax.rem(rown, HL) == lax.rem(coln, HL)) & (coln <= rown)

        nxt = (l, m + 1) if m + 1 < NB else (l + 1, 0)

        def chunk(c, _):
            slot = c
            wait(kv_copies(l, m, c, slot))
            for k in range(CB):
                i = c * CB + k
                q = QS[:, i].reshape(T * HL, HEAD_DIM).astype(BF)
                kn = KS[:, i].reshape(T * HL, HEAD_DIM).astype(BF)
                vn = VS[:, i].reshape(T * HL, HEAD_DIM).astype(BF)
                limit = start_ref[m * RB + i] * HL
                s_old = jnp.where(colm < limit, dot_t(q, KB[slot, k]) * SCORE_SCALE, NEG_BIG)
                s_new = jnp.where(newm, dot_t(q, kn) * SCORE_SCALE, NEG_BIG)
                top = jnp.maximum(jnp.max(s_old, axis=1, keepdims=True), jnp.max(s_new, axis=1, keepdims=True))
                e_old = jnp.exp(s_old - top)
                e_new = jnp.exp(s_new - top)
                den = jnp.sum(e_old, axis=1, keepdims=True) + jnp.sum(e_new, axis=1, keepdims=True)
                o = dot((e_old / den).astype(BF), VB[slot, k]) + dot((e_new / den).astype(BF), vn)
                OS[:, i] = o.reshape(T, HL, HEAD_DIM)
                KO[m, i] = kn
                VO[m, i] = vn
            if nxt[0] < L:
                start(kv_copies(nxt[0], nxt[1], c, slot))
            return 0
        lax.fori_loop(0, NCH, chunk, 0)
        start(ko_copies(l, m))

        def body(i, _):
            rows = pl.ds(pl.multiple_of(i * 16, 16), 16)
            for h in range(8):
                OB[m, ty, rows, pl.ds(h * 128, 128)] = OS[i, :, h, :].astype(BF)
            return 0
        lax.fori_loop(0, R // 16, body, 0)
        o_copy(m).start()

    def p_copy(m):
        return rc(XP.at[m, :, oth_half], XC.at[m], p_ss.at[m], p_rs.at[m], cpeer)

    def x_copy(ph, m):
        return rc(XS.at[m], XR.at[ph, m], x_ss.at[m], x_rs.at[ph, m], xpeer)

    def a_copy(m):
        return rc(AF.at[m, :, own_half], AF.at[m, :, own_half], a_ss.at[m], a_rs.at[m], cpeer)

    def phase_o(m, l):
        o_copy(m).wait()
        for half in (1 - core, core):
            def body(i, _):
                cols = pl.ds(pl.multiple_of(half * HALF + i * TW, TW), TW)
                XP[m, :, cols] = dot(OB[m].reshape(2 * R, QW), WO[:, cols]).astype(BF)
                return 0
            lax.fori_loop(0, 2, body, 0)
            if half is not core:
                p_copy(m).start()

    def phase_d(m, l):
        for n in range(3):
            c_copy(m, n).wait()
        for half in (1 - core, core):
            def body(i, _):
                cols = pl.ds(pl.multiple_of(half * HALF + i * TW, TW), TW)
                cm = C[m].reshape(2 * R, FP)
                XP[m, :, cols] = dot(cm[:, :FW], WD[:, cols]).astype(BF)
                return 0
            lax.fori_loop(0, 2, body, 0)
            if half is not core:
                p_copy(m).start()

    def phase_2(ph, m):
        p_copy(m).wait()

        def body(i, _):
            rows = pl.ds(pl.multiple_of(i * 16, 16), 16)
            XS[m, rows] = (XP[m, rows, own_half].astype(F32) + XC[m, rows].astype(F32)).astype(BF)
            return 0
        lax.fori_loop(0, 2 * R // 16, body, 0)
        x_copy(ph, m).start()

    def phase_3(ph, m):
        x_copy(ph, m).wait()

        def body(i, _):
            rows = pl.ds(pl.multiple_of(i * 16, 16), 16)
            z = (XS[m, rows].astype(F32) + XR[ph, m, rows].astype(F32)).astype(BF)
            AF[m, rows, own_half] = z
            zf = z.astype(F32)
            acc = lane_fold(zf * zf)
            RSUM[i // RC, pl.ds(pl.multiple_of(lax.rem(i, RC) * 16, 16), 16)] = acc
            return 0
        lax.fori_loop(0, 2 * R // 16, body, 0)
        a_copy(m).start()
        stat_send(1 + ph, m)

    def phase_h(ph, m, l):
        gain = (ag_ref, mg_ref)[ph]
        stat_recv(1 + ph, m)
        a_copy(m).wait()

        def body(i, _):
            y = i // RC
            rows = pl.ds(pl.multiple_of(lax.rem(i, RC) * 16, 16), 16)
            arow = pl.ds(pl.multiple_of(i * 16, 16), 16)
            scale = jnp.concatenate([RSC[y, rows]] * 16, axis=1)
            X[m, y, rows] = (X[m, y, rows].astype(F32) + AF[m, arow].astype(F32) * scale * gain[pl.ds(l, 1)].astype(F32)).astype(BF)
            return 0
        lax.fori_loop(0, 2 * R // 16, body, 0)

    def c_copy(m, n):
        cols = pl.ds(*GU_SENDS[n])
        return rc(C.at[m, ty, :, cols], C.at[m, ty, :, cols], c_ss.at[m, n], c_rs.at[m, n], ypeer)

    def phase_c(m, lo, hi):
        for n in range(lo, hi):
            g_copy(m, n).wait()

            def body(i, _):
                rows = pl.ds(pl.multiple_of(i * 16, 16), 16)
                cols = pl.ds(*GU_SENDS[n])
                g = (GP[m, 0, ty, rows, cols].astype(F32) + GR[m, 0, rows, cols].astype(F32)).astype(BF).astype(F32)
                u = (GP[m, 1, ty, rows, cols].astype(F32) + GR[m, 1, rows, cols].astype(F32)).astype(BF).astype(F32)
                C[m, ty, rows, cols] = (jax.nn.silu(g) * u).astype(BF)
                return 0
            lax.fori_loop(0, R // 16, body, 0)
            c_copy(m, n).start()

    def y_copies(m):
        out = []
        for y in range(2):
            for t in range(T):
                out.append(lc(X.at[m, y, pl.ds(t * RB, RB)], y_ref.at[t, pl.ds(y * NB * RB + m * RB, RB)], y_sem.at[(m * 2 + y) * T + t]))
        return out

    wait(emb_copies())
    seen = set()
    for op, *arg in ORDER:
        if op == "Lg":
            start(gu_loads(arg[0]))
        elif op == "Lq":
            start(qkv_loads(arg[0]))
        elif op == "Lo":
            start(wo_loads(arg[0]))
        elif op == "Ld":
            start(wd_loads(arg[0]))
        elif op == "Q":
            m, l = arg
            phase_q(m, l, ("q", l) not in seen)
            seen.add(("q", l))
        elif op == "Qs":
            m, l, lo, hi = arg
            send_q(m, lo, hi)
        elif op == "S":
            phase_s(arg[0])
        elif op == "T":
            m, l = arg
            phase_t1(m, l)
            phase_t2(m, l)
        elif op == "O":
            m, l = arg
            if ("o", l) not in seen:
                wait(wo_loads(l))
                seen.add(("o", l))
            phase_o(m, l)
        elif op == "2":
            phase_2(arg[0], arg[1])
        elif op == "3":
            phase_3(arg[0], arg[1])
        elif op == "H":
            ph, m, l = arg
            phase_h(ph, m, l)
            if ph == 1 and l == L - 1:
                start(y_copies(m))
        elif op == "G":
            m, l = arg
            if ("g", l) not in seen:
                wait(gu_loads(l))
                seen.add(("g", l))
            phase_g(m)
        elif op == "Gs":
            m, l, lo, hi = arg
            send_g(m, lo, hi)
        elif op == "C":
            m, l, lo, hi = arg
            phase_c(m, lo, hi)
        elif op == "D":
            m, l = arg
            if ("d", l) not in seen:
                wait(wd_loads(l))
                seen.add(("d", l))
            phase_d(m, l)
    for m in range(NB):
        wait(y_copies(m))
    for m in range(NB):
        wait(ko_copies(L - 1, m))


def cache_kernel(start_ref, k_ref, v_ref, kn_ref, vn_ref, ko_ref, vo_ref):
    c = pl.program_id(1)
    ko_ref[...] = k_ref[...]
    vo_ref[...] = v_ref[...]
    for i in range(k_ref.shape[1]):
        p = start_ref[c * k_ref.shape[1] + i]
        for t in range(T):
            ko_ref[0, i, p + t] = kn_ref[0, i, t]
            vo_ref[0, i, p + t] = vn_ref[0, i, t]


def solution(mesh):
    act_spec = P(None, 'dp', 'tpy')
    cache_spec = P(None, ('dp', 'tpy'), None, 'tpx', None)
    col_spec = P(None, 'tpy', 'tpx')
    row_spec = P(None, 'tpx', 'tpy')
    head_gain = P(None, 'tpx')
    width_gain = P(None, 'tpy')

    def device_fn(embeds, start_pos, k_cache, v_cache, w_query, w_key, w_value, w_out, w_gate, w_up, w_down, q_gain, k_gain, attn_gain, mlp_gain):
        rows = NB * RB
        start_local = lax.dynamic_slice_in_dim(start_pos, lax.axis_index('tpy') * rows, rows)
        pos = (start_local.reshape(NB, 1, RB) + jnp.arange(T, dtype=jnp.int32)[None, :, None]).reshape(NB, R)
        inv_freq = jnp.power(THETA, jnp.arange(HEAD_DIM // 2, dtype=F32) * (-2.0 / HEAD_DIM))
        ang = pos.astype(F32)[..., None] * inv_freq
        cos_part, sin_part = jnp.cos(ang), jnp.sin(ang)
        cos2 = jnp.concatenate([cos_part, cos_part], axis=-1)
        sin2 = jnp.concatenate([-sin_part, sin_part], axis=-1)
        hbm = pl.BlockSpec(memory_space=pl.ANY)
        vm = pl.BlockSpec(memory_space=pltpu.VMEM)
        dma = pltpu.SemaphoreType.DMA
        y, kn, vn = pl.pallas_call(
            main_kernel,
            out_shape=[
                jax.ShapeDtypeStruct(embeds.shape, BF),
                jax.ShapeDtypeStruct((L, rows, T * HL, HEAD_DIM), BF),
                jax.ShapeDtypeStruct((L, rows, T * HL, HEAD_DIM), BF),
            ],
            in_specs=[pl.BlockSpec(memory_space=pltpu.SMEM)] + [hbm] * 10 + [vm] * 6,
            out_specs=[hbm] * 3,
            scratch_shapes=[
                pltpu.VMEM((NB, 2, R, DW), BF),
                pltpu.VMEM((2, FW, DW), BF),
                pltpu.VMEM((QW, DW), BF),
                pltpu.VMEM((FW, DW), BF),
                pltpu.VMEM((NB, 2, 2, R, FP), BF),
                pltpu.VMEM((NB, 2, R, FP), BF),
                pltpu.VMEM((NB, 2, R, FP), BF),
                pltpu.VMEM((NB, 2, R, QW), BF),
                pltpu.VMEM((T, RB, HL, HEAD_DIM), F32),
                pltpu.VMEM((T, RB, HL, HEAD_DIM), F32),
                pltpu.VMEM((T, RB, HL, HEAD_DIM), F32),
                pltpu.VMEM((T, RB, HL, HEAD_DIM), F32),
                pltpu.VMEM((NB, RB, T * HL, HEAD_DIM), BF),
                pltpu.VMEM((NB, RB, T * HL, HEAD_DIM), BF),
                pltpu.VMEM((SLOTS, CB, SH, HEAD_DIM), BF),
                pltpu.VMEM((SLOTS, CB, SH, HEAD_DIM), BF),
                pltpu.VMEM((NB, 2 * R, DW), BF),
                pltpu.VMEM((NB, 2 * R, HALF), BF),
                pltpu.VMEM((NB, 2 * R, HALF), BF),
                pltpu.VMEM((2, NB, 2 * R, HALF), BF),
                pltpu.VMEM((NB, 2 * R, DW), BF),
                pltpu.VMEM((2, R, 128), F32),
                pltpu.VMEM((2, R, 128), F32),
                pltpu.VMEM((3, NB, 8, 128), F32),
                pltpu.VMEM((3, NB, 3, 8, 128), F32),
                dma((NB * 2 * T,)), dma((6,)), dma((8,)), dma((1,)), dma((4,)), dma((2, SLOTS)), dma((2, NB)), dma((NB * 2 * T,)),
                dma((NB, 3)), dma((NB, 3)), dma((NB, 3)), dma((NB, 3)), dma((NB,)), dma((NB,)),
                dma((NB,)), dma((NB,)), dma((NB,)), dma((2, NB)), dma((NB,)), dma((NB,)), dma((3, NB, 3)), dma((3, NB, 3)),
            ],
            compiler_params=pltpu.CompilerParams(collective_id=0, has_side_effects=True, vmem_limit_bytes=67043328),
            name="layers",
        )(start_local, embeds, k_cache.reshape(L, rows, SH, HEAD_DIM), v_cache.reshape(L, rows, SH, HEAD_DIM),
          w_query, w_key, w_value, w_out, w_gate.transpose(0, 2, 1), w_up.transpose(0, 2, 1), w_down, q_gain, k_gain, attn_gain, mlp_gain, cos2, sin2)
        bc = 8
        big = pl.BlockSpec((1, bc, SEQ, HL, HEAD_DIM), lambda l, c, s: (l, c, 0, 0, 0))
        small = pl.BlockSpec((1, bc, T, HL, HEAD_DIM), lambda l, c, s: (l, c, 0, 0, 0))
        k_out, v_out = pl.pallas_call(
            cache_kernel,
            out_shape=[jax.ShapeDtypeStruct(k_cache.shape, BF)] * 2,
            grid_spec=pltpu.PrefetchScalarGridSpec(
                num_scalar_prefetch=1, grid=(L, rows // bc), in_specs=[big, big, small, small], out_specs=[big, big]),
            name="caches",
        )(start_local, k_cache, v_cache, kn.reshape(L, rows, T, HL, HEAD_DIM), vn.reshape(L, rows, T, HL, HEAD_DIM))
        return y, k_out, v_out

    return jax.shard_map(device_fn, mesh=mesh, in_specs=(act_spec, P('dp'), cache_spec, cache_spec, col_spec, col_spec, col_spec, row_spec, col_spec, col_spec, row_spec, head_gain, head_gain, width_gain, width_gain), out_specs=(act_spec, cache_spec, cache_spec), check_vma=False)
```

```python
import functools
import math
import jax
import jax.numpy as jnp
from jax import lax
from jax.experimental import pallas as pl
from jax.experimental.pallas import tpu as pltpu
from jax.sharding import PartitionSpec as P

HEAD_DIM = 128
EPS = 1e-6
THETA = 500000.0
SCORE_SCALE = 1.0 / math.sqrt(HEAD_DIM)
NEG_BIG = -1e30
MESH = pl.DeviceIdType.MESH
BF = jnp.bfloat16
F32 = jnp.float32

L = 2
T = 3
NB = 4
RB = 16
R = T * RB
HL = 8
DW = 2048
QW = HL * HEAD_DIM
FW = 2752
FP = 2816
SEQ = 64
SH = SEQ * HL
CB = 4
NCH = RB // CB
SLOTS = 4
TW = 512
HALF = DW // 2
RC = R // 16
GU_SENDS = [(0, 1024), (1024, 1024), (2048, 768)]
QKV_TILES = [(0, 0), (0, 512), (0, 1024), (0, 1536), (1, 0), (1, 512)]


ORDER = [
    ("Q", 0, 0),
    ("Qs", 0, 0, 0, 2),
    ("Q", 2, 0),
    ("Q", 1, 0),
    ("Qs", 1, 0, 0, 1),
    ("Q", 3, 0),
    ("S", 0, 0),
    ("Qs", 1, 0, 1, 2),
    ("Lg", 0),
    ("Qs", 2, 0, 0, 1),
    ("T", 0, 0),
    ("S", 1, 0),
    ("Qs", 2, 0, 1, 2),
    ("T", 1, 0),
    ("O", 0, 0),
    ("S", 2, 0),
    ("2", 0, 0, 0),
    ("T", 2, 0),
    ("O", 1, 0),
    ("3", 0, 0, 0),
    ("2", 0, 1, 0),
    ("Qs", 3, 0, 0, 1),
    ("H", 0, 0, 0),
    ("Qs", 3, 0, 1, 2),
    ("G", 0, 0),
    ("Gs", 0, 0, 0, 1),
    ("S", 3, 0),
    ("3", 0, 1, 0),
    ("O", 2, 0),
    ("Gs", 0, 0, 1, 2),
    ("T", 3, 0),
    ("H", 0, 1, 0),
    ("2", 0, 2, 0),
    ("C", 0, 0, 0, 1),
    ("Gs", 0, 0, 2, 3),
    ("C", 0, 0, 1, 2),
    ("G", 1, 0),
    ("C", 0, 0, 2, 3),
    ("3", 0, 2, 0),
    ("O", 3, 0),
    ("Gs", 1, 0, 0, 3),
    ("H", 0, 2, 0),
    ("2", 0, 3, 0),
    ("G", 2, 0),
    ("C", 1, 0, 0, 1),
    ("Gs", 2, 0, 0, 1),
    ("C", 1, 0, 1, 2),
    ("3", 0, 3, 0),
    ("C", 1, 0, 2, 3),
    ("D", 0, 0),
    ("2", 1, 0, 0),
    ("Gs", 2, 0, 1, 3),
    ("C", 2, 0, 0, 1),
    ("H", 0, 3, 0),
    ("3", 1, 0, 0),
    ("G", 3, 0),
    ("C", 2, 0, 1, 2),
    ("Gs", 3, 0, 0, 1),
    ("Lq", 1),
    ("D", 1, 0),
    ("2", 1, 1, 0),
    ("H", 1, 0, 0),
    ("C", 2, 0, 2, 3),
    ("Gs", 3, 0, 1, 2),
    ("Q", 0, 1),
    ("Qs", 0, 1, 0, 1),
    ("D", 2, 0),
    ("2", 1, 2, 0),
    ("3", 1, 1, 0),
    ("Qs", 0, 1, 1, 2),
    ("Gs", 3, 0, 2, 3),
    ("C", 3, 0, 0, 1),
    ("H", 1, 1, 0),
    ("S", 0, 1),
    ("C", 3, 0, 1, 2),
    ("3", 1, 2, 0),
    ("Q", 1, 1),
    ("C", 3, 0, 2, 3),
    ("Qs", 1, 1, 0, 2),
    ("T", 0, 1),
    ("H", 1, 2, 0),
    ("D", 3, 0),
    ("2", 1, 3, 0),
    ("Lo", 1),
    ("Q", 2, 1),
    ("Qs", 2, 1, 0, 1),
    ("S", 1, 1),
    ("O", 0, 1),
    ("3", 1, 3, 0),
    ("Qs", 2, 1, 1, 2),
    ("T", 1, 1),
    ("2", 0, 0, 1),
    ("H", 1, 3, 0),
    ("Q", 3, 1),
    ("Lg", 1),
    ("S", 2, 1),
    ("O", 1, 1),
    ("3", 0, 0, 1),
    ("Qs", 3, 1, 0, 1),
    ("T", 2, 1),
    ("Qs", 3, 1, 1, 2),
    ("2", 0, 1, 1),
    ("H", 0, 0, 1),
    ("G", 0, 1),
    ("Ld", 1),
    ("Gs", 0, 1, 0, 1),
    ("O", 2, 1),
    ("S", 3, 1),
    ("Gs", 0, 1, 1, 2),
    ("3", 0, 1, 1),
    ("2", 0, 2, 1),
    ("T", 3, 1),
    ("C", 0, 1, 0, 1),
    ("3", 0, 2, 1),
    ("C", 0, 1, 1, 2),
    ("Gs", 0, 1, 2, 3),
    ("H", 0, 1, 1),
    ("G", 1, 1),
    ("Gs", 1, 1, 0, 3),
    ("O", 3, 1),
    ("2", 0, 3, 1),
    ("H", 0, 2, 1),
    ("G", 2, 1),
    ("Gs", 2, 1, 0, 1),
    ("C", 1, 1, 0, 1),
    ("3", 0, 3, 1),
    ("Gs", 2, 1, 1, 2),
    ("C", 0, 1, 2, 3),
    ("H", 0, 3, 1),
    ("C", 1, 1, 1, 3),
    ("C", 2, 1, 0, 1),
    ("G", 3, 1),
    ("Gs", 2, 1, 2, 3),
    ("Gs", 3, 1, 0, 1),
    ("D", 0, 1),
    ("C", 2, 1, 1, 2),
    ("Gs", 3, 1, 1, 2),
    ("D", 1, 1),
    ("2", 1, 0, 1),
    ("C", 2, 1, 2, 3),
    ("2", 1, 1, 1),
    ("Gs", 3, 1, 2, 3),
    ("C", 3, 1, 0, 2),
    ("D", 2, 1),
    ("2", 1, 2, 1),
    ("C", 3, 1, 2, 3),
    ("3", 1, 0, 1),
    ("3", 1, 1, 1),
    ("D", 3, 1),
    ("2", 1, 3, 1),
    ("H", 1, 1, 1),
    ("H", 1, 0, 1),
    ("3", 1, 2, 1),
    ("3", 1, 3, 1),
    ("H", 1, 2, 1),
    ("H", 1, 3, 1),
]


def lane_fold(z):
    return jnp.broadcast_to(jnp.sum(z, axis=1, keepdims=True), (z.shape[0], 128))


def dot(a, b):
    return jnp.dot(a, b, preferred_element_type=F32)


def dot_t(a, b):
    return lax.dot_general(a, b, (((1,), (1,)), ((), ())), preferred_element_type=F32)


def main_kernel(start_ref, emb_ref, kc_ref, vc_ref, wq_ref, wk_ref, wv_ref, wo_ref, wg_ref, wu_ref, wd_ref,
                qg_ref, kg_ref, ag_ref, mg_ref, cos_ref, sin_ref,
                y_ref, kn_ref, vn_ref,
                X, W1, WO, WD, GP, GR, C, OB, QS, KS, VS, OS, KO, VO, KB, VB, XP, XC, XS, XR, AF, RSUM, RSC, ST, SR,
                in_sem, q_wsem, g_wsem, o_wsem, d_wsem, kv_sem, ko_sem, y_sem,
                g_ss, g_rs, c_ss, c_rs, o_ss, o_rs, p_ss, p_rs, x_ss, x_rs, a_ss, a_rs, st_ss, st_rs):
    ty = lax.axis_index("tpy")
    tx = lax.axis_index("tpx")
    core = lax.rem(tx, 2)
    oy = 1 - ty
    cx = tx + 1 - 2 * core
    xx = lax.rem(tx + 2, 4)
    dx = 3 - tx
    ypeer = {"tpy": oy}
    cpeer = {"tpx": cx}
    xpeer = {"tpx": xx}
    xdiag = {"tpx": dx}
    ydiag = {"tpy": oy, "tpx": cx}
    own_half = pl.ds(pl.multiple_of(core * HALF, HALF), HALF)
    oth_half = pl.ds(pl.multiple_of((1 - core) * HALF, HALF), HALF)

    def rc(src, dst, ss, rs, dev):
        return pltpu.make_async_remote_copy(src_ref=src, dst_ref=dst, send_sem=ss, recv_sem=rs, device_id=dev, device_id_type=MESH)

    def lc(src, dst, sem):
        return pltpu.make_async_copy(src, dst, sem)

    def emb_copies():
        out = []
        for m in range(NB):
            for y in range(2):
                for t in range(T):
                    out.append(lc(emb_ref.at[t, pl.ds(y * NB * RB + m * RB, RB)], X.at[m, y, pl.ds(t * RB, RB)], in_sem.at[(m * 2 + y) * T + t]))
        return out

    def qkv_load(l, n):
        j, c0 = QKV_TILES[n]
        src = (wq_ref, wk_ref, wv_ref)[n // 2]
        return lc(src.at[l, :, pl.ds((n % 2) * TW, TW)], W1.at[j, pl.ds(0, DW), pl.ds(c0, TW)], q_wsem.at[n])

    def qkv_loads(l):
        return [qkv_load(l, n) for n in range(6)]

    def gu_loads(l):
        return [lc((wg_ref, wu_ref)[j].at[l, pl.ds(r * 688, 688)], W1.at[j, pl.ds(r * 688, 688)], g_wsem.at[j * 4 + r]) for r in range(4) for j in range(2)]

    def wo_loads(l):
        return [lc(wo_ref.at[l], WO, o_wsem.at[0])]

    def wd_loads(l):
        return [lc(wd_ref.at[l, pl.ds(r * 688, 688)], WD.at[pl.ds(r * 688, 688)], d_wsem.at[r]) for r in range(4)]

    def start(copies):
        for cp in copies:
            cp.start()

    def wait(copies):
        for cp in copies:
            cp.wait()

    def kv_copies(l, m, c, slot):
        rows = pl.ds(m * RB + c * CB, CB)
        return [lc(kc_ref.at[l, rows], KB.at[slot], kv_sem.at[0, slot]), lc(vc_ref.at[l, rows], VB.at[slot], kv_sem.at[1, slot])]

    start(emb_copies())
    start(qkv_loads(0))

    barrier = pltpu.get_barrier_semaphore()
    for dev in (ypeer, cpeer, xpeer, xdiag, ydiag):
        pl.semaphore_signal(barrier, inc=1, device_id=dev, device_id_type=MESH)
    pl.semaphore_wait(barrier, 5)

    for c in range(SLOTS):
        start(kv_copies(0, 0, c, c))
    start(wo_loads(0))
    start(wd_loads(0))

    def q_copy(m, n):
        cols = pl.ds(0, (2 * QW, QW)[n])
        return rc(GP.at[m, n, oy, :, cols], GR.at[m, n, :, cols], g_ss.at[m, n], g_rs.at[m, n], ypeer)

    def g_copy(m, n):
        cols = pl.ds(*GU_SENDS[n])
        return rc(GP.at[m, :, oy, :, cols], GR.at[m, :, :, cols], g_ss.at[m, n], g_rs.at[m, n], ypeer)

    def compute_tile(m, j, c0, w, transposed=False):
        xm = X[m].reshape(2 * R, DW)
        if transposed:
            res = dot_t(xm, W1[j, pl.ds(c0, w), :]).astype(BF)
        else:
            res = dot(xm, W1[j, pl.ds(0, DW), pl.ds(c0, w)]).astype(BF)
        GP[m, j, :, :, pl.ds(c0, w)] = res.reshape(2, R, w)

    def phase_q(m, l, fresh):
        for j, cnt in ((0, 4), (1, 2)):
            if fresh:
                for i in range(cnt):
                    qkv_load(l, j * 4 + i).wait()

            def body(i, _):
                compute_tile(m, j, pl.multiple_of(i * TW, TW), TW)
                return 0
            lax.fori_loop(0, cnt, body, 0)

    def send_q(m, lo, hi):
        for n in range(lo, hi):
            q_copy(m, n).start()

    def phase_g(m):
        def body(i, _):
            for j in range(2):
                compute_tile(m, j, pl.multiple_of(i * TW, TW), TW, True)
            return 0
        lax.fori_loop(0, 5, body, 0)
        for j in range(2):
            compute_tile(m, j, 2560, 192, True)

    def send_g(m, lo, hi):
        for n in range(lo, hi):
            g_copy(m, n).start()

    def stat_copies(kind, m):
        peers = (cpeer, xpeer, xdiag) if kind == 0 else (cpeer, ypeer, ydiag)
        return [rc(ST.at[kind, m], SR.at[kind, m, k], st_ss.at[kind, m, k], st_rs.at[kind, m, k], peers[k]) for k in range(3)]

    def stat_send(kind, m):
        v0 = RSUM[0]
        v1 = RSUM[1]
        lane = lax.broadcasted_iota(jnp.int32, (R, 128), 1)
        both = jnp.where(lane == 0, v0, v1)
        full = jnp.concatenate([both, jnp.zeros((128 - R, 128), F32)], axis=0)
        ST[kind, m] = full.T[0:8]
        start(stat_copies(kind, m))

    def stat_recv(kind, m):
        wait(stat_copies(kind, m))
        total = (ST[kind, m] + SR[kind, m, 0]) + (SR[kind, m, 1] + SR[kind, m, 2])
        back = jnp.concatenate([total] * 16, axis=0).T
        scale = lax.rsqrt(back / 4096.0 + EPS)
        RSC[0] = jnp.broadcast_to(scale[0:R, 0:1], (R, 128))
        RSC[1] = jnp.broadcast_to(scale[0:R, 1:2], (R, 128))

    def phase_s(m):
        for n in range(2):
            q_copy(m, n).wait()

        def body(i, _):
            rows = pl.ds(pl.multiple_of(i * 16, 16), 16)
            qk = pl.ds(0, 2 * QW)
            z = (GP[m, 0, ty, rows, qk].astype(F32) + GR[m, 0, rows, qk].astype(F32)).astype(BF)
            GR[m, 0, rows, qk] = z
            zf = z.astype(F32)
            sq = zf * zf
            RSUM[0, rows] = lane_fold(sq[:, :QW])
            RSUM[1, rows] = lane_fold(sq[:, QW:])
            cols = pl.ds(0, QW)
            GR[m, 1, rows, cols] = (GP[m, 1, ty, rows, cols].astype(F32) + GR[m, 1, rows, cols].astype(F32)).astype(BF)
            return 0
        lax.fori_loop(0, R // 16, body, 0)
        stat_send(0, m)

    def phase_t1(m, l):
        stat_recv(0, m)

        gain = jnp.concatenate([qg_ref[pl.ds(l, 1)], kg_ref[pl.ds(l, 1)]], axis=1).astype(F32)
        low = lax.rem(lax.broadcasted_iota(jnp.int32, (RB, 2 * QW), 1), HEAD_DIM) < HEAD_DIM // 2

        def body(i, _):
            rows = pl.ds(pl.multiple_of(i * RB, RB), RB)
            scale = jnp.concatenate([RSC[0, rows]] * HL + [RSC[1, rows]] * HL, axis=1)
            z = GR[m, 0, rows, pl.ds(0, 2 * QW)].astype(F32) * scale * gain
            turned = jnp.where(low, pltpu.roll(z, 2 * QW - HEAD_DIM // 2, 1), pltpu.roll(z, HEAD_DIM // 2, 1))
            rot = z * jnp.concatenate([cos_ref[ty, m, rows]] * (2 * HL), axis=1) + turned * jnp.concatenate([sin_ref[ty, m, rows]] * (2 * HL), axis=1)
            rot = rot.astype(BF).astype(F32)
            v = GR[m, 1, rows, pl.ds(0, QW)].astype(F32)
            for h in range(HL):
                QS[i, :, h, :] = rot[:, h * HEAD_DIM:(h + 1) * HEAD_DIM]
                KS[i, :, h, :] = rot[:, QW + h * HEAD_DIM:QW + (h + 1) * HEAD_DIM]
                VS[i, :, h, :] = v[:, h * HEAD_DIM:(h + 1) * HEAD_DIM]
            return 0
        lax.fori_loop(0, T, body, 0)

    def ko_copies(l, m):
        rows = pl.ds(m * RB, RB)
        return [lc(KO.at[m], kn_ref.at[l, rows], ko_sem.at[0, m]), lc(VO.at[m], vn_ref.at[l, rows], ko_sem.at[1, m])]

    def o_copy(m):
        return rc(OB.at[m, ty], OB.at[m, ty], o_ss.at[m], o_rs.at[m], ypeer)

    def phase_t2(m, l):
        if l > 0:
            wait(ko_copies(l - 1, m))
        row = lax.broadcasted_iota(jnp.int32, (T * HL, SH), 0)
        col = lax.broadcasted_iota(jnp.int32, (T * HL, SH), 1)
        colm = jnp.where(lax.rem(row, HL) == lax.rem(col, HL), col, SH)
        rown = lax.broadcasted_iota(jnp.int32, (T * HL, T * HL), 0)
        coln = lax.broadcasted_iota(jnp.int32, (T * HL, T * HL), 1)
        newm = (lax.rem(rown, HL) == lax.rem(coln, HL)) & (coln <= rown)

        nxt = (l, m + 1) if m + 1 < NB else (l + 1, 0)

        def chunk(c, _):
            slot = lax.rem(c, SLOTS)
            wait(kv_copies(l, m, c, slot))
            for k in range(CB):
                i = c * CB + k
                q = QS[:, i].reshape(T * HL, HEAD_DIM).astype(BF)
                kn = KS[:, i].reshape(T * HL, HEAD_DIM).astype(BF)
                vn = VS[:, i].reshape(T * HL, HEAD_DIM).astype(BF)
                limit = start_ref[ty * NB * RB + m * RB + i] * HL
                s_old = jnp.where(colm < limit, dot_t(q, KB[slot, k]) * SCORE_SCALE, NEG_BIG)
                s_new = jnp.where(newm, dot_t(q, kn) * SCORE_SCALE, NEG_BIG)
                top = jnp.maximum(jnp.max(s_old, axis=1, keepdims=True), jnp.max(s_new, axis=1, keepdims=True))
                e_old = jnp.exp(s_old - top)
                e_new = jnp.exp(s_new - top)
                den = jnp.sum(e_old, axis=1, keepdims=True) + jnp.sum(e_new, axis=1, keepdims=True)
                o = dot((e_old / den).astype(BF), VB[slot, k]) + dot((e_new / den).astype(BF), vn)
                OS[:, i] = o.reshape(T, HL, HEAD_DIM)
                KO[m, i] = kn
                VO[m, i] = vn
            if NCH > SLOTS:
                @pl.when(c < NCH - SLOTS)
                def _():
                    start(kv_copies(l, m, c + SLOTS, slot))

            if nxt[0] < L:
                @pl.when(c >= NCH - SLOTS)
                def _():
                    start(kv_copies(nxt[0], nxt[1], c - (NCH - SLOTS), slot))
            return 0
        lax.fori_loop(0, NCH, chunk, 0)
        start(ko_copies(l, m))

        def body(i, _):
            rows = pl.ds(pl.multiple_of(i * RB, RB), RB)
            for h in range(8):
                OB[m, ty, rows, pl.ds(h * 128, 128)] = OS[i, :, h, :].astype(BF)
            return 0
        lax.fori_loop(0, T, body, 0)
        o_copy(m).start()

    def p_copy(m):
        return rc(XP.at[m, :, oth_half], XC.at[m], p_ss.at[m], p_rs.at[m], cpeer)

    def x_copy(ph, m):
        return rc(XS.at[m], XR.at[ph, m], x_ss.at[m], x_rs.at[ph, m], xpeer)

    def a_copy(m):
        return rc(AF.at[m, :, own_half], AF.at[m, :, own_half], a_ss.at[m], a_rs.at[m], cpeer)

    def phase_o(m, l):
        o_copy(m).wait()
        for half in (1 - core, core):
            def body(i, _):
                cols = pl.ds(pl.multiple_of(half * HALF + i * TW, TW), TW)
                XP[m, :, cols] = dot(OB[m].reshape(2 * R, QW), WO[:, cols]).astype(BF)
                return 0
            lax.fori_loop(0, 2, body, 0)
            if half is not core:
                p_copy(m).start()

    def phase_d(m, l):
        for n in range(3):
            c_copy(m, n).wait()
        for half in (1 - core, core):
            def body(i, _):
                cols = pl.ds(pl.multiple_of(half * HALF + i * TW, TW), TW)
                cm = C[m].reshape(2 * R, FP)
                XP[m, :, cols] = dot(cm[:, :FW], WD[:, cols]).astype(BF)
                return 0
            lax.fori_loop(0, 2, body, 0)
            if half is not core:
                p_copy(m).start()

    def phase_2(ph, m):
        p_copy(m).wait()

        def body(i, _):
            rows = pl.ds(pl.multiple_of(i * 16, 16), 16)
            XS[m, rows] = (XP[m, rows, own_half].astype(F32) + XC[m, rows].astype(F32)).astype(BF)
            return 0
        lax.fori_loop(0, 2 * R // 16, body, 0)
        x_copy(ph, m).start()

    def phase_3(ph, m):
        x_copy(ph, m).wait()

        def body(i, _):
            rows = pl.ds(pl.multiple_of(i * 16, 16), 16)
            z = (XS[m, rows].astype(F32) + XR[ph, m, rows].astype(F32)).astype(BF)
            AF[m, rows, own_half] = z
            zf = z.astype(F32)
            acc = lane_fold(zf * zf)
            RSUM[i // RC, pl.ds(pl.multiple_of(lax.rem(i, RC) * 16, 16), 16)] = acc
            return 0
        lax.fori_loop(0, 2 * R // 16, body, 0)
        a_copy(m).start()
        stat_send(1 + ph, m)

    def phase_h(ph, m, l):
        gain = (ag_ref, mg_ref)[ph]
        stat_recv(1 + ph, m)
        a_copy(m).wait()

        def body(i, _):
            y = i // RC
            rows = pl.ds(pl.multiple_of(lax.rem(i, RC) * 16, 16), 16)
            arow = pl.ds(pl.multiple_of(i * 16, 16), 16)
            scale = jnp.concatenate([RSC[y, rows]] * 16, axis=1)
            X[m, y, rows] = (X[m, y, rows].astype(F32) + AF[m, arow].astype(F32) * scale * gain[pl.ds(l, 1)].astype(F32)).astype(BF)
            return 0
        lax.fori_loop(0, 2 * R // 16, body, 0)

    def c_copy(m, n):
        cols = pl.ds(*GU_SENDS[n])
        return rc(C.at[m, ty, :, cols], C.at[m, ty, :, cols], c_ss.at[m, n], c_rs.at[m, n], ypeer)

    def phase_c(m, lo, hi):
        for n in range(lo, hi):
            g_copy(m, n).wait()

            def body(i, _):
                rows = pl.ds(pl.multiple_of(i * 16, 16), 16)
                cols = pl.ds(*GU_SENDS[n])
                g = (GP[m, 0, ty, rows, cols].astype(F32) + GR[m, 0, rows, cols].astype(F32)).astype(BF).astype(F32)
                u = (GP[m, 1, ty, rows, cols].astype(F32) + GR[m, 1, rows, cols].astype(F32)).astype(BF).astype(F32)
                C[m, ty, rows, cols] = (jax.nn.silu(g) * u).astype(BF)
                return 0
            lax.fori_loop(0, R // 16, body, 0)
            c_copy(m, n).start()

    def y_copies(m):
        out = []
        for y in range(2):
            for t in range(T):
                out.append(lc(X.at[m, y, pl.ds(t * RB, RB)], y_ref.at[t, pl.ds(y * NB * RB + m * RB, RB)], y_sem.at[(m * 2 + y) * T + t]))
        return out

    wait(emb_copies())
    seen = set()
    for op, *arg in ORDER:
        if op == "Lg":
            start(gu_loads(arg[0]))
        elif op == "Lq":
            start(qkv_loads(arg[0]))
        elif op == "Lo":
            start(wo_loads(arg[0]))
        elif op == "Ld":
            start(wd_loads(arg[0]))
        elif op == "Q":
            m, l = arg
            phase_q(m, l, ("q", l) not in seen)
            seen.add(("q", l))
        elif op == "Qs":
            m, l, lo, hi = arg
            send_q(m, lo, hi)
        elif op == "S":
            phase_s(arg[0])
        elif op == "T":
            m, l = arg
            phase_t1(m, l)
            phase_t2(m, l)
        elif op == "O":
            m, l = arg
            if ("o", l) not in seen:
                wait(wo_loads(l))
                seen.add(("o", l))
            phase_o(m, l)
        elif op == "2":
            phase_2(arg[0], arg[1])
        elif op == "3":
            phase_3(arg[0], arg[1])
        elif op == "H":
            ph, m, l = arg
            phase_h(ph, m, l)
            if ph == 1 and l == L - 1:
                start(y_copies(m))
        elif op == "G":
            m, l = arg
            if ("g", l) not in seen:
                wait(gu_loads(l))
                seen.add(("g", l))
            phase_g(m)
        elif op == "Gs":
            m, l, lo, hi = arg
            send_g(m, lo, hi)
        elif op == "C":
            m, l, lo, hi = arg
            phase_c(m, lo, hi)
        elif op == "D":
            m, l = arg
            if ("d", l) not in seen:
                wait(wd_loads(l))
                seen.add(("d", l))
            phase_d(m, l)
    for m in range(NB):
        wait(y_copies(m))
    for m in range(NB):
        wait(ko_copies(L - 1, m))


def cache_kernel(start_ref, k_ref, v_ref, kn_ref, vn_ref, ko_ref, vo_ref):
    c = pl.program_id(1)
    base = lax.axis_index("tpy") * NB * RB + c * k_ref.shape[1]
    ko_ref[...] = k_ref[...]
    vo_ref[...] = v_ref[...]
    for i in range(k_ref.shape[1]):
        p = start_ref[base + i]
        for t in range(T):
            ko_ref[0, i, p + t] = kn_ref[0, i, t]
            vo_ref[0, i, p + t] = vn_ref[0, i, t]


def solution(mesh):
    act_spec = P(None, 'dp', 'tpy')
    cache_spec = P(None, ('dp', 'tpy'), None, 'tpx', None)
    col_spec = P(None, 'tpy', 'tpx')
    row_spec = P(None, 'tpx', 'tpy')
    head_gain = P(None, 'tpx')
    width_gain = P(None, 'tpy')

    def device_fn(embeds, start_pos, k_cache, v_cache, w_query, w_key, w_value, w_out, w_gate, w_up, w_down, q_gain, k_gain, attn_gain, mlp_gain):
        rows = NB * RB
        pos = (start_pos.reshape(2, NB, 1, RB) + jnp.arange(T, dtype=jnp.int32)[None, None, :, None]).reshape(2, NB, R)
        inv_freq = jnp.power(THETA, jnp.arange(HEAD_DIM // 2, dtype=F32) * (-2.0 / HEAD_DIM))
        ang = pos.astype(F32)[..., None] * inv_freq
        cos_part, sin_part = jnp.cos(ang), jnp.sin(ang)
        cos2 = jnp.concatenate([cos_part, cos_part], axis=-1)
        sin2 = jnp.concatenate([-sin_part, sin_part], axis=-1)
        hbm = pl.BlockSpec(memory_space=pl.ANY)
        vm = pl.BlockSpec(memory_space=pltpu.VMEM)
        dma = pltpu.SemaphoreType.DMA
        y, kn, vn = pl.pallas_call(
            main_kernel,
            out_shape=[
                jax.ShapeDtypeStruct(embeds.shape, BF),
                jax.ShapeDtypeStruct((L, rows, T * HL, HEAD_DIM), BF),
                jax.ShapeDtypeStruct((L, rows, T * HL, HEAD_DIM), BF),
            ],
            in_specs=[pl.BlockSpec(memory_space=pltpu.SMEM)] + [hbm] * 10 + [vm] * 6,
            out_specs=[hbm] * 3,
            scratch_shapes=[
                pltpu.VMEM((NB, 2, R, DW), BF),
                pltpu.VMEM((2, FW, DW), BF),
                pltpu.VMEM((QW, DW), BF),
                pltpu.VMEM((FW, DW), BF),
                pltpu.VMEM((NB, 2, 2, R, FP), BF),
                pltpu.VMEM((NB, 2, R, FP), BF),
                pltpu.VMEM((NB, 2, R, FP), BF),
                pltpu.VMEM((NB, 2, R, QW), BF),
                pltpu.VMEM((T, RB, HL, HEAD_DIM), F32),
                pltpu.VMEM((T, RB, HL, HEAD_DIM), F32),
                pltpu.VMEM((T, RB, HL, HEAD_DIM), F32),
                pltpu.VMEM((T, RB, HL, HEAD_DIM), F32),
                pltpu.VMEM((NB, RB, T * HL, HEAD_DIM), BF),
                pltpu.VMEM((NB, RB, T * HL, HEAD_DIM), BF),
                pltpu.VMEM((SLOTS, CB, SH, HEAD_DIM), BF),
                pltpu.VMEM((SLOTS, CB, SH, HEAD_DIM), BF),
                pltpu.VMEM((NB, 2 * R, DW), BF),
                pltpu.VMEM((NB, 2 * R, HALF), BF),
                pltpu.VMEM((NB, 2 * R, HALF), BF),
                pltpu.VMEM((2, NB, 2 * R, HALF), BF),
                pltpu.VMEM((NB, 2 * R, DW), BF),
                pltpu.VMEM((2, R, 128), F32),
                pltpu.VMEM((2, R, 128), F32),
                pltpu.VMEM((3, NB, 8, 128), F32),
                pltpu.VMEM((3, NB, 3, 8, 128), F32),
                dma((NB * 2 * T,)), dma((6,)), dma((8,)), dma((1,)), dma((4,)), dma((2, SLOTS)), dma((2, NB)), dma((NB * 2 * T,)),
                dma((NB, 3)), dma((NB, 3)), dma((NB, 3)), dma((NB, 3)), dma((NB,)), dma((NB,)),
                dma((NB,)), dma((NB,)), dma((NB,)), dma((2, NB)), dma((NB,)), dma((NB,)), dma((3, NB, 3)), dma((3, NB, 3)),
            ],
            compiler_params=pltpu.CompilerParams(collective_id=0, has_side_effects=True, vmem_limit_bytes=67043328),
            name="layers",
        )(start_pos, embeds, k_cache.reshape(L, rows, SH, HEAD_DIM), v_cache.reshape(L, rows, SH, HEAD_DIM),
          w_query, w_key, w_value, w_out, w_gate.transpose(0, 2, 1), w_up.transpose(0, 2, 1), w_down, q_gain, k_gain, attn_gain, mlp_gain, cos2, sin2)
        bc = 16
        big = pl.BlockSpec((1, bc, SEQ, HL, HEAD_DIM), lambda l, c, s: (l, c, 0, 0, 0))
        small = pl.BlockSpec((1, bc, T, HL, HEAD_DIM), lambda l, c, s: (l, c, 0, 0, 0))
        k_out, v_out = pl.pallas_call(
            cache_kernel,
            out_shape=[jax.ShapeDtypeStruct(k_cache.shape, BF)] * 2,
            grid_spec=pltpu.PrefetchScalarGridSpec(
                num_scalar_prefetch=1, grid=(L, rows // bc), in_specs=[big, big, small, small], out_specs=[big, big]),
            compiler_params=pltpu.CompilerParams(vmem_limit_bytes=48 * 1024 * 1024),
            name="caches",
        )(start_pos, k_cache, v_cache, kn.reshape(L, rows, T, HL, HEAD_DIM), vn.reshape(L, rows, T, HL, HEAD_DIM))
        return y, k_out, v_out

    return jax.shard_map(device_fn, mesh=mesh, in_specs=(act_spec, P('dp'), cache_spec, cache_spec, col_spec, col_spec, col_spec, row_spec, col_spec, col_spec, row_spec, head_gain, head_gain, width_gain, width_gain), out_specs=(act_spec, cache_spec, cache_spec), check_vma=False)
```

```python
import functools
import math
import jax
import jax.numpy as jnp
from jax import lax
from jax.experimental import pallas as pl
from jax.experimental.pallas import tpu as pltpu
from jax.sharding import PartitionSpec as P

HEAD_DIM = 128
EPS = 1e-6
THETA = 500000.0
SCORE_SCALE = 1.0 / math.sqrt(HEAD_DIM)
NEG_BIG = -1e30
MESH = pl.DeviceIdType.MESH
BF = jnp.bfloat16
F32 = jnp.float32

L = 2
T = 3
NB = 4
RB = 16
R = T * RB
HL = 8
DW = 2048
QW = HL * HEAD_DIM
FW = 2752
FP = 2816
SEQ = 64
SH = SEQ * HL
CB = 4
NCH = RB // CB
SLOTS = 4
TW = 512
HALF = DW // 2
RC = R // 16
GU_SENDS = [(0, 1024), (1024, 1024), (2048, 768)]
QKV_TILES = [(0, 0), (0, 512), (0, 1024), (0, 1536), (1, 0), (1, 512)]


Q_ROWS = (2, 1)
G_ROWS = 1
ORDER = [
    ("Q", 0, 0),
    ("Qs", 0, 0, 0, 2),
    ("Q", 2, 0),
    ("Qs", 1, 0, 0, 1),
    ("S", 0, 0),
    ("Qs", 1, 0, 1, 2),
    ("Qs", 2, 0, 0, 1),
    ("T", 0, 0),
    ("Qs", 2, 0, 1, 2),
    ("Qs", 3, 0, 0, 1),
    ("S", 1, 0),
    ("T", 1, 0),
    ("Qs", 3, 0, 1, 2),
    ("O", 0, 0),
    ("S", 2, 0),
    ("Lg", 0),
    ("2", 0, 0, 0),
    ("T", 2, 0),
    ("O", 1, 0),
    ("3", 0, 0, 0),
    ("2", 0, 1, 0),
    ("S", 3, 0),
    ("H", 0, 0, 0),
    ("G", 0, 0),
    ("Gs", 0, 0, 0, 1),
    ("O", 2, 0),
    ("3", 0, 1, 0),
    ("Gs", 0, 0, 1, 2),
    ("T", 3, 0),
    ("2", 0, 2, 0),
    ("C", 0, 0, 0, 1),
    ("Gs", 0, 0, 2, 3),
    ("H", 0, 1, 0),
    ("G", 1, 0),
    ("Gs", 1, 0, 0, 1),
    ("3", 0, 2, 0),
    ("O", 3, 0),
    ("2", 0, 3, 0),
    ("C", 0, 0, 1, 3),
    ("C", 1, 0, 0, 1),
    ("Gs", 1, 0, 1, 3),
    ("H", 0, 2, 0),
    ("G", 2, 0),
    ("3", 0, 3, 0),
    ("Gs", 2, 0, 0, 1),
    ("D", 0, 0),
    ("2", 1, 0, 0),
    ("Gs", 2, 0, 1, 2),
    ("C", 1, 0, 1, 3),
    ("H", 0, 3, 0),
    ("Gs", 2, 0, 2, 3),
    ("G", 3, 0),
    ("C", 2, 0, 0, 1),
    ("3", 1, 0, 0),
    ("Gs", 3, 0, 0, 1),
    ("C", 2, 0, 1, 3),
    ("Gs", 3, 0, 1, 2),
    ("D", 1, 0),
    ("Lq", 1),
    ("H", 1, 0, 0),
    ("2", 1, 1, 0),
    ("Q", 0, 1),
    ("3", 1, 1, 0),
    ("Qs", 0, 1, 0, 1),
    ("D", 2, 0),
    ("Qs", 0, 1, 1, 2),
    ("Gs", 3, 0, 2, 3),
    ("H", 1, 1, 0),
    ("2", 1, 2, 0),
    ("C", 3, 0, 0, 2),
    ("Q", 1, 1),
    ("S", 0, 1),
    ("C", 3, 0, 2, 3),
    ("3", 1, 2, 0),
    ("Qs", 1, 1, 0, 1),
    ("Lo", 1),
    ("Qs", 1, 1, 1, 2),
    ("T", 0, 1),
    ("D", 3, 0),
    ("2", 1, 3, 0),
    ("H", 1, 2, 0),
    ("Q", 2, 1),
    ("S", 1, 1),
    ("Qs", 2, 1, 0, 1),
    ("O", 0, 1),
    ("3", 1, 3, 0),
    ("Qs", 2, 1, 1, 2),
    ("2", 0, 0, 1),
    ("T", 1, 1),
    ("H", 1, 3, 0),
    ("Q", 3, 1),
    ("Qs", 3, 1, 0, 1),
    ("S", 2, 1),
    ("Lg", 1),
    ("O", 1, 1),
    ("Qs", 3, 1, 1, 2),
    ("3", 0, 0, 1),
    ("T", 2, 1),
    ("2", 0, 1, 1),
    ("S", 3, 1),
    ("H", 0, 0, 1),
    ("G", 0, 1),
    ("Gs", 0, 1, 0, 1),
    ("3", 0, 1, 1),
    ("Gs", 0, 1, 1, 2),
    ("O", 2, 1),
    ("T", 3, 1),
    ("Gs", 0, 1, 2, 3),
    ("2", 0, 2, 1),
    ("C", 0, 1, 0, 1),
    ("H", 0, 1, 1),
    ("G", 1, 1),
    ("Gs", 1, 1, 0, 1),
    ("3", 0, 2, 1),
    ("C", 0, 1, 1, 2),
    ("Gs", 1, 1, 1, 2),
    ("O", 3, 1),
    ("Ld", 1),
    ("2", 0, 3, 1),
    ("Gs", 1, 1, 2, 3),
    ("H", 0, 2, 1),
    ("C", 0, 1, 2, 3),
    ("C", 1, 1, 0, 1),
    ("G", 2, 1),
    ("Gs", 2, 1, 0, 1),
    ("3", 0, 3, 1),
    ("C", 1, 1, 1, 2),
    ("Gs", 2, 1, 1, 3),
    ("C", 1, 1, 2, 3),
    ("H", 0, 3, 1),
    ("C", 2, 1, 0, 1),
    ("G", 3, 1),
    ("Gs", 3, 1, 0, 1),
    ("C", 2, 1, 1, 2),
    ("D", 0, 1),
    ("Gs", 3, 1, 1, 2),
    ("D", 1, 1),
    ("C", 2, 1, 2, 3),
    ("Gs", 3, 1, 2, 3),
    ("C", 3, 1, 0, 1),
    ("2", 1, 0, 1),
    ("C", 3, 1, 1, 2),
    ("2", 1, 1, 1),
    ("C", 3, 1, 2, 3),
    ("D", 2, 1),
    ("3", 1, 0, 1),
    ("2", 1, 2, 1),
    ("3", 1, 1, 1),
    ("D", 3, 1),
    ("2", 1, 3, 1),
    ("H", 1, 0, 1),
    ("3", 1, 2, 1),
    ("H", 1, 2, 1),
    ("3", 1, 3, 1),
    ("H", 1, 1, 1),
    ("H", 1, 3, 1),
]


def lane_fold(z):
    return jnp.broadcast_to(jnp.sum(z, axis=1, keepdims=True), (z.shape[0], 128))


def dot(a, b):
    return jnp.dot(a, b, preferred_element_type=F32)


def dot_t(a, b):
    return lax.dot_general(a, b, (((1,), (1,)), ((), ())), preferred_element_type=F32)


def main_kernel(start_ref, emb_ref, kc_ref, vc_ref, wq_ref, wk_ref, wv_ref, wo_ref, wg_ref, wu_ref, wd_ref,
                qg_ref, kg_ref, ag_ref, mg_ref, cos_ref, sin_ref,
                y_ref, kn_ref, vn_ref,
                X, W1, WO, WD, GP, GR, C, OB, QS, KS, VS, OS, KO, VO, KB, VB, XP, XC, XS, XR, AF, RSUM, RSC, ST, SR,
                in_sem, q_wsem, g_wsem, o_wsem, d_wsem, kv_sem, ko_sem, y_sem,
                g_ss, g_rs, c_ss, c_rs, o_ss, o_rs, p_ss, p_rs, x_ss, x_rs, a_ss, a_rs, st_ss, st_rs):
    ty = lax.axis_index("tpy")
    tx = lax.axis_index("tpx")
    core = lax.rem(tx, 2)
    oy = 1 - ty
    cx = tx + 1 - 2 * core
    xx = lax.rem(tx + 2, 4)
    dx = 3 - tx
    ypeer = {"tpy": oy}
    cpeer = {"tpx": cx}
    xpeer = {"tpx": xx}
    xdiag = {"tpx": dx}
    ydiag = {"tpy": oy, "tpx": cx}
    own_half = pl.ds(pl.multiple_of(core * HALF, HALF), HALF)
    oth_half = pl.ds(pl.multiple_of((1 - core) * HALF, HALF), HALF)

    def rc(src, dst, ss, rs, dev):
        return pltpu.make_async_remote_copy(src_ref=src, dst_ref=dst, send_sem=ss, recv_sem=rs, device_id=dev, device_id_type=MESH)

    def lc(src, dst, sem):
        return pltpu.make_async_copy(src, dst, sem)

    def emb_copies():
        out = []
        for m in range(NB):
            for y in range(2):
                for t in range(T):
                    out.append(lc(emb_ref.at[t, pl.ds(y * NB * RB + m * RB, RB)], X.at[m, y, pl.ds(t * RB, RB)], in_sem.at[(m * 2 + y) * T + t]))
        return out

    def qkv_load(l, n):
        j, c0 = QKV_TILES[n]
        src = (wq_ref, wk_ref, wv_ref)[n // 2]
        return lc(src.at[l, :, pl.ds((n % 2) * TW, TW)], W1.at[j, pl.ds(0, DW), pl.ds(c0, TW)], q_wsem.at[n])

    def qkv_loads(l):
        return [qkv_load(l, n) for n in range(6)]

    def gu_loads(l):
        return [lc((wg_ref, wu_ref)[j].at[l, pl.ds(r * 688, 688)], W1.at[j, pl.ds(r * 688, 688)], g_wsem.at[j * 4 + r]) for r in range(4) for j in range(2)]

    def wo_loads(l):
        return [lc(wo_ref.at[l], WO, o_wsem.at[0])]

    def wd_loads(l):
        return [lc(wd_ref.at[l, pl.ds(r * 688, 688)], WD.at[pl.ds(r * 688, 688)], d_wsem.at[r]) for r in range(4)]

    def start(copies):
        for cp in copies:
            cp.start()

    def wait(copies):
        for cp in copies:
            cp.wait()

    def kv_copies(l, m, c, slot):
        rows = pl.ds(m * RB + c * CB, CB)
        return [lc(kc_ref.at[l, rows], KB.at[slot], kv_sem.at[0, slot]), lc(vc_ref.at[l, rows], VB.at[slot], kv_sem.at[1, slot])]

    start(emb_copies())
    start(qkv_loads(0))

    barrier = pltpu.get_barrier_semaphore()
    for dev in (ypeer, cpeer, xpeer, xdiag, ydiag):
        pl.semaphore_signal(barrier, inc=1, device_id=dev, device_id_type=MESH)
    pl.semaphore_wait(barrier, 5)

    for c in range(SLOTS):
        start(kv_copies(0, 0, c, c))
    start(wo_loads(0))
    start(wd_loads(0))

    def q_copy(m, n):
        cols = pl.ds(0, (2 * QW, QW)[n])
        return rc(GP.at[m, n, oy, :, cols], GR.at[m, n, :, cols], g_ss.at[m, n], g_rs.at[m, n], ypeer)

    def g_copy(m, n):
        cols = pl.ds(*GU_SENDS[n])
        return rc(GP.at[m, :, oy, :, cols], GR.at[m, :, :, cols], g_ss.at[m, n], g_rs.at[m, n], ypeer)

    def compute_tile(m, k, j, c0, w, transposed=False):
        xm = X[pl.ds(m, k)].reshape(k * 2 * R, DW)
        if transposed:
            res = dot_t(xm, W1[j, pl.ds(c0, w), :]).astype(BF)
        else:
            res = dot(xm, W1[j, pl.ds(0, DW), pl.ds(c0, w)]).astype(BF)
        GP[pl.ds(m, k), j, :, :, pl.ds(c0, w)] = res.reshape(k, 2, R, w)

    def phase_q(m, k, l, fresh):
        for j, cnt in ((0, 4), (1, 2)):
            if fresh:
                for i in range(cnt):
                    qkv_load(l, j * 4 + i).wait()

            def body(i, _):
                compute_tile(m, k, j, pl.multiple_of(i * TW, TW), TW)
                return 0
            lax.fori_loop(0, cnt, body, 0)

    def send_q(m, lo, hi):
        for n in range(lo, hi):
            q_copy(m, n).start()

    def phase_g(m, k):
        def body(i, _):
            for j in range(2):
                compute_tile(m, k, j, pl.multiple_of(i * TW, TW), TW, True)
            return 0
        lax.fori_loop(0, 5, body, 0)
        for j in range(2):
            compute_tile(m, k, j, 2560, 192, True)

    def send_g(m, lo, hi):
        for n in range(lo, hi):
            g_copy(m, n).start()

    def stat_copies(kind, m):
        peers = (cpeer, xpeer, xdiag) if kind == 0 else (cpeer, ypeer, ydiag)
        return [rc(ST.at[kind, m], SR.at[kind, m, k], st_ss.at[kind, m, k], st_rs.at[kind, m, k], peers[k]) for k in range(3)]

    def stat_send(kind, m):
        v0 = RSUM[0]
        v1 = RSUM[1]
        lane = lax.broadcasted_iota(jnp.int32, (R, 128), 1)
        both = jnp.where(lane == 0, v0, v1)
        full = jnp.concatenate([both, jnp.zeros((128 - R, 128), F32)], axis=0)
        ST[kind, m] = full.T[0:8]
        start(stat_copies(kind, m))

    def stat_recv(kind, m):
        wait(stat_copies(kind, m))
        total = (ST[kind, m] + SR[kind, m, 0]) + (SR[kind, m, 1] + SR[kind, m, 2])
        back = jnp.concatenate([total] * 16, axis=0).T
        scale = lax.rsqrt(back / 4096.0 + EPS)
        RSC[0] = jnp.broadcast_to(scale[0:R, 0:1], (R, 128))
        RSC[1] = jnp.broadcast_to(scale[0:R, 1:2], (R, 128))

    def phase_s(m):
        for n in range(2):
            q_copy(m, n).wait()

        def body(i, _):
            rows = pl.ds(pl.multiple_of(i * 16, 16), 16)
            qk = pl.ds(0, 2 * QW)
            z = (GP[m, 0, ty, rows, qk].astype(F32) + GR[m, 0, rows, qk].astype(F32)).astype(BF)
            GR[m, 0, rows, qk] = z
            zf = z.astype(F32)
            sq = zf * zf
            RSUM[0, rows] = lane_fold(sq[:, :QW])
            RSUM[1, rows] = lane_fold(sq[:, QW:])
            cols = pl.ds(0, QW)
            GR[m, 1, rows, cols] = (GP[m, 1, ty, rows, cols].astype(F32) + GR[m, 1, rows, cols].astype(F32)).astype(BF)
            return 0
        lax.fori_loop(0, R // 16, body, 0)
        stat_send(0, m)

    def phase_t1(m, l):
        stat_recv(0, m)

        gain = jnp.concatenate([qg_ref[pl.ds(l, 1)], kg_ref[pl.ds(l, 1)]], axis=1).astype(F32)
        low = lax.rem(lax.broadcasted_iota(jnp.int32, (RB, 2 * QW), 1), HEAD_DIM) < HEAD_DIM // 2

        def body(i, _):
            rows = pl.ds(pl.multiple_of(i * RB, RB), RB)
            scale = jnp.concatenate([RSC[0, rows]] * HL + [RSC[1, rows]] * HL, axis=1)
            z = GR[m, 0, rows, pl.ds(0, 2 * QW)].astype(F32) * scale * gain
            turned = jnp.where(low, pltpu.roll(z, 2 * QW - HEAD_DIM // 2, 1), pltpu.roll(z, HEAD_DIM // 2, 1))
            rot = z * jnp.concatenate([cos_ref[ty, m, rows]] * (2 * HL), axis=1) + turned * jnp.concatenate([sin_ref[ty, m, rows]] * (2 * HL), axis=1)
            rot = rot.astype(BF).astype(F32)
            v = GR[m, 1, rows, pl.ds(0, QW)].astype(F32)
            for h in range(HL):
                QS[i, :, h, :] = rot[:, h * HEAD_DIM:(h + 1) * HEAD_DIM]
                KS[i, :, h, :] = rot[:, QW + h * HEAD_DIM:QW + (h + 1) * HEAD_DIM]
                VS[i, :, h, :] = v[:, h * HEAD_DIM:(h + 1) * HEAD_DIM]
            return 0
        lax.fori_loop(0, T, body, 0)

    def ko_copies(l, m):
        rows = pl.ds(m * RB, RB)
        return [lc(KO.at[m], kn_ref.at[l, rows], ko_sem.at[0, m]), lc(VO.at[m], vn_ref.at[l, rows], ko_sem.at[1, m])]

    def o_copy(m):
        return rc(OB.at[m, ty], OB.at[m, ty], o_ss.at[m], o_rs.at[m], ypeer)

    def phase_t2(m, l):
        if l > 0:
            wait(ko_copies(l - 1, m))
        row = lax.broadcasted_iota(jnp.int32, (T * HL, SH), 0)
        col = lax.broadcasted_iota(jnp.int32, (T * HL, SH), 1)
        colm = jnp.where(lax.rem(row, HL) == lax.rem(col, HL), col, SH)
        rown = lax.broadcasted_iota(jnp.int32, (T * HL, T * HL), 0)
        coln = lax.broadcasted_iota(jnp.int32, (T * HL, T * HL), 1)
        newm = (lax.rem(rown, HL) == lax.rem(coln, HL)) & (coln <= rown)

        nxt = (l, m + 1) if m + 1 < NB else (l + 1, 0)

        def chunk(c, _):
            slot = lax.rem(c, SLOTS)
            wait(kv_copies(l, m, c, slot))
            for k in range(CB):
                i = c * CB + k
                q = QS[:, i].reshape(T * HL, HEAD_DIM).astype(BF)
                kn = KS[:, i].reshape(T * HL, HEAD_DIM).astype(BF)
                vn = VS[:, i].reshape(T * HL, HEAD_DIM).astype(BF)
                limit = start_ref[ty * NB * RB + m * RB + i] * HL
                s_old = jnp.where(colm < limit, dot_t(q, KB[slot, k]) * SCORE_SCALE, NEG_BIG)
                s_new = jnp.where(newm, dot_t(q, kn) * SCORE_SCALE, NEG_BIG)
                top = jnp.maximum(jnp.max(s_old, axis=1, keepdims=True), jnp.max(s_new, axis=1, keepdims=True))
                e_old = jnp.exp(s_old - top)
                e_new = jnp.exp(s_new - top)
                den = jnp.sum(e_old, axis=1, keepdims=True) + jnp.sum(e_new, axis=1, keepdims=True)
                o = dot((e_old / den).astype(BF), VB[slot, k]) + dot((e_new / den).astype(BF), vn)
                OS[:, i] = o.reshape(T, HL, HEAD_DIM)
                KO[m, i] = kn
                VO[m, i] = vn
            if NCH > SLOTS:
                @pl.when(c < NCH - SLOTS)
                def _():
                    start(kv_copies(l, m, c + SLOTS, slot))

            if nxt[0] < L:
                @pl.when(c >= NCH - SLOTS)
                def _():
                    start(kv_copies(nxt[0], nxt[1], c - (NCH - SLOTS), slot))
            return 0
        lax.fori_loop(0, NCH, chunk, 0)
        start(ko_copies(l, m))

        def body(i, _):
            rows = pl.ds(pl.multiple_of(i * RB, RB), RB)
            for h in range(8):
                OB[m, ty, rows, pl.ds(h * 128, 128)] = OS[i, :, h, :].astype(BF)
            return 0
        lax.fori_loop(0, T, body, 0)
        o_copy(m).start()

    def p_copy(m):
        return rc(XP.at[m, :, oth_half], XC.at[m], p_ss.at[m], p_rs.at[m], cpeer)

    def x_copy(ph, m):
        return rc(XS.at[m], XR.at[ph, m], x_ss.at[m], x_rs.at[ph, m], xpeer)

    def a_copy(m):
        return rc(AF.at[m, :, own_half], AF.at[m, :, own_half], a_ss.at[m], a_rs.at[m], cpeer)

    def phase_o(m, l):
        o_copy(m).wait()
        for half in (1 - core, core):
            def body(i, _):
                cols = pl.ds(pl.multiple_of(half * HALF + i * TW, TW), TW)
                XP[m, :, cols] = dot(OB[m].reshape(2 * R, QW), WO[:, cols]).astype(BF)
                return 0
            lax.fori_loop(0, 2, body, 0)
            if half is not core:
                p_copy(m).start()

    def phase_d(m, l):
        for n in range(3):
            c_copy(m, n).wait()
        for half in (1 - core, core):
            def body(i, _):
                cols = pl.ds(pl.multiple_of(half * HALF + i * TW, TW), TW)
                cm = C[m].reshape(2 * R, FP)
                XP[m, :, cols] = dot(cm[:, :FW], WD[:, cols]).astype(BF)
                return 0
            lax.fori_loop(0, 2, body, 0)
            if half is not core:
                p_copy(m).start()

    def phase_2(ph, m):
        p_copy(m).wait()

        def body(i, _):
            rows = pl.ds(pl.multiple_of(i * 16, 16), 16)
            XS[m, rows] = (XP[m, rows, own_half].astype(F32) + XC[m, rows].astype(F32)).astype(BF)
            return 0
        lax.fori_loop(0, 2 * R // 16, body, 0)
        x_copy(ph, m).start()

    def phase_3(ph, m):
        x_copy(ph, m).wait()

        def body(i, _):
            rows = pl.ds(pl.multiple_of(i * 16, 16), 16)
            z = (XS[m, rows].astype(F32) + XR[ph, m, rows].astype(F32)).astype(BF)
            AF[m, rows, own_half] = z
            zf = z.astype(F32)
            acc = lane_fold(zf * zf)
            RSUM[i // RC, pl.ds(pl.multiple_of(lax.rem(i, RC) * 16, 16), 16)] = acc
            return 0
        lax.fori_loop(0, 2 * R // 16, body, 0)
        a_copy(m).start()
        stat_send(1 + ph, m)

    def phase_h(ph, m, l):
        gain = (ag_ref, mg_ref)[ph]
        stat_recv(1 + ph, m)
        a_copy(m).wait()

        def body(i, _):
            y = i // RC
            rows = pl.ds(pl.multiple_of(lax.rem(i, RC) * 16, 16), 16)
            arow = pl.ds(pl.multiple_of(i * 16, 16), 16)
            scale = jnp.concatenate([RSC[y, rows]] * 16, axis=1)
            X[m, y, rows] = (X[m, y, rows].astype(F32) + AF[m, arow].astype(F32) * scale * gain[pl.ds(l, 1)].astype(F32)).astype(BF)
            return 0
        lax.fori_loop(0, 2 * R // 16, body, 0)

    def c_copy(m, n):
        cols = pl.ds(*GU_SENDS[n])
        return rc(C.at[m, ty, :, cols], C.at[m, ty, :, cols], c_ss.at[m, n], c_rs.at[m, n], ypeer)

    def phase_c(m, lo, hi):
        for n in range(lo, hi):
            g_copy(m, n).wait()

            def body(i, _):
                rows = pl.ds(pl.multiple_of(i * 16, 16), 16)
                cols = pl.ds(*GU_SENDS[n])
                g = (GP[m, 0, ty, rows, cols].astype(F32) + GR[m, 0, rows, cols].astype(F32)).astype(BF).astype(F32)
                u = (GP[m, 1, ty, rows, cols].astype(F32) + GR[m, 1, rows, cols].astype(F32)).astype(BF).astype(F32)
                C[m, ty, rows, cols] = (jax.nn.silu(g) * u).astype(BF)
                return 0
            lax.fori_loop(0, R // 16, body, 0)
            c_copy(m, n).start()

    def y_copies(m):
        out = []
        for y in range(2):
            for t in range(T):
                out.append(lc(X.at[m, y, pl.ds(t * RB, RB)], y_ref.at[t, pl.ds(y * NB * RB + m * RB, RB)], y_sem.at[(m * 2 + y) * T + t]))
        return out

    wait(emb_copies())
    seen = set()
    for op, *arg in ORDER:
        if op == "Lg":
            start(gu_loads(arg[0]))
        elif op == "Lq":
            start(qkv_loads(arg[0]))
        elif op == "Lo":
            start(wo_loads(arg[0]))
        elif op == "Ld":
            start(wd_loads(arg[0]))
        elif op == "Q":
            m, l = arg
            phase_q(m, Q_ROWS[l], l, ("q", l) not in seen)
            seen.add(("q", l))
        elif op == "Qs":
            m, l, lo, hi = arg
            send_q(m, lo, hi)
        elif op == "S":
            phase_s(arg[0])
        elif op == "T":
            m, l = arg
            phase_t1(m, l)
            phase_t2(m, l)
        elif op == "O":
            m, l = arg
            if ("o", l) not in seen:
                wait(wo_loads(l))
                seen.add(("o", l))
            phase_o(m, l)
        elif op == "2":
            phase_2(arg[0], arg[1])
        elif op == "3":
            phase_3(arg[0], arg[1])
        elif op == "H":
            ph, m, l = arg
            phase_h(ph, m, l)
            if ph == 1 and l == L - 1:
                start(y_copies(m))
        elif op == "G":
            m, l = arg
            if ("g", l) not in seen:
                wait(gu_loads(l))
                seen.add(("g", l))
            phase_g(m, G_ROWS)
        elif op == "Gs":
            m, l, lo, hi = arg
            send_g(m, lo, hi)
        elif op == "C":
            m, l, lo, hi = arg
            phase_c(m, lo, hi)
        elif op == "D":
            m, l = arg
            if ("d", l) not in seen:
                wait(wd_loads(l))
                seen.add(("d", l))
            phase_d(m, l)
    for m in range(NB):
        wait(y_copies(m))
    for m in range(NB):
        wait(ko_copies(L - 1, m))


def cache_kernel(start_ref, k_ref, v_ref, kn_ref, vn_ref, ko_ref, vo_ref):
    c = pl.program_id(1)
    base = lax.axis_index("tpy") * NB * RB + c * k_ref.shape[1]
    ko_ref[...] = k_ref[...]
    vo_ref[...] = v_ref[...]
    for i in range(k_ref.shape[1]):
        p = start_ref[base + i]
        for t in range(T):
            ko_ref[0, i, p + t] = kn_ref[0, i, t]
            vo_ref[0, i, p + t] = vn_ref[0, i, t]


def solution(mesh):
    act_spec = P(None, 'dp', 'tpy')
    cache_spec = P(None, ('dp', 'tpy'), None, 'tpx', None)
    col_spec = P(None, 'tpy', 'tpx')
    row_spec = P(None, 'tpx', 'tpy')
    head_gain = P(None, 'tpx')
    width_gain = P(None, 'tpy')

    def device_fn(embeds, start_pos, k_cache, v_cache, w_query, w_key, w_value, w_out, w_gate, w_up, w_down, q_gain, k_gain, attn_gain, mlp_gain):
        rows = NB * RB
        pos = (start_pos.reshape(2, NB, 1, RB) + jnp.arange(T, dtype=jnp.int32)[None, None, :, None]).reshape(2, NB, R)
        inv_freq = jnp.power(THETA, jnp.arange(HEAD_DIM // 2, dtype=F32) * (-2.0 / HEAD_DIM))
        ang = pos.astype(F32)[..., None] * inv_freq
        cos_part, sin_part = jnp.cos(ang), jnp.sin(ang)
        cos2 = jnp.concatenate([cos_part, cos_part], axis=-1)
        sin2 = jnp.concatenate([-sin_part, sin_part], axis=-1)
        hbm = pl.BlockSpec(memory_space=pl.ANY)
        vm = pl.BlockSpec(memory_space=pltpu.VMEM)
        dma = pltpu.SemaphoreType.DMA
        y, kn, vn = pl.pallas_call(
            main_kernel,
            out_shape=[
                jax.ShapeDtypeStruct(embeds.shape, BF),
                jax.ShapeDtypeStruct((L, rows, T * HL, HEAD_DIM), BF),
                jax.ShapeDtypeStruct((L, rows, T * HL, HEAD_DIM), BF),
            ],
            in_specs=[pl.BlockSpec(memory_space=pltpu.SMEM)] + [hbm] * 10 + [vm] * 6,
            out_specs=[hbm] * 3,
            scratch_shapes=[
                pltpu.VMEM((NB, 2, R, DW), BF),
                pltpu.VMEM((2, FW, DW), BF),
                pltpu.VMEM((QW, DW), BF),
                pltpu.VMEM((FW, DW), BF),
                pltpu.VMEM((NB, 2, 2, R, FP), BF),
                pltpu.VMEM((NB, 2, R, FP), BF),
                pltpu.VMEM((NB, 2, R, FP), BF),
                pltpu.VMEM((NB, 2, R, QW), BF),
                pltpu.VMEM((T, RB, HL, HEAD_DIM), F32),
                pltpu.VMEM((T, RB, HL, HEAD_DIM), F32),
                pltpu.VMEM((T, RB, HL, HEAD_DIM), F32),
                pltpu.VMEM((T, RB, HL, HEAD_DIM), F32),
                pltpu.VMEM((NB, RB, T * HL, HEAD_DIM), BF),
                pltpu.VMEM((NB, RB, T * HL, HEAD_DIM), BF),
                pltpu.VMEM((SLOTS, CB, SH, HEAD_DIM), BF),
                pltpu.VMEM((SLOTS, CB, SH, HEAD_DIM), BF),
                pltpu.VMEM((NB, 2 * R, DW), BF),
                pltpu.VMEM((NB, 2 * R, HALF), BF),
                pltpu.VMEM((NB, 2 * R, HALF), BF),
                pltpu.VMEM((2, NB, 2 * R, HALF), BF),
                pltpu.VMEM((NB, 2 * R, DW), BF),
                pltpu.VMEM((2, R, 128), F32),
                pltpu.VMEM((2, R, 128), F32),
                pltpu.VMEM((3, NB, 8, 128), F32),
                pltpu.VMEM((3, NB, 3, 8, 128), F32),
                dma((NB * 2 * T,)), dma((6,)), dma((8,)), dma((1,)), dma((4,)), dma((2, SLOTS)), dma((2, NB)), dma((NB * 2 * T,)),
                dma((NB, 3)), dma((NB, 3)), dma((NB, 3)), dma((NB, 3)), dma((NB,)), dma((NB,)),
                dma((NB,)), dma((NB,)), dma((NB,)), dma((2, NB)), dma((NB,)), dma((NB,)), dma((3, NB, 3)), dma((3, NB, 3)),
            ],
            compiler_params=pltpu.CompilerParams(collective_id=0, has_side_effects=True, vmem_limit_bytes=67043328),
            name="layers",
        )(start_pos, embeds, k_cache.reshape(L, rows, SH, HEAD_DIM), v_cache.reshape(L, rows, SH, HEAD_DIM),
          w_query, w_key, w_value, w_out, w_gate.transpose(0, 2, 1), w_up.transpose(0, 2, 1), w_down, q_gain, k_gain, attn_gain, mlp_gain, cos2, sin2)
        bc = 16
        big = pl.BlockSpec((1, bc, SEQ, HL, HEAD_DIM), lambda l, c, s: (l, c, 0, 0, 0))
        small = pl.BlockSpec((1, bc, T, HL, HEAD_DIM), lambda l, c, s: (l, c, 0, 0, 0))
        k_out, v_out = pl.pallas_call(
            cache_kernel,
            out_shape=[jax.ShapeDtypeStruct(k_cache.shape, BF)] * 2,
            grid_spec=pltpu.PrefetchScalarGridSpec(
                num_scalar_prefetch=1, grid=(L, rows // bc), in_specs=[big, big, small, small], out_specs=[big, big]),
            compiler_params=pltpu.CompilerParams(vmem_limit_bytes=67043328),
            name="caches",
        )(start_pos, k_cache, v_cache, kn.reshape(L, rows, T, HL, HEAD_DIM), vn.reshape(L, rows, T, HL, HEAD_DIM))
        return y, k_out, v_out

    return jax.shard_map(device_fn, mesh=mesh, in_specs=(act_spec, P('dp'), cache_spec, cache_spec, col_spec, col_spec, col_spec, row_spec, col_spec, col_spec, row_spec, head_gain, head_gain, width_gain, width_gain), out_specs=(act_spec, cache_spec, cache_spec), check_vma=False)
```
